256 devices in a mesh: gx: 8 (over z), gy: 4 (over y), gz: 8 (over x, core).
Axes of the slice: x: 4, y: 4, z: 8, core: 2. Of those that a mesh axis runs over, the one named last changes fastest.
Arguments:
- point_data: float32 [1, 6, 131072], P(None, None, ('gx', 'gy', 'gz')), may hold values from -1 to 1
- neighbours: int32 [1, 64, 64, 64, 32], P(None, 'gx', 'gy', 'gz'), may hold values from 0 to 131071, as said below
- counts: int32 [1, 64, 64, 64], P(None, 'gx', 'gy', 'gz'), may hold values from 1 to 32, as said below
- kernel_in: bfloat16 [6, 80], replicated, may hold values from -2.5 to 2.5
- kernel_mid: bfloat16 [80, 80], replicated, may hold values from -0.625 to 0.625
- kernel_out: bfloat16 [80, 64], replicated, may hold values from -0.625 to 0.625
- spectral: bfloat16 [2, 16, 16, 16, 64, 64], P(None, 'gz', 'gx', 'gy'), may hold values from -48 to 48
- skip_weight: bfloat16 [64, 64], replicated, may hold values from -0.75 to 0.75
Outputs:
- latent_out: float32 [1, 64, 64, 64, 64], P(None, 'gx', 'gy', 'gz')
The draws below stay inside these ranges and needn't reach their ends.
Inputs may be any that keep to these rules, and one draw needn't show every extreme that they name: `neighbours`: points are owned by location: point j of a geometry belongs to the device at position j // 512 in the order gx, gy, gz. Every neighbour of a node is owned by the node's own device or by a device whose gx, gy and gz indices each differ from it by at most one. Slots s >= counts of the node are padding that names some point all the same. `counts`: on every device some node of every geometry has all 32 slots valid.
All inputs are finite; a program needn't handle non-finite values.
Results may differ from the reference program's by a relative error of at most 0.02.
Values may be sent and summed in bfloat16 or wider, within the bound.
No kernel may reach another device: no remote copies, remote signals or barrier semaphores. Data moves between devices by JAX's collectives and lax.ppermute only.
A program may use at most 64 MiB of HBM per device.

```python
import math
import jax
import jax.numpy as jnp
from jax import lax

GRID = 64
CH = 64
MODES = 16
KH = 80
NB = 32
PT_DEV = 512
GEOMS = 1
LX = 8
LY = 16
LZ = 8
POINTS = 131072


def draw_neighbours(key, part):
    code_key, slot_key = jax.random.split(jax.random.fold_in(key, 11))
    shape = (GEOMS, GRID, GRID, GRID, NB)
    codes = jax.random.randint(code_key, shape, 0, 54)
    codes = jnp.where(codes >= 27, 13, codes)
    count_x = GRID // LX
    count_y = GRID // LY
    count_z = GRID // LZ
    home_x = (jnp.arange(GRID, dtype=jnp.int32) // LX).reshape(1, GRID, 1, 1, 1)
    home_y = (jnp.arange(GRID, dtype=jnp.int32) // LY).reshape(1, 1, GRID, 1, 1)
    home_z = (jnp.arange(GRID, dtype=jnp.int32) // LZ).reshape(1, 1, 1, GRID, 1)
    owner_x = jnp.clip(home_x + codes // 9 - 1, 0, count_x - 1)
    owner_y = jnp.clip(home_y + codes // 3 % 3 - 1, 0, count_y - 1)
    owner_z = jnp.clip(home_z + codes % 3 - 1, 0, count_z - 1)
    slots = jax.random.randint(slot_key, shape, 0, PT_DEV)
    return (((owner_x * count_y + owner_y) * count_z + owner_z) * PT_DEV + slots).astype(jnp.int32)


def draw_counts(key, part):
    values = jax.random.randint(jax.random.fold_in(key, 12), (GEOMS, GRID, GRID, GRID), 1, NB + 1)
    return values.at[:, ::LX, ::LY, ::LZ].set(NB).astype(jnp.int32)


def block_scale(own_key, extent, cuts, low, high):
    def one(dim, parts):
        draws = jax.random.uniform(jax.random.fold_in(jax.random.fold_in(own_key, 6), dim), (parts,), jnp.float32, low / len(cuts), high / len(cuts))
        return jnp.repeat(jnp.exp(draws), extent[dim] // parts).reshape((-1,) + (1,) * (len(extent) - dim - 1))

    level = one(*cuts[0])
    for cut in cuts[1:]:
        level = level * one(*cut)
    return level


def normal_values(key, shape, deviation, most, pieces=(), kind=jnp.bfloat16):
    drawn = deviation * jax.random.normal(key, shape, jnp.float32)
    if pieces:
        drawn = drawn * block_scale(key, shape, pieces, -0.22, 0.18)
    return jnp.clip(drawn, -most, most).astype(kind)


def setup_inputs(seed: int = 0) -> dict:
    key_list = jax.random.split(jax.random.key(seed), 9)
    return {
        "point_data": jnp.clip(jax.random.uniform(key_list[0], (GEOMS, 6, POINTS), jnp.float32, -1.0, 1.0) * block_scale(key_list[0], (GEOMS, 6, POINTS), ((2, 256),), -0.4, 0.0), -1.0, 1.0),
        "neighbours": draw_neighbours(jax.random.fold_in(key_list[8], 71), 0),
        "counts": draw_counts(jax.random.fold_in(key_list[8], 71), 0),
        "kernel_in": normal_values(key_list[3], (6, KH), 6 ** -0.5, 2.5),
        "kernel_mid": normal_values(key_list[4], (KH, KH), KH ** -0.5, 0.625),
        "kernel_out": normal_values(key_list[5], (KH, CH), KH ** -0.5, 0.625),
        "spectral": normal_values(key_list[6], (2, MODES, MODES, MODES, CH, CH), 8.0, 48.0, ((1, 8), (2, 8), (3, 4))),
        "skip_weight": normal_values(key_list[7], (CH, CH), CH ** -0.5, 0.75),
    }


HIGHEST = lax.Precision.HIGHEST
NORM_FLOOR = 1.0

def tables(length, keep_count, centred):
    position = jnp.arange(length, dtype=jnp.int32)
    frequency = jnp.arange(keep_count, dtype=jnp.int32)
    if centred:
        frequency = jnp.where(frequency < keep_count // 2, frequency, frequency + length - keep_count)
    phases = frequency[:, None] * position[None, :] % length
    angles = phases.astype(jnp.float32) * (2.0 * math.pi / length)
    return (jnp.cos(angles), jnp.sin(angles))

def third_weights(cos_table, sin_table, length):
    factor = jnp.where(jnp.arange(cos_table.shape[0]) == 0, 1.0, 2.0).astype(jnp.float32)[:, None] / length ** 3
    return (cos_table * factor, sin_table * factor)

def contract(pattern, operand, table):
    return jnp.einsum(pattern, operand, table, precision=HIGHEST)

def forward_real(values, cos_table, sin_table, pattern):
    return (contract(pattern, values, cos_table), -contract(pattern, values, sin_table))

def forward_complex(real_part, imag_part, cos_table, sin_table, pattern):
    new_real = contract(pattern, real_part, cos_table) + contract(pattern, imag_part, sin_table)
    new_imag = contract(pattern, imag_part, cos_table) - contract(pattern, real_part, sin_table)
    return (new_real, new_imag)

def inverse_complex(real_part, imag_part, cos_table, sin_table, pattern):
    new_real = contract(pattern, real_part, cos_table) - contract(pattern, imag_part, sin_table)
    new_imag = contract(pattern, real_part, sin_table) + contract(pattern, imag_part, cos_table)
    return (new_real, new_imag)

def inverse_real(real_part, imag_part, cos_table, sin_table, pattern):
    return contract(pattern, real_part, cos_table) - contract(pattern, imag_part, sin_table)

def kernel_mean(pair, valid, kernel_in, kernel_mid, kernel_out):
    hidden_one = jax.nn.gelu(jnp.dot(kernel_in.T, pair, preferred_element_type=jnp.float32), approximate=True).astype(jnp.bfloat16)
    hidden_two = jax.nn.gelu(jnp.dot(kernel_mid.T, hidden_one, preferred_element_type=jnp.float32), approximate=True).astype(jnp.bfloat16)
    values = jnp.dot(kernel_out.T, hidden_two, preferred_element_type=jnp.float32)
    values = values.reshape(values.shape[0], -1, NB)
    slots = jnp.arange(NB, dtype=jnp.int32)
    used = (slots[None, :] < valid[:, None]).astype(jnp.float32)
    total = lax.optimization_barrier(jnp.sum(values * used[None], axis=2))
    return (total / valid.astype(jnp.float32)[None]).T.astype(jnp.bfloat16)

def reference(point_data, neighbours, counts, kernel_in, kernel_mid, kernel_out, spectral, skip_weight):
    centres = (jnp.arange(GRID, dtype=jnp.int32).astype(jnp.float32) + 0.5) / GRID
    row_y = jnp.broadcast_to(centres[:, None, None], (GRID, GRID, NB)).reshape(1, -1)
    row_z = jnp.broadcast_to(centres[None, :, None], (GRID, GRID, NB)).reshape(1, -1)

    def one_slab(step):
        geometry = step // GRID
        slab = step % GRID
        points = lax.dynamic_index_in_dim(point_data, geometry, 0, keepdims=False)
        near = lax.dynamic_index_in_dim(lax.dynamic_index_in_dim(neighbours, geometry, 0, keepdims=False), slab, 0, keepdims=False).reshape(-1)
        valid = lax.dynamic_index_in_dim(lax.dynamic_index_in_dim(counts, geometry, 0, keepdims=False), slab, 0, keepdims=False).reshape(-1)
        picked = jnp.take(points, near, axis=1)
        row_x = (slab.astype(jnp.float32) + 0.5) / GRID
        pair = jnp.concatenate([picked[0:1] - row_x, picked[1:2] - row_y, picked[2:3] - row_z, picked[3:6]], axis=0).astype(jnp.bfloat16)
        return kernel_mean(pair, valid, kernel_in, kernel_mid, kernel_out)
    latent = lax.map(one_slab, jnp.arange(GEOMS * GRID, dtype=jnp.int32)).reshape(GEOMS, GRID, GRID, GRID, CH)
    cos_centred, sin_centred = tables(GRID, MODES, True)
    cos_third, sin_third = tables(GRID, MODES, False)
    back_cos, back_sin = third_weights(cos_third, sin_third, GRID)
    latent_wide = latent.astype(jnp.float32)
    real_part, imag_part = forward_real(latent_wide, cos_third, sin_third, 'gxyzc,kz->gxykc')
    real_part, imag_part = forward_complex(real_part, imag_part, cos_centred, sin_centred, 'gxykc,jy->gxjkc')
    real_part, imag_part = forward_complex(real_part, imag_part, cos_centred, sin_centred, 'gxjkc,ix->gijkc')
    spec_real = lax.optimization_barrier(real_part.astype(jnp.bfloat16)).astype(jnp.float32)
    spec_imag = lax.optimization_barrier(imag_part.astype(jnp.bfloat16)).astype(jnp.float32)
    mix_real = spectral[0].astype(jnp.float32)
    mix_imag = spectral[1].astype(jnp.float32)
    mixed_real = jnp.einsum('gijkc,ijkco->gijko', spec_real, mix_real) - jnp.einsum('gijkc,ijkco->gijko', spec_imag, mix_imag)
    mixed_imag = jnp.einsum('gijkc,ijkco->gijko', spec_real, mix_imag) + jnp.einsum('gijkc,ijkco->gijko', spec_imag, mix_real)
    mixed_real = lax.optimization_barrier(mixed_real.astype(jnp.bfloat16)).astype(jnp.float32)
    mixed_imag = lax.optimization_barrier(mixed_imag.astype(jnp.bfloat16)).astype(jnp.float32)
    real_part, imag_part = inverse_complex(mixed_real, mixed_imag, cos_centred, sin_centred, 'gijkc,ix->gxjkc')
    real_part, imag_part = inverse_complex(real_part, imag_part, cos_centred, sin_centred, 'gxjkc,jy->gxykc')
    branch = inverse_real(real_part, imag_part, back_cos, back_sin, 'gxykc,kz->gxyzc')
    cells_total = float(GRID ** 3)
    mean = lax.optimization_barrier(jnp.sum(branch, axis=(1, 2, 3))) / cells_total
    centred_branch = branch - mean[:, None, None, None, :]
    variance = lax.optimization_barrier(jnp.sum(centred_branch * centred_branch, axis=(1, 2, 3))) / cells_total
    skip = jnp.dot(latent.reshape(-1, CH), skip_weight, preferred_element_type=jnp.float32).reshape(GEOMS, GRID, GRID, GRID, CH)
    normed = centred_branch / jnp.sqrt(variance + NORM_FLOOR)[:, None, None, None, :]
    return jax.nn.gelu(normed + skip, approximate=True)
```

```python
import math

import jax
import jax.numpy as jnp
import numpy as np
from jax import lax
from jax.experimental import pallas as pl
from jax.experimental.pallas import tpu as pltpu
from jax.sharding import Mesh
from jax.sharding import PartitionSpec as P

f32 = jnp.float32
bf16 = jnp.bfloat16
i32 = jnp.int32

GRID = 64
NB = 32
CELLS = float(GRID**3)
NORM_FLOOR = 1.0
GZ = ("gz_0", "gz_1")
ALL = ("gx", "gy", "gz_0", "gz_1")
C0 = math.sqrt(2.0 / math.pi)
C1 = C0 * 0.044715
VMEM = pl.BlockSpec(memory_space=pltpu.VMEM)
SMEM = pl.BlockSpec(memory_space=pltpu.SMEM)


def freq(n):
    return np.where(n < 8, n, n - 16)


def angle(f, m):
    return 2.0 * math.pi * ((f * m) % GRID) / GRID


def split_two(a):
    hi = a.astype(bf16)
    lo = (a - hi.astype(a.dtype)).astype(bf16)
    return hi, lo


def third_forward():
    kh, r, kl, c = np.meshgrid(*map(np.arange, (4, 2, 4, 8)), indexing="ij")
    k, r, c = (4 * kh + kl).reshape(-1, 1), r.reshape(-1, 1), c.reshape(-1, 1)
    z = np.repeat(np.arange(64), 8)[None, :]
    cc = np.tile(np.arange(8), 64)[None, :]
    a = angle(k, z)
    v = np.where(r == 0, np.cos(a), -np.sin(a)) * (c == cc)
    return split_two(v)


def third_inverse():
    z = np.repeat(np.arange(64), 8)[:, None]
    o = np.tile(np.arange(8), 64)[:, None]
    s, kh, kl, r, oo = (
        a.reshape(1, -1) for a in np.meshgrid(*map(np.arange, (2, 4, 4, 2, 8)), indexing="ij")
    )
    k = 4 * kh + kl
    a = angle(k, z)
    w = np.where(k == 0, 1.0, 2.0) / CELLS
    cos, sin = np.cos(a), np.sin(a)
    v = np.where(s == 0, np.where(r == 0, cos, -sin), np.where(r == 0, -sin, -cos))
    return (v * w * (o == oo)).astype(bf16)


def plane_tables():
    jl, il, jh, ih = (a.reshape(-1) for a in np.meshgrid(*map(np.arange, (2, 2, 8, 8)), indexing="ij"))
    fwd = freq(2 * ih + il), freq(2 * jh + jl)
    il, jh, ih, jl = (a.reshape(-1) for a in np.meshgrid(*map(np.arange, (2, 8, 8, 2)), indexing="ij"))
    inv = freq(2 * ih + il), freq(2 * jh + jl)
    return fwd, inv, np.repeat(np.arange(8), 16), np.tile(np.arange(16), 8)


def partner_table():
    _, (fi, fj), _, _ = plane_tables()
    hit = (fi[:, None] == -fi[None, :]) & (fj[:, None] == -fj[None, :])
    return hit.astype(np.float32).astype(bf16)


def mode_masks():
    jl, il, kl = (a.reshape(-1, 1) for a in np.meshgrid(*map(np.arange, (2, 2, 4)), indexing="ij"))
    jc, ic, _, kc, _ = (
        a.reshape(1, -1) for a in np.meshgrid(*map(np.arange, (2, 2, 2, 4, 8)), indexing="ij")
    )
    own = ((jl == jc) & (il == ic) & (kl == kc)).astype(np.float32)
    _, ib, kb, _, _ = (
        a.reshape(1, -1) for a in np.meshgrid(*map(np.arange, (8, 2, 4, 2, 8)), indexing="ij")
    )
    place = ((il == ib) & (kl == kb)).astype(np.float32)
    half = np.zeros((8, 16), np.float32)
    half[jl[:, 0], np.arange(16)] = 1.0
    return own, place, half.astype(bf16)


def placing():
    ro, oh, ol = (a.reshape(-1, 1) for a in np.meshgrid(*map(np.arange, (2, 8, 8)), indexing="ij"))
    oc, _, _, rc, lc = (
        a.reshape(1, -1) for a in np.meshgrid(*map(np.arange, (8, 2, 4, 2, 8)), indexing="ij")
    )
    return ((ro == rc) & (oh == oc) & (ol == lc)).astype(np.float32).astype(bf16)


def dot(a, b):
    return jnp.dot(a, b, preferred_element_type=f32)


def dot_t(a, b):
    return lax.dot_general(a, b, (((1,), (1,)), ((), ())), preferred_element_type=f32)


def gelu_twice(v):
    return v * jnp.tanh(v * (v * v * C1 + C0)) + v


def encoder_kernel(
    place_ref, below_ref, own_ref, above_ref, nb_ref, cnt_ref, ki_ref, km_ref, ko_ref, out_ref, turn, acc_ref
):
    px, py, pz = place_ref[0], place_ref[1], place_ref[2]
    lane = lax.broadcasted_iota(i32, (8, 128), 1)
    row = lax.broadcasted_iota(i32, (8, 128), 0)
    centres = (
        ((px * 8 + (lane >> 4)).astype(f32) + 0.5) / GRID,
        ((py * 16 + (lane & 15)).astype(f32) + 0.5) / GRID,
        ((pz * 8 + row).astype(f32) + 0.5) / GRID,
    )
    counts = cnt_ref[...]
    turn[...] = jnp.zeros(turn.shape, f32)
    acc_ref[...] = jnp.zeros(acc_ref.shape, f32)
    parts = (below_ref, own_ref, above_ref)

    def gather(s):
        j = nb_ref[s]
        owner = j >> 9
        dz = (owner & 7) - pz + 1
        dy = ((owner >> 3) & 3) - py + 1
        dx = (owner >> 5) - px + 1
        chunk = ((dz * 3 + dy) * 3 + dx) * 4 + ((j >> 7) & 3)
        at = j & 127
        bits = [((chunk >> b) & 1) == 1 for b in range(7)]
        valid = counts > s
        for c in range(6):

            def pick(lo, level):
                if lo >= 108:
                    return None
                if level == 0:
                    line = jnp.broadcast_to(parts[lo // 36][lo % 36, c : c + 1, :], (8, 128))
                    return jnp.take_along_axis(line, at, axis=1, mode="promise_in_bounds")
                first = pick(lo, level - 1)
                second = pick(lo + (1 << (level - 1)), level - 1)
                return first if second is None else jnp.where(bits[level - 1], second, first)

            value = pick(0, 7)
            if c < 3:
                value = value - centres[c]
            turn[c] = jnp.where(valid, value, 0.0)
        return jnp.concatenate([turn[:, z, :] for z in range(8)], axis=1)

    def step(s, pair):
        following = gather(jnp.minimum(s + 1, NB - 1))
        hidden = gelu_twice(dot(ki_ref[...], pair.astype(bf16))).astype(bf16)
        acc_ref[...] += gelu_twice(dot(km_ref[...], hidden))
        return following

    lax.fori_loop(0, NB, step, gather(0))
    inverse = 0.5 / counts.astype(f32)
    total = acc_ref[...] * jnp.concatenate([inverse[z : z + 1, :] for z in range(8)], axis=1)
    upper = total.astype(bf16)
    lower = (total - upper.astype(f32)).astype(bf16)
    latent = dot(ko_ref[...], upper) + dot(ko_ref[...], lower)
    out_ref[...] = latent.astype(bf16).reshape(8, 8, 1024)


def forward_kernel(m_ref, ahi_ref, alo_ref, whi_ref, wlo_ref, out_ref):
    rows = [
        m_ref[s].astype(f32)[:, z * 128 : (z + 1) * 128] for s in range(8) for z in range(8)
    ]
    cells = jnp.concatenate(rows, axis=0).astype(bf16)
    z = dot(ahi_ref[...], cells) + dot(alo_ref[...], cells)
    right = []
    for kh in range(4):
        right += [z[kh * 64 + 32 : kh * 64 + 64], -z[kh * 64 : kh * 64 + 32]]
    both = jnp.concatenate([z, jnp.concatenate(right, axis=0)], axis=1).astype(bf16)
    p = dot_t(whi_ref[...], both) + dot_t(wlo_ref[...], both)
    for kh in range(4):
        for h in range(2):
            line = jnp.concatenate(
                [p[q * 64 : (q + 1) * 64, kh * 64 : (kh + 1) * 64] for q in (2 * h, 2 * h + 1)], axis=1
            )
            for jh in range(8):
                out_ref[pl.ds(((jh * 4 + kh) * 8) * 2 + h, 8, stride=2), :] = line[jh * 8 : jh * 8 + 8]


def mix_kernel(r_ref, w_ref, own_ref, sel_ref, place_ref, half_ref, out_ref):
    s = jnp.sum(r_ref[...], axis=0)
    s = s.astype(bf16).astype(f32)
    own = own_ref[...]
    g = jnp.zeros((16, 128), f32)
    for ch in range(8):
        line = jnp.concatenate([s[2 * ch : 2 * ch + 1], s[2 * ch + 1 : 2 * ch + 2]], axis=1)
        g = g + dot((line * own).astype(bf16), w_ref[ch])
    spread = dot(g.astype(bf16), sel_ref[...]) * place_ref[...]
    d = dot(half_ref[...], spread.astype(bf16))
    d = jnp.concatenate([d[0:2, oh * 128 : (oh + 1) * 128] for oh in range(8)], axis=0).astype(bf16)
    for n in range(32):
        out_ref[n] = d


def inverse_kernel(q_ref, v_ref, bc_ref, bs_ref, partner_ref, out_ref):
    blocks = []
    for kh in range(4):
        rows = jnp.concatenate([q_ref[jh, kh] for jh in range(8)], axis=0).astype(f32)
        blocks.append(jnp.concatenate([rows[:, 0:64], rows[:, 64:128]], axis=0))
    x = jnp.concatenate(blocks, axis=1)
    row = lax.broadcasted_iota(i32, (256, 256), 0)
    lane = lax.broadcasted_iota(i32, (256, 256), 1)
    x = jnp.where((row == 0) & (lane < 8), 0.0, x)
    xb = x.astype(bf16)
    twin = dot(partner_ref[...], xb[:, 0:128])
    low = lane[0:1, 0:128]
    side = jnp.where(low < 8, 0.5, jnp.where(low < 16, -0.5, 0.0))
    weight = jnp.where(lane[0:1, :] < 16, 0.5, 2.0)
    power = jnp.sum(x * x, axis=0, keepdims=True) * weight
    cross = jnp.sum(x[:, 0:128] * twin, axis=0, keepdims=True) * side
    power = jnp.broadcast_to(power[:, 0:128] + power[:, 128:256] + cross, (8, 128))
    for shift in (8, 16, 32, 64):
        power = power + pltpu.roll(power, shift, 1)
    scale = lax.rsqrt(power * (1.0 / (CELLS * CELLS)) + NORM_FLOOR)[0:1]
    scale = jnp.concatenate([scale, scale], axis=1)
    g = (dot(v_ref[...], xb) * scale).astype(bf16)
    out = dot_t(bc_ref[...], g[0:128]) + dot_t(bs_ref[...], g[128:256])
    out_ref[...] = out.astype(bf16).reshape(8, 8, 8, 128)


def output_kernel(y_ref, lat_ref, w_ref, out_ref):
    for z in range(8):
        y = jnp.concatenate([y_ref[s, z].astype(f32) for s in range(8)], axis=0)
        lat = jnp.concatenate(
            [lat_ref[s].astype(f32)[:, z * 128 : (z + 1) * 128] for s in range(8)], axis=0
        )
        both = jnp.concatenate([lat, y], axis=0).T.astype(bf16)
        v = dot(both, w_ref[...])
        out_ref[:, z, :] = 0.5 * gelu_twice(v)


def call(kernel, name, shape, dtype, *args, scratch=(), smem=0):
    return pl.pallas_call(
        kernel,
        out_shape=jax.ShapeDtypeStruct(shape, dtype),
        in_specs=[SMEM] * smem + [VMEM] * (len(args) - smem),
        out_specs=VMEM,
        scratch_shapes=list(scratch),
        compiler_params=pltpu.CompilerParams(vmem_limit_bytes=48 * 1024 * 1024),
        name=name,
    )(*args)


def beside(cells, axis):
    count = lax.axis_size(axis)
    ends = count - 1
    return (
        lax.ppermute(cells, axis, [(i, i + 1) for i in range(ends)]),
        cells,
        lax.ppermute(cells, axis, [(i + 1, i) for i in range(ends)]),
    )


def turned(cos, sin, phase):
    c, s = jnp.cos(phase), jnp.sin(phase)
    return cos * c - sin * s, sin * c + cos * s


def body(point_data, neighbours, counts, kernel_in, kernel_mid, kernel_out, spectral, skip_weight):
    gx = lax.axis_index("gx")
    gy = lax.axis_index("gy")
    gz = lax.axis_index(GZ)
    place = jnp.stack([gx, gy, gz]).astype(i32)

    own = jnp.pad(point_data[0].reshape(6, 4, 128).transpose(1, 0, 2), ((0, 0), (0, 2), (0, 0)))
    line = jnp.concatenate(beside(own, "gx"), axis=0)
    plane = jnp.concatenate(beside(line, "gy"), axis=0)
    below, same, above = beside(plane, GZ)

    near = neighbours[0].transpose(3, 2, 0, 1).reshape(NB, 8, 128)
    valid = counts[0].transpose(2, 0, 1).reshape(8, 128)
    ki = jnp.pad(kernel_in.T, ((0, 0), (0, 2)))
    km = kernel_mid.T * jnp.bfloat16(0.5)
    latent = call(
        encoder_kernel,
        "encoder",
        (8, 8, 1024),
        bf16,
        place,
        below,
        same,
        above,
        near,
        valid,
        ki,
        km,
        kernel_out.T,
        scratch=(pltpu.VMEM((8, 8, 128), f32), pltpu.VMEM((80, 1024), f32)),
        smem=1,
    )

    (ffi, ffj), (ifi, ifj), xl, yl = plane_tables()
    local = angle(1, ffi[:, None] * xl[None, :] + ffj[:, None] * yl[None, :])
    phase = ((jnp.asarray(ffi, i32) * 8 * gx + jnp.asarray(ffj, i32) * 16 * gy) % GRID).astype(f32)
    cos, sin = turned(
        np.cos(local).astype(np.float32),
        np.sin(local).astype(np.float32),
        (phase * (2.0 * math.pi / GRID))[:, None],
    )
    whi, wlo = split_two(jnp.concatenate([cos, sin], axis=1))
    local = angle(1, ifi[None, :] * xl[:, None] + ifj[None, :] * yl[:, None])
    phase = ((jnp.asarray(ifi, i32) * 8 * gx + jnp.asarray(ifj, i32) * 16 * gy) % GRID).astype(f32)
    cos, sin = turned(
        np.cos(local).astype(np.float32),
        np.sin(local).astype(np.float32),
        (phase * (2.0 * math.pi / GRID))[None, :],
    )
    back = jnp.concatenate([cos, sin], axis=0).astype(bf16)

    w = spectral.reshape(2, 2, 2, 4, 8, 8, 64).transpose(0, 4, 2, 1, 3, 5, 6)
    wr, wi = w[0], w[1]
    mixing = jnp.stack(
        [jnp.concatenate([wr, wi], axis=-1), jnp.concatenate([-wi, wr], axis=-1)], axis=3
    ).reshape(8, 256, 128)
    joint = jnp.concatenate([skip_weight, jnp.eye(64, dtype=bf16)], axis=0)

    depth = lax.all_to_all(latent, GZ, split_axis=0, concat_axis=0)
    ahi, alo = third_forward()
    partial = call(forward_kernel, "forward", (512, 128), f32, depth, ahi, alo, whi, wlo)
    partial = lax.all_to_all(partial.reshape(256, 2, 128), ALL, split_axis=0, concat_axis=0)
    own_mask, place_mask, half = mode_masks()
    mixed = call(
        mix_kernel,
        "mix",
        (32, 16, 128),
        bf16,
        partial.reshape(32, 16, 128),
        mixing,
        own_mask,
        placing(),
        place_mask,
        half,
    )
    mixed = lax.all_to_all(mixed.reshape(256, 2, 128), ALL, split_axis=0, concat_axis=0)
    third = third_inverse()
    branch = call(
        inverse_kernel,
        "inverse",
        (8, 8, 8, 128),
        bf16,
        mixed.reshape(8, 4, 16, 128),
        back,
        third[:, :256],
        third[:, 256:],
        partner_table(),
    )
    branch = lax.all_to_all(branch, GZ, split_axis=0, concat_axis=0)
    out = call(output_kernel, "output", (128, 8, 64), f32, branch, latent, joint)
    return out.reshape(1, 8, 16, 8, 64)


def solution(mesh):
    split = Mesh(
        mesh.devices.reshape(mesh.shape["gx"], mesh.shape["gy"], 4, 2), ("gx", "gy", "gz_0", "gz_1")
    )
    return jax.shard_map(
        body,
        mesh=split,
        in_specs=(
            P(None, None, ALL),
            P(None, "gx", "gy", GZ, None),
            P(None, "gx", "gy", GZ),
            P(),
            P(),
            P(),
            P(None, GZ, "gx", "gy", None, None),
            P(),
        ),
        out_specs=P(None, "gx", "gy", GZ, None),
        check_vma=False,
    )
```

```python
import math

import jax
import jax.numpy as jnp
import numpy as np
from jax import lax
from jax.experimental import pallas as pl
from jax.experimental.pallas import tpu as pltpu
from jax.sharding import Mesh
from jax.sharding import PartitionSpec as P

f32 = jnp.float32
bf16 = jnp.bfloat16
i32 = jnp.int32

GRID = 64
NB = 32
CELLS = float(GRID**3)
NORM_FLOOR = 1.0
GZ = ("gz_0", "gz_1")
ALL = ("gx", "gy", "gz_0", "gz_1")
C0 = math.sqrt(2.0 / math.pi)
C1 = C0 * 0.044715
VMEM = pl.BlockSpec(memory_space=pltpu.VMEM)
SMEM = pl.BlockSpec(memory_space=pltpu.SMEM)


def freq(n):
    return np.where(n < 8, n, n - 16)


def angle(f, m):
    return 2.0 * math.pi * ((f * m) % GRID) / GRID


def split_two(a):
    hi = a.astype(bf16)
    lo = (a - hi.astype(a.dtype)).astype(bf16)
    return hi, lo


def third_forward():
    kh, r, kl, c = np.meshgrid(*map(np.arange, (4, 2, 4, 8)), indexing="ij")
    k, r, c = (4 * kh + kl).reshape(-1, 1), r.reshape(-1, 1), c.reshape(-1, 1)
    z = np.repeat(np.arange(64), 8)[None, :]
    cc = np.tile(np.arange(8), 64)[None, :]
    a = angle(k, z)
    v = np.where(r == 0, np.cos(a), -np.sin(a)) * (c == cc)
    return split_two(v)


def third_inverse():
    z = np.repeat(np.arange(64), 8)[:, None]
    o = np.tile(np.arange(8), 64)[:, None]
    s, kh, kl, r, oo = (
        a.reshape(1, -1) for a in np.meshgrid(*map(np.arange, (2, 4, 4, 2, 8)), indexing="ij")
    )
    k = 4 * kh + kl
    a = angle(k, z)
    w = np.where(k == 0, 1.0, 2.0) / CELLS
    cos, sin = np.cos(a), np.sin(a)
    v = np.where(s == 0, np.where(r == 0, cos, -sin), np.where(r == 0, -sin, -cos))
    return (v * w * (o == oo)).astype(bf16)


def plane_tables():
    jl, il, jh, ih = (a.reshape(-1) for a in np.meshgrid(*map(np.arange, (2, 2, 8, 8)), indexing="ij"))
    fwd = freq(2 * ih + il), freq(2 * jh + jl)
    il, jh, ih, jl = (a.reshape(-1) for a in np.meshgrid(*map(np.arange, (2, 8, 8, 2)), indexing="ij"))
    inv = freq(2 * ih + il), freq(2 * jh + jl)
    return fwd, inv, np.repeat(np.arange(8), 16), np.tile(np.arange(16), 8)


def partner_table():
    _, (fi, fj), _, _ = plane_tables()
    hit = (fi[:, None] == -fi[None, :]) & (fj[:, None] == -fj[None, :])
    return hit.astype(np.float32).astype(bf16)


def mode_masks():
    jl, il, kl = (a.reshape(-1, 1) for a in np.meshgrid(*map(np.arange, (2, 2, 4)), indexing="ij"))
    jc, ic, _, kc, _ = (
        a.reshape(1, -1) for a in np.meshgrid(*map(np.arange, (2, 2, 2, 4, 8)), indexing="ij")
    )
    own = ((jl == jc) & (il == ic) & (kl == kc)).astype(np.float32)
    _, ib, kb, _, _ = (
        a.reshape(1, -1) for a in np.meshgrid(*map(np.arange, (8, 2, 4, 2, 8)), indexing="ij")
    )
    place = ((il == ib) & (kl == kb)).astype(np.float32)
    half = np.zeros((8, 16), np.float32)
    half[jl[:, 0], np.arange(16)] = 1.0
    return own, place, half.astype(bf16)


def placing():
    ro, oh, ol = (a.reshape(-1, 1) for a in np.meshgrid(*map(np.arange, (2, 8, 8)), indexing="ij"))
    oc, _, _, rc, lc = (
        a.reshape(1, -1) for a in np.meshgrid(*map(np.arange, (8, 2, 4, 2, 8)), indexing="ij")
    )
    return ((ro == rc) & (oh == oc) & (ol == lc)).astype(np.float32).astype(bf16)


def dot(a, b):
    return jnp.dot(a, b, preferred_element_type=f32)


def dot_t(a, b):
    return lax.dot_general(a, b, (((1,), (1,)), ((), ())), preferred_element_type=f32)


def gelu_twice(v):
    return v * jnp.tanh(v * (v * v * C1 + C0)) + v


def column(line):
    return jnp.broadcast_to(line, (128, 128)).T


def rank_rows(rank, first, count):
    r = lax.broadcasted_iota(i32, (count, 1024), 0) + first
    return jnp.where(r == rank, 1.0, 0.0).astype(bf16)


def sort_kernel(place_ref, nb_ref, cnt_ref, code_ref, cnt8_ref, cen_ref, rank_ref, scnt_ref, steps_ref):
    px, py, pz = place_ref[0], place_ref[1], place_ref[2]
    j = nb_ref[...]
    owner = j >> 9
    dz = (owner & 7) - pz + 1
    dy = ((owner >> 3) & 3) - py + 1
    dx = (owner >> 5) - px + 1
    chunk = (((dz * 3 + dy) * 3 + dx) * 4 + ((j >> 7) & 3)) & 127
    chunk = chunk.astype(f32)
    lane = (j & 127).astype(f32)
    counts = cnt_ref[...].astype(f32)
    row8 = lax.broadcasted_iota(i32, (8, 128), 0)
    lane8 = lax.broadcasted_iota(i32, (8, 128), 1)
    key = counts * 1024.0 - (row8 * 128 + lane8).astype(f32)
    flat = [key[z : z + 1] for z in range(8)]
    ranks = [jnp.zeros((128, 128), f32) for _ in range(8)]
    for z in range(8):
        own = column(flat[z])
        ranks = [r + jnp.where(own > line, 1.0, 0.0) for r, line in zip(ranks, flat)]
    rank = jnp.concatenate([jnp.sum(r, axis=0, keepdims=True) for r in ranks], axis=1).astype(i32)
    rank_ref[...] = jnp.broadcast_to(rank, (8, 1024))
    flat = [
        jnp.concatenate([a[:, z, :] for z in range(8)], axis=1) for a in (chunk, lane)
    ]
    node = lax.broadcasted_iota(i32, (8, 1024), 1)
    wide = lax.broadcasted_iota(i32, (8, 1024), 0)
    line = jnp.concatenate([counts[z : z + 1] for z in range(8)], axis=1)
    tail = jnp.where(
        wide == 0,
        line,
        jnp.where(wide == 1, (node >> 7).astype(f32), (node & 127).astype(f32)),
    )
    rows = jnp.concatenate(flat + [tail], axis=0).astype(bf16)
    odd = (row8 & 1) == 1
    for t in range(4):
        found = dot_t(rows, rank_rows(rank, t * 256, 256))
        code = (found[0:32] * 128.0 + found[32:64]).astype(i32)
        for s in range(4):
            for h in range(2):
                code_ref[t, pl.ds(s * 16 + h, 8, stride=2), :] = code[
                    s * 8 : s * 8 + 8, h * 128 : h * 128 + 128
                ]
        tail = found[64:72]

        def both(n):
            return jnp.where(odd, tail[n : n + 1, 128:256], tail[n : n + 1, 0:128])

        cnt8_ref[t] = both(0).astype(i32)
        cell = both(2).astype(i32)
        cen_ref[t, 0] = ((px * 8 + (cell >> 4)).astype(f32) + 0.5) / GRID
        cen_ref[t, 1] = ((py * 16 + (cell & 15)).astype(f32) + 0.5) / GRID
        cen_ref[t, 2] = ((pz * 8).astype(f32) + both(1) + 0.5) / GRID
        scnt_ref[:, t * 256 : t * 256 + 256] = jnp.broadcast_to(tail[0:1], (8, 256))
        steps_ref[t] = (jnp.max(tail[0:1]).astype(i32) + 3) >> 2


def encoder_kernel(
    steps_ref,
    below_ref,
    own_ref,
    above_ref,
    code_ref,
    cnt8_ref,
    cen_ref,
    rank_ref,
    scnt_ref,
    ki_ref,
    km_ref,
    ko_ref,
    out_ref,
    words,
    off_ref,
    turn,
    acc_ref,
):
    parts = (below_ref, own_ref, above_ref)
    most = jnp.zeros((8, 128), f32)
    for part in parts:
        most = jnp.maximum(most, jnp.max(jnp.abs(part[...]), axis=0))
    most = jnp.maximum(jnp.max(most, axis=1, keepdims=True), 1e-30)
    scale = jnp.broadcast_to(32767.0 / most, (8, 128))
    unit = jnp.broadcast_to(most * (1.0 / 32767.0), (8, 128))
    for n in range(108):
        q = (parts[n // 36][n % 36] * scale + 32768.5).astype(i32)
        words[n] = (q << 16) | pltpu.roll(q, 5, 0)
    units = [jnp.broadcast_to(unit[c : c + 1], (8, 128)) for c in range(6)]
    for t in range(4):
        for c in range(3):
            off_ref[t, c] = cen_ref[t, c] + 32768.0 * units[c]
    turn[...] = jnp.zeros(turn.shape, f32)
    acc_ref[...] = jnp.zeros(acc_ref.shape, f32)
    slot = lax.broadcasted_iota(i32, (8, 128), 0) >> 1

    def gather(t, b):
        code = code_ref[t, pl.ds(pl.multiple_of(b * 8, 8), 8), :]
        at = code & 127
        bits = [(code & (128 << n)) != 0 for n in range(7)]
        valid = cnt8_ref[t] > slot + b * 4
        for c in range(3):

            def pick(lo, level):
                if lo >= 108:
                    return None
                if level == 0:
                    line = jnp.broadcast_to(words[lo, c : c + 1, :], (8, 128))
                    return jnp.take_along_axis(line, at, axis=1, mode="promise_in_bounds")
                first = pick(lo, level - 1)
                second = pick(lo + (1 << (level - 1)), level - 1)
                return first if second is None else jnp.where(bits[level - 1], second, first)

            word = pick(0, 7)
            place = lax.shift_right_logical(word, 16).astype(f32) * units[c] - off_ref[t, c]
            normal = ((word & 65535) - 32768).astype(f32) * units[c + 3]
            turn[c] = jnp.where(valid, place, 0.0)
            turn[c + 3] = jnp.where(valid, normal, 0.0)
        return jnp.concatenate([turn[:, n, :] for n in range(8)], axis=1)

    def step(_, carry):
        t, b, pair = carry
        last = b + 1 >= steps_ref[t]
        nt = jnp.where(last, jnp.minimum(t + 1, 3), t)
        nb = jnp.where(last, 0, b + 1)
        following = gather(nt, nb)
        hidden = gelu_twice(dot(ki_ref[...], pair.astype(bf16))).astype(bf16)
        hidden = gelu_twice(dot(km_ref[...], hidden))
        acc_ref[t] += (
            hidden[:, 0:256] + hidden[:, 256:512] + hidden[:, 512:768] + hidden[:, 768:1024]
        )
        return nt, nb, following

    total = steps_ref[0] + steps_ref[1] + steps_ref[2] + steps_ref[3]
    lax.fori_loop(0, total, step, (jnp.int32(0), jnp.int32(0), gather(0, 0)))
    mean = jnp.concatenate([acc_ref[t] for t in range(4)], axis=1) * (0.5 / scnt_ref[0:1])
    upper = mean.astype(bf16)
    lower = (mean - upper.astype(f32)).astype(bf16)
    latent = (dot(ko_ref[...], upper) + dot(ko_ref[...], lower)).astype(bf16)
    rank = rank_ref[0:1]
    spread = jnp.zeros((64, 1024), f32)
    for t in range(4):
        spread = spread + dot(latent[:, t * 256 : t * 256 + 256], rank_rows(rank, t * 256, 256))
    out_ref[...] = spread.astype(bf16).reshape(8, 8, 1024)


def forward_kernel(m_ref, ahi_ref, alo_ref, whi_ref, wlo_ref, out_ref, wide):
    rows = [
        m_ref[s].astype(f32)[:, z * 128 : (z + 1) * 128] for s in range(8) for z in range(8)
    ]
    cells = jnp.concatenate(rows, axis=0).astype(bf16)
    z = dot(ahi_ref[...], cells) + dot(alo_ref[...], cells)
    right = []
    for kh in range(4):
        right += [z[kh * 64 + 32 : kh * 64 + 64], -z[kh * 64 : kh * 64 + 32]]
    both = jnp.concatenate([z, jnp.concatenate(right, axis=0)], axis=1).astype(bf16)
    p = dot_t(whi_ref[...], both) + dot_t(wlo_ref[...], both)
    for kh in range(4):
        for h in range(2):
            line = jnp.concatenate(
                [p[q * 64 : (q + 1) * 64, kh * 64 : (kh + 1) * 64] for q in (2 * h, 2 * h + 1)], axis=1
            )
            for jh in range(8):
                wide[pl.ds(((jh * 4 + kh) * 8) * 2 + h, 8, stride=2), :] = line[jh * 8 : jh * 8 + 8]
    out_ref[...] = wide[...].astype(bf16)


def mix_kernel(r_ref, w_ref, own_ref, sel_ref, place_ref, half_ref, out_ref):
    s = jnp.sum(r_ref[...].astype(f32), axis=0)
    s = s.astype(bf16).astype(f32)
    own = own_ref[...]
    g = jnp.zeros((16, 128), f32)
    for ch in range(8):
        line = jnp.concatenate([s[2 * ch : 2 * ch + 1], s[2 * ch + 1 : 2 * ch + 2]], axis=1)
        g = g + dot((line * own).astype(bf16), w_ref[ch])
    spread = dot(g.astype(bf16), sel_ref[...]) * place_ref[...]
    d = dot(half_ref[...], spread.astype(bf16))
    d = jnp.concatenate([d[0:2, oh * 128 : (oh + 1) * 128] for oh in range(8)], axis=0).astype(bf16)
    for n in range(32):
        out_ref[n] = d


def inverse_kernel(q_ref, v_ref, bc_ref, bs_ref, partner_ref, out_ref):
    blocks = []
    for kh in range(4):
        rows = jnp.concatenate([q_ref[jh, kh] for jh in range(8)], axis=0).astype(f32)
        blocks.append(jnp.concatenate([rows[:, 0:64], rows[:, 64:128]], axis=0))
    x = jnp.concatenate(blocks, axis=1)
    row = lax.broadcasted_iota(i32, (256, 256), 0)
    lane = lax.broadcasted_iota(i32, (256, 256), 1)
    x = jnp.where((row == 0) & (lane < 8), 0.0, x)
    xb = x.astype(bf16)
    twin = dot(partner_ref[...], xb[:, 0:128])
    low = lane[0:1, 0:128]
    side = jnp.where(low < 8, 0.5, jnp.where(low < 16, -0.5, 0.0))
    weight = jnp.where(lane[0:1, :] < 16, 0.5, 2.0)
    power = jnp.sum(x * x, axis=0, keepdims=True) * weight
    cross = jnp.sum(x[:, 0:128] * twin, axis=0, keepdims=True) * side
    power = jnp.broadcast_to(power[:, 0:128] + power[:, 128:256] + cross, (8, 128))
    for shift in (8, 16, 32, 64):
        power = power + pltpu.roll(power, shift, 1)
    scale = lax.rsqrt(power * (1.0 / (CELLS * CELLS)) + NORM_FLOOR)[0:1]
    scale = jnp.concatenate([scale, scale], axis=1)
    g = (dot(v_ref[...], xb) * scale).astype(bf16)
    out = dot_t(bc_ref[...], g[0:128]) + dot_t(bs_ref[...], g[128:256])
    out_ref[...] = out.astype(bf16).reshape(8, 8, 8, 128)


def output_kernel(y_ref, lat_ref, w_ref, out_ref):
    for z in range(8):
        y = jnp.concatenate([y_ref[s, z].astype(f32) for s in range(8)], axis=0)
        lat = jnp.concatenate(
            [lat_ref[s].astype(f32)[:, z * 128 : (z + 1) * 128] for s in range(8)], axis=0
        )
        both = jnp.concatenate([lat, y], axis=0).T.astype(bf16)
        v = dot(both, w_ref[...])
        out_ref[:, z, :] = 0.5 * gelu_twice(v)


def call(kernel, name, shape, dtype, *args, scratch=(), smem=0):
    return pl.pallas_call(
        kernel,
        out_shape=jax.ShapeDtypeStruct(shape, dtype),
        in_specs=[SMEM] * smem + [VMEM] * (len(args) - smem),
        out_specs=VMEM,
        scratch_shapes=list(scratch),
        compiler_params=pltpu.CompilerParams(vmem_limit_bytes=48 * 1024 * 1024),
        name=name,
    )(*args)


def sorted_nodes(place, near, valid):
    shapes = (
        ((4, 64, 128), i32),
        ((4, 8, 128), i32),
        ((4, 3, 8, 128), f32),
        ((8, 1024), i32),
        ((8, 1024), f32),
        ((4,), i32),
    )
    return pl.pallas_call(
        sort_kernel,
        out_shape=[jax.ShapeDtypeStruct(*s) for s in shapes],
        in_specs=[SMEM, VMEM, VMEM],
        out_specs=[VMEM] * 5 + [SMEM],
        compiler_params=pltpu.CompilerParams(vmem_limit_bytes=48 * 1024 * 1024),
        name="sort",
    )(place, near, valid)


def encode(steps, tables, pieces, ki, km, ko):
    return call(
        encoder_kernel,
        "encoder",
        (8, 8, 1024),
        bf16,
        steps,
        *pieces,
        *tables,
        ki,
        km,
        ko,
        scratch=(
            pltpu.VMEM((108, 8, 128), i32),
            pltpu.VMEM((4, 3, 8, 128), f32),
            pltpu.VMEM((8, 8, 128), f32),
            pltpu.VMEM((4, 80, 256), f32),
        ),
        smem=1,
    )


def beside(cells, axis):
    count = lax.axis_size(axis)
    ends = count - 1
    return (
        lax.ppermute(cells, axis, [(i, i + 1) for i in range(ends)]),
        cells,
        lax.ppermute(cells, axis, [(i + 1, i) for i in range(ends)]),
    )


def turned(cos, sin, phase):
    c, s = jnp.cos(phase), jnp.sin(phase)
    return cos * c - sin * s, sin * c + cos * s


def body(point_data, neighbours, counts, kernel_in, kernel_mid, kernel_out, spectral, skip_weight):
    gx = lax.axis_index("gx")
    gy = lax.axis_index("gy")
    gz = lax.axis_index(GZ)
    place = jnp.stack([gx, gy, gz]).astype(i32)

    own = jnp.pad(point_data[0].reshape(6, 4, 128).transpose(1, 0, 2), ((0, 0), (0, 2), (0, 0)))
    line = jnp.concatenate(beside(own, "gx"), axis=0)
    plane = jnp.concatenate(beside(line, "gy"), axis=0)
    below, same, above = beside(plane, GZ)

    near = neighbours[0].transpose(3, 2, 0, 1).reshape(NB, 8, 128)
    valid = counts[0].transpose(2, 0, 1).reshape(8, 128)
    ki = jnp.pad(kernel_in.T, ((0, 0), (0, 2)))
    km = kernel_mid.T * jnp.bfloat16(0.5)
    *tables, steps = sorted_nodes(place, near, valid)
    latent = encode(steps, tables, (below, same, above), ki, km, kernel_out.T)

    (ffi, ffj), (ifi, ifj), xl, yl = plane_tables()
    local = angle(1, ffi[:, None] * xl[None, :] + ffj[:, None] * yl[None, :])
    phase = ((jnp.asarray(ffi, i32) * 8 * gx + jnp.asarray(ffj, i32) * 16 * gy) % GRID).astype(f32)
    cos, sin = turned(
        np.cos(local).astype(np.float32),
        np.sin(local).astype(np.float32),
        (phase * (2.0 * math.pi / GRID))[:, None],
    )
    whi, wlo = split_two(jnp.concatenate([cos, sin], axis=1))
    local = angle(1, ifi[None, :] * xl[:, None] + ifj[None, :] * yl[:, None])
    phase = ((jnp.asarray(ifi, i32) * 8 * gx + jnp.asarray(ifj, i32) * 16 * gy) % GRID).astype(f32)
    cos, sin = turned(
        np.cos(local).astype(np.float32),
        np.sin(local).astype(np.float32),
        (phase * (2.0 * math.pi / GRID))[None, :],
    )
    back = jnp.concatenate([cos, sin], axis=0).astype(bf16)

    w = spectral.reshape(2, 2, 2, 4, 8, 8, 64).transpose(0, 4, 2, 1, 3, 5, 6)
    wr, wi = w[0], w[1]
    mixing = jnp.stack(
        [jnp.concatenate([wr, wi], axis=-1), jnp.concatenate([-wi, wr], axis=-1)], axis=3
    ).reshape(8, 256, 128)
    joint = jnp.concatenate([skip_weight, jnp.eye(64, dtype=bf16)], axis=0)

    depth = lax.all_to_all(latent, GZ, split_axis=0, concat_axis=0)
    ahi, alo = third_forward()
    partial = call(forward_kernel, "forward", (512, 128), bf16, depth, ahi, alo, whi, wlo, scratch=(pltpu.VMEM((512, 128), f32),))
    partial = lax.all_to_all(partial.reshape(256, 2, 128), ALL, split_axis=0, concat_axis=0)
    own_mask, place_mask, half = mode_masks()
    mixed = call(
        mix_kernel,
        "mix",
        (32, 16, 128),
        bf16,
        partial.reshape(32, 16, 128),
        mixing,
        own_mask,
        placing(),
        place_mask,
        half,
    )
    mixed = lax.all_to_all(mixed.reshape(256, 2, 128), ALL, split_axis=0, concat_axis=0)
    third = third_inverse()
    branch = call(
        inverse_kernel,
        "inverse",
        (8, 8, 8, 128),
        bf16,
        mixed.reshape(8, 4, 16, 128),
        back,
        third[:, :256],
        third[:, 256:],
        partner_table(),
    )
    branch = lax.all_to_all(branch, GZ, split_axis=0, concat_axis=0)
    out = call(output_kernel, "output", (128, 8, 64), f32, branch, latent, joint)
    return out.reshape(1, 8, 16, 8, 64)


def solution(mesh):
    split = Mesh(
        mesh.devices.reshape(mesh.shape["gx"], mesh.shape["gy"], 4, 2), ("gx", "gy", "gz_0", "gz_1")
    )
    return jax.shard_map(
        body,
        mesh=split,
        in_specs=(
            P(None, None, ALL),
            P(None, "gx", "gy", GZ, None),
            P(None, "gx", "gy", GZ),
            P(),
            P(),
            P(),
            P(None, GZ, "gx", "gy", None, None),
            P(),
        ),
        out_specs=P(None, "gx", "gy", GZ, None),
        check_vma=False,
    )
```

```python
import math

import jax
import jax.numpy as jnp
import numpy as np
from jax import lax
from jax.experimental import pallas as pl
from jax.experimental.pallas import tpu as pltpu
from jax.sharding import Mesh
from jax.sharding import PartitionSpec as P

f32 = jnp.float32
bf16 = jnp.bfloat16
i32 = jnp.int32

GRID = 64
NB = 32
NEAR_EARLY = True
CELLS = float(GRID**3)
NORM_FLOOR = 1.0
GZ = ("gz_0", "gz_1")
ALL = ("gx", "gy", "gz_0", "gz_1")
C0 = math.sqrt(2.0 / math.pi)
C1 = C0 * 0.044715
VMEM = pl.BlockSpec(memory_space=pltpu.VMEM)
SMEM = pl.BlockSpec(memory_space=pltpu.SMEM)


def freq(n):
    return np.where(n < 8, n, n - 16)


def angle(f, m):
    return 2.0 * math.pi * ((f * m) % GRID) / GRID


def split_two(a):
    hi = a.astype(bf16)
    lo = (a - hi.astype(a.dtype)).astype(bf16)
    return hi, lo


def third_forward():
    kh, r, kl, c = np.meshgrid(*map(np.arange, (4, 2, 4, 8)), indexing="ij")
    k, r, c = (4 * kh + kl).reshape(-1, 1), r.reshape(-1, 1), c.reshape(-1, 1)
    z = np.repeat(np.arange(64), 8)[None, :]
    cc = np.tile(np.arange(8), 64)[None, :]
    a = angle(k, z)
    v = np.where(r == 0, np.cos(a), -np.sin(a)) * (c == cc)
    return split_two(v)


def third_inverse():
    z = np.repeat(np.arange(64), 8)[:, None]
    o = np.tile(np.arange(8), 64)[:, None]
    s, kh, kl, r, oo = (
        a.reshape(1, -1) for a in np.meshgrid(*map(np.arange, (2, 4, 4, 2, 8)), indexing="ij")
    )
    k = 4 * kh + kl
    a = angle(k, z)
    w = np.where(k == 0, 1.0, 2.0) / CELLS
    cos, sin = np.cos(a), np.sin(a)
    v = np.where(s == 0, np.where(r == 0, cos, -sin), np.where(r == 0, -sin, -cos))
    return (v * w * (o == oo)).astype(bf16)


def plane_tables():
    jl, il, jh, ih = (a.reshape(-1) for a in np.meshgrid(*map(np.arange, (2, 2, 8, 8)), indexing="ij"))
    fwd = freq(2 * ih + il), freq(2 * jh + jl)
    il, jh, ih, jl = (a.reshape(-1) for a in np.meshgrid(*map(np.arange, (2, 8, 8, 2)), indexing="ij"))
    inv = freq(2 * ih + il), freq(2 * jh + jl)
    return fwd, inv, np.repeat(np.arange(8), 16), np.tile(np.arange(16), 8)


def partner_table():
    _, (fi, fj), _, _ = plane_tables()
    hit = (fi[:, None] == -fi[None, :]) & (fj[:, None] == -fj[None, :])
    return hit.astype(np.float32).astype(bf16)


def mode_masks():
    jl, il, kl = (a.reshape(-1, 1) for a in np.meshgrid(*map(np.arange, (2, 2, 4)), indexing="ij"))
    jc, ic, _, kc, _ = (
        a.reshape(1, -1) for a in np.meshgrid(*map(np.arange, (2, 2, 2, 4, 8)), indexing="ij")
    )
    own = ((jl == jc) & (il == ic) & (kl == kc)).astype(np.float32)
    _, ib, kb, _, _ = (
        a.reshape(1, -1) for a in np.meshgrid(*map(np.arange, (8, 2, 4, 2, 8)), indexing="ij")
    )
    place = ((il == ib) & (kl == kb)).astype(np.float32)
    half = np.zeros((8, 16), np.float32)
    half[jl[:, 0], np.arange(16)] = 1.0
    return own, place, half.astype(bf16)


def placing():
    ro, oh, ol = (a.reshape(-1, 1) for a in np.meshgrid(*map(np.arange, (2, 8, 8)), indexing="ij"))
    oc, _, _, rc, lc = (
        a.reshape(1, -1) for a in np.meshgrid(*map(np.arange, (8, 2, 4, 2, 8)), indexing="ij")
    )
    return ((ro == rc) & (oh == oc) & (ol == lc)).astype(np.float32).astype(bf16)


def dot(a, b):
    return jnp.dot(a, b, preferred_element_type=f32)


def dot_t(a, b):
    return lax.dot_general(a, b, (((1,), (1,)), ((), ())), preferred_element_type=f32)


def gelu_twice(v):
    return v * jnp.tanh(v * (v * v * C1 + C0)) + v


def column(line):
    return jnp.broadcast_to(line, (128, 128)).T


def rank_rows(rank, first, count):
    r = lax.broadcasted_iota(i32, (count, 1024), 0) + first
    return jnp.where(r == rank, 1.0, 0.0).astype(bf16)


def sort_kernel(
    place_ref, nb_ref, cnt_ref, far_ref, near_ref, far8_ref, near8_ref, cen_ref, rank_ref, scnt_ref, steps_ref, lists
):
    px, py, pz = place_ref[0], place_ref[1], place_ref[2]
    me = (px * 4 + py) * 8 + pz
    counts = cnt_ref[...]
    nothing = jnp.full((8, 128), -1, i32)
    far = jnp.zeros((8, 128), i32)
    near = jnp.zeros((8, 128), i32)
    codes, far_at, near_at = [], [], []
    for s in range(NB):
        j = nb_ref[s]
        owner = j >> 9
        dz = (owner & 7) - pz + 1
        dy = ((owner >> 3) & 3) - py + 1
        dx = (owner >> 5) - px + 1
        chunk = (((dz * 3 + dy) * 3 + dx) * 4 + ((j >> 7) & 3)) & 127
        codes.append(chunk * 128 + (j & 127))
        valid = counts > s
        mine = owner == me
        is_far = valid & jnp.logical_not(mine)
        is_near = valid & mine
        far_at.append(jnp.where(is_far, far, nothing))
        near_at.append(jnp.where(is_near, near, nothing))
        far = far + is_far.astype(i32)
        near = near + is_near.astype(i32)
    for p in range(NB):
        first = jnp.zeros((8, 128), i32)
        second = jnp.zeros((8, 128), i32)
        for s in range(p, NB):
            first = jnp.where(far_at[s] == p, codes[s], first)
            second = jnp.where(near_at[s] == p, codes[s], second)
        lists[p] = (first >> 7).astype(f32)
        lists[NB + p] = (first & 127).astype(f32)
        lists[2 * NB + p] = ((second >> 7) & 3).astype(f32)
        lists[3 * NB + p] = (second & 127).astype(f32)
    far, near = far.astype(f32), near.astype(f32)
    row8 = lax.broadcasted_iota(i32, (8, 128), 0)
    lane8 = lax.broadcasted_iota(i32, (8, 128), 1)
    key = far * 1024.0 - (row8 * 128 + lane8).astype(f32)
    flat = [key[z : z + 1] for z in range(8)]
    ranks = [jnp.zeros((128, 128), f32) for _ in range(8)]
    for z in range(8):
        own = column(flat[z])
        ranks = [r + jnp.where(own > line, 1.0, 0.0) for r, line in zip(ranks, flat)]
    rank = jnp.concatenate([jnp.sum(r, axis=0, keepdims=True) for r in ranks], axis=1).astype(i32)
    rank_ref[...] = jnp.broadcast_to(rank, (8, 1024))
    node = lax.broadcasted_iota(i32, (8, 1024), 1)
    wide = lax.broadcasted_iota(i32, (8, 1024), 0)
    far = jnp.concatenate([far[z : z + 1] for z in range(8)], axis=1)
    near = jnp.concatenate([near[z : z + 1] for z in range(8)], axis=1)
    tail = jnp.where(wide == 2, (node >> 7).astype(f32), (node & 127).astype(f32))
    tail = jnp.where(wide == 0, far, jnp.where(wide == 1, near, tail))
    rows = jnp.concatenate([lists[:, z, :] for z in range(8)], axis=1)
    rows = jnp.concatenate([rows, tail], axis=0).astype(bf16)
    odd = (row8 & 1) == 1
    for t in range(4):
        found = dot_t(rows, rank_rows(rank, t * 256, 256))
        for ref, at in ((far_ref, 0), (near_ref, 2 * NB)):
            code = (found[at : at + 32] * 128.0 + found[at + 32 : at + 64]).astype(i32)
            for s in range(4):
                for h in range(2):
                    ref[t, pl.ds(s * 16 + h, 8, stride=2), :] = code[
                        s * 8 : s * 8 + 8, h * 128 : h * 128 + 128
                    ]
        tail = found[4 * NB : 4 * NB + 8]

        def both(n):
            return jnp.where(odd, tail[n : n + 1, 128:256], tail[n : n + 1, 0:128])

        far8_ref[t] = both(0).astype(i32)
        near8_ref[t] = both(1).astype(i32)
        cell = both(3).astype(i32)
        cen_ref[t, 0] = ((px * 8 + (cell >> 4)).astype(f32) + 0.5) / GRID
        cen_ref[t, 1] = ((py * 16 + (cell & 15)).astype(f32) + 0.5) / GRID
        cen_ref[t, 2] = ((pz * 8).astype(f32) + both(2) + 0.5) / GRID
        scnt_ref[:, t * 256 : t * 256 + 256] = jnp.broadcast_to(tail[0:1] + tail[1:2], (8, 256))
        steps_ref[t] = jnp.maximum((jnp.max(tail[0:1]).astype(i32) + 3) >> 2, 1)
        steps_ref[4 + t] = jnp.maximum((jnp.max(tail[1:2]).astype(i32) + 3) >> 2, 1)


def pair_sums(steps_ref, at, gather, ki_ref, km_ref, acc_ref):
    def step(_, carry):
        t, b, pair = carry
        last = b + 1 >= steps_ref[at + t]
        nt = jnp.where(last, jnp.minimum(t + 1, 3), t)
        nb = jnp.where(last, 0, b + 1)
        following = gather(nt, nb)
        hidden = gelu_twice(dot(ki_ref[...], pair.astype(bf16))).astype(bf16)
        hidden = gelu_twice(dot(km_ref[...], hidden))
        acc_ref[t] += (
            hidden[:, 0:256] + hidden[:, 256:512] + hidden[:, 512:768] + hidden[:, 768:1024]
        )
        return nt, nb, following

    total = steps_ref[at] + steps_ref[at + 1] + steps_ref[at + 2] + steps_ref[at + 3]
    lax.fori_loop(0, total, step, (jnp.int32(0), jnp.int32(0), gather(0, 0)))


def near_kernel(steps_ref, own_ref, code_ref, cnt8_ref, cen_ref, ki_ref, km_ref, acc_ref, turn):
    turn[...] = jnp.zeros(turn.shape, f32)
    acc_ref[...] = jnp.zeros(acc_ref.shape, f32)
    slot = lax.broadcasted_iota(i32, (8, 128), 0) >> 1

    def gather(t, b):
        code = code_ref[t, pl.ds(pl.multiple_of(b * 8, 8), 8), :]
        at = code & 127
        low, high = (code & 128) != 0, (code & 256) != 0
        valid = cnt8_ref[t] > slot + b * 4
        for c in range(6):
            found = [
                jnp.take_along_axis(
                    jnp.broadcast_to(own_ref[n, c : c + 1, :], (8, 128)), at, axis=1, mode="promise_in_bounds"
                )
                for n in range(4)
            ]
            value = jnp.where(
                high, jnp.where(low, found[3], found[2]), jnp.where(low, found[1], found[0])
            )
            if c < 3:
                value = value - cen_ref[t, c]
            turn[c] = jnp.where(valid, value, 0.0)
        return jnp.concatenate([turn[:, n, :] for n in range(8)], axis=1)

    pair_sums(steps_ref, 4, gather, ki_ref, km_ref, acc_ref)


def encoder_kernel(
    steps_ref,
    below_ref,
    own_ref,
    above_ref,
    code_ref,
    cnt8_ref,
    cen_ref,
    rank_ref,
    scnt_ref,
    sum_ref,
    ki_ref,
    km_ref,
    ko_ref,
    out_ref,
    words,
    off_ref,
    turn,
    acc_ref,
):
    parts = (below_ref, own_ref, above_ref)
    most = jnp.zeros((8, 128), f32)
    for part in parts:
        most = jnp.maximum(most, jnp.max(jnp.abs(part[...]), axis=0))
    most = jnp.maximum(jnp.max(most, axis=1, keepdims=True), 1e-30)
    scale = jnp.broadcast_to(32767.0 / most, (8, 128))
    unit = jnp.broadcast_to(most * (1.0 / 32767.0), (8, 128))
    for n in range(108):
        q = (parts[n // 36][n % 36] * scale + 32768.5).astype(i32)
        words[n] = (q << 16) | pltpu.roll(q, 5, 0)
    units = [jnp.broadcast_to(unit[c : c + 1], (8, 128)) for c in range(6)]
    for t in range(4):
        for c in range(3):
            off_ref[t, c] = cen_ref[t, c] + 32768.0 * units[c]
    turn[...] = jnp.zeros(turn.shape, f32)
    acc_ref[...] = sum_ref[...]
    slot = lax.broadcasted_iota(i32, (8, 128), 0) >> 1

    def gather(t, b):
        code = code_ref[t, pl.ds(pl.multiple_of(b * 8, 8), 8), :]
        at = code & 127
        bits = [(code & (128 << n)) != 0 for n in range(7)]
        valid = cnt8_ref[t] > slot + b * 4
        for c in range(3):

            def pick(lo, level):
                if lo >= 108:
                    return None
                if level == 0:
                    line = jnp.broadcast_to(words[lo, c : c + 1, :], (8, 128))
                    return jnp.take_along_axis(line, at, axis=1, mode="promise_in_bounds")
                first = pick(lo, level - 1)
                second = pick(lo + (1 << (level - 1)), level - 1)
                return first if second is None else jnp.where(bits[level - 1], second, first)

            word = pick(0, 7)
            place = lax.shift_right_logical(word, 16).astype(f32) * units[c] - off_ref[t, c]
            normal = ((word & 65535) - 32768).astype(f32) * units[c + 3]
            turn[c] = jnp.where(valid, place, 0.0)
            turn[c + 3] = jnp.where(valid, normal, 0.0)
        return jnp.concatenate([turn[:, n, :] for n in range(8)], axis=1)

    pair_sums(steps_ref, 0, gather, ki_ref, km_ref, acc_ref)
    mean = jnp.concatenate([acc_ref[t] for t in range(4)], axis=1) * (0.5 / scnt_ref[0:1])
    upper = mean.astype(bf16)
    lower = (mean - upper.astype(f32)).astype(bf16)
    latent = (dot(ko_ref[...], upper) + dot(ko_ref[...], lower)).astype(bf16)
    rank = rank_ref[0:1]
    spread = jnp.zeros((64, 1024), f32)
    for t in range(4):
        spread = spread + dot(latent[:, t * 256 : t * 256 + 256], rank_rows(rank, t * 256, 256))
    out_ref[...] = spread.astype(bf16).reshape(8, 8, 1024)


def forward_kernel(m_ref, ahi_ref, alo_ref, whi_ref, wlo_ref, out_ref, wide):
    rows = [
        m_ref[s].astype(f32)[:, z * 128 : (z + 1) * 128] for s in range(8) for z in range(8)
    ]
    cells = jnp.concatenate(rows, axis=0).astype(bf16)
    z = dot(ahi_ref[...], cells) + dot(alo_ref[...], cells)
    right = []
    for kh in range(4):
        right += [z[kh * 64 + 32 : kh * 64 + 64], -z[kh * 64 : kh * 64 + 32]]
    both = jnp.concatenate([z, jnp.concatenate(right, axis=0)], axis=1).astype(bf16)
    p = dot_t(whi_ref[...], both) + dot_t(wlo_ref[...], both)
    for kh in range(4):
        for h in range(2):
            line = jnp.concatenate(
                [p[q * 64 : (q + 1) * 64, kh * 64 : (kh + 1) * 64] for q in (2 * h, 2 * h + 1)], axis=1
            )
            for jh in range(8):
                wide[pl.ds(((jh * 4 + kh) * 8) * 2 + h, 8, stride=2), :] = line[jh * 8 : jh * 8 + 8]
    out_ref[...] = wide[...].astype(bf16)


def mix_kernel(r_ref, w_ref, own_ref, sel_ref, place_ref, half_ref, out_ref):
    s = jnp.sum(r_ref[...].astype(f32), axis=0)
    s = s.astype(bf16).astype(f32)
    own = own_ref[...]
    g = jnp.zeros((16, 128), f32)
    for ch in range(8):
        line = jnp.concatenate([s[2 * ch : 2 * ch + 1], s[2 * ch + 1 : 2 * ch + 2]], axis=1)
        g = g + dot((line * own).astype(bf16), w_ref[ch])
    spread = dot(g.astype(bf16), sel_ref[...]) * place_ref[...]
    d = dot(half_ref[...], spread.astype(bf16))
    d = jnp.concatenate([d[0:2, oh * 128 : (oh + 1) * 128] for oh in range(8)], axis=0).astype(bf16)
    for n in range(32):
        out_ref[n] = d


def inverse_kernel(q_ref, v_ref, bc_ref, bs_ref, partner_ref, out_ref):
    blocks = []
    for kh in range(4):
        rows = jnp.concatenate([q_ref[jh, kh] for jh in range(8)], axis=0).astype(f32)
        blocks.append(jnp.concatenate([rows[:, 0:64], rows[:, 64:128]], axis=0))
    x = jnp.concatenate(blocks, axis=1)
    row = lax.broadcasted_iota(i32, (256, 256), 0)
    lane = lax.broadcasted_iota(i32, (256, 256), 1)
    x = jnp.where((row == 0) & (lane < 8), 0.0, x)
    xb = x.astype(bf16)
    twin = dot(partner_ref[...], xb[:, 0:128])
    low = lane[0:1, 0:128]
    side = jnp.where(low < 8, 0.5, jnp.where(low < 16, -0.5, 0.0))
    weight = jnp.where(lane[0:1, :] < 16, 0.5, 2.0)
    power = jnp.sum(x * x, axis=0, keepdims=True) * weight
    cross = jnp.sum(x[:, 0:128] * twin, axis=0, keepdims=True) * side
    power = jnp.broadcast_to(power[:, 0:128] + power[:, 128:256] + cross, (8, 128))
    for shift in (8, 16, 32, 64):
        power = power + pltpu.roll(power, shift, 1)
    scale = lax.rsqrt(power * (1.0 / (CELLS * CELLS)) + NORM_FLOOR)[0:1]
    scale = jnp.concatenate([scale, scale], axis=1)
    g = (dot(v_ref[...], xb) * scale).astype(bf16)
    out = dot_t(bc_ref[...], g[0:128]) + dot_t(bs_ref[...], g[128:256])
    out_ref[...] = out.astype(bf16).reshape(8, 8, 8, 128)


def output_kernel(y_ref, lat_ref, w_ref, out_ref):
    for z in range(8):
        y = jnp.concatenate([y_ref[s, z].astype(f32) for s in range(8)], axis=0)
        lat = jnp.concatenate(
            [lat_ref[s].astype(f32)[:, z * 128 : (z + 1) * 128] for s in range(8)], axis=0
        )
        both = jnp.concatenate([lat, y], axis=0).T.astype(bf16)
        v = dot(both, w_ref[...])
        out_ref[:, z, :] = 0.5 * gelu_twice(v)


def call(kernel, name, shape, dtype, *args, scratch=(), smem=0):
    return pl.pallas_call(
        kernel,
        out_shape=jax.ShapeDtypeStruct(shape, dtype),
        in_specs=[SMEM] * smem + [VMEM] * (len(args) - smem),
        out_specs=VMEM,
        scratch_shapes=list(scratch),
        compiler_params=pltpu.CompilerParams(vmem_limit_bytes=48 * 1024 * 1024),
        name=name,
    )(*args)


def sorted_nodes(place, near, valid):
    shapes = (
        ((4, 64, 128), i32),
        ((4, 64, 128), i32),
        ((4, 8, 128), i32),
        ((4, 8, 128), i32),
        ((4, 3, 8, 128), f32),
        ((8, 1024), i32),
        ((8, 1024), f32),
        ((8,), i32),
    )
    return pl.pallas_call(
        sort_kernel,
        out_shape=[jax.ShapeDtypeStruct(*s) for s in shapes],
        in_specs=[SMEM, VMEM, VMEM],
        out_specs=[VMEM] * 7 + [SMEM],
        scratch_shapes=[pltpu.VMEM((4 * NB, 8, 128), f32)],
        compiler_params=pltpu.CompilerParams(vmem_limit_bytes=48 * 1024 * 1024),
        name="sort",
    )(place, near, valid)


def beside(cells, axis):
    count = lax.axis_size(axis)
    ends = count - 1
    return (
        lax.ppermute(cells, axis, [(i, i + 1) for i in range(ends)]),
        cells,
        lax.ppermute(cells, axis, [(i + 1, i) for i in range(ends)]),
    )


def turned(cos, sin, phase):
    c, s = jnp.cos(phase), jnp.sin(phase)
    return cos * c - sin * s, sin * c + cos * s


def body(point_data, neighbours, counts, kernel_in, kernel_mid, kernel_out, spectral, skip_weight):
    gx = lax.axis_index("gx")
    gy = lax.axis_index("gy")
    gz = lax.axis_index(GZ)
    place = jnp.stack([gx, gy, gz]).astype(i32)

    own = jnp.pad(point_data[0].reshape(6, 4, 128).transpose(1, 0, 2), ((0, 0), (0, 2), (0, 0)))
    near = neighbours[0].transpose(3, 2, 0, 1).reshape(NB, 8, 128)
    valid = counts[0].transpose(2, 0, 1).reshape(8, 128)
    ki = jnp.pad(kernel_in.T, ((0, 0), (0, 2)))
    km = kernel_mid.T * jnp.bfloat16(0.5)

    line = jnp.concatenate(beside(own, "gx"), axis=0)
    tables = sorted_nodes(place, near, valid)
    line, tables = lax.optimization_barrier((line, tables))
    far_code, near_code, far8, near8, centres, rank, sorted_counts, steps = tables
    plane = jnp.concatenate(beside(line, "gy"), axis=0)
    sums = call(
        near_kernel,
        "near",
        (4, 80, 256),
        f32,
        steps,
        own,
        near_code,
        near8,
        centres,
        ki,
        km,
        scratch=(pltpu.VMEM((8, 8, 128), f32),),
        smem=1,
    )
    if NEAR_EARLY:
        plane, sums = lax.optimization_barrier((plane, sums))
    below, same, above = beside(plane, GZ)
    latent = call(
        encoder_kernel,
        "encoder",
        (8, 8, 1024),
        bf16,
        steps,
        below,
        same,
        above,
        far_code,
        far8,
        centres,
        rank,
        sorted_counts,
        sums,
        ki,
        km,
        kernel_out.T,
        scratch=(
            pltpu.VMEM((108, 8, 128), i32),
            pltpu.VMEM((4, 3, 8, 128), f32),
            pltpu.VMEM((8, 8, 128), f32),
            pltpu.VMEM((4, 80, 256), f32),
        ),
        smem=1,
    )

    (ffi, ffj), (ifi, ifj), xl, yl = plane_tables()
    local = angle(1, ffi[:, None] * xl[None, :] + ffj[:, None] * yl[None, :])
    phase = ((jnp.asarray(ffi, i32) * 8 * gx + jnp.asarray(ffj, i32) * 16 * gy) % GRID).astype(f32)
    cos, sin = turned(
        np.cos(local).astype(np.float32),
        np.sin(local).astype(np.float32),
        (phase * (2.0 * math.pi / GRID))[:, None],
    )
    whi, wlo = split_two(jnp.concatenate([cos, sin], axis=1))
    local = angle(1, ifi[None, :] * xl[:, None] + ifj[None, :] * yl[:, None])
    phase = ((jnp.asarray(ifi, i32) * 8 * gx + jnp.asarray(ifj, i32) * 16 * gy) % GRID).astype(f32)
    cos, sin = turned(
        np.cos(local).astype(np.float32),
        np.sin(local).astype(np.float32),
        (phase * (2.0 * math.pi / GRID))[None, :],
    )
    back = jnp.concatenate([cos, sin], axis=0).astype(bf16)

    w = spectral.reshape(2, 2, 2, 4, 8, 8, 64).transpose(0, 4, 2, 1, 3, 5, 6)
    wr, wi = w[0], w[1]
    mixing = jnp.stack(
        [jnp.concatenate([wr, wi], axis=-1), jnp.concatenate([-wi, wr], axis=-1)], axis=3
    ).reshape(8, 256, 128)
    joint = jnp.concatenate([skip_weight, jnp.eye(64, dtype=bf16)], axis=0)

    depth = lax.all_to_all(latent, GZ, split_axis=0, concat_axis=0)
    ahi, alo = third_forward()
    partial = call(forward_kernel, "forward", (512, 128), bf16, depth, ahi, alo, whi, wlo, scratch=(pltpu.VMEM((512, 128), f32),))
    partial = lax.all_to_all(partial.reshape(256, 2, 128), ALL, split_axis=0, concat_axis=0)
    own_mask, place_mask, half = mode_masks()
    mixed = call(
        mix_kernel,
        "mix",
        (32, 16, 128),
        bf16,
        partial.reshape(32, 16, 128),
        mixing,
        own_mask,
        placing(),
        place_mask,
        half,
    )
    mixed = lax.all_to_all(mixed.reshape(256, 2, 128), ALL, split_axis=0, concat_axis=0)
    third = third_inverse()
    branch = call(
        inverse_kernel,
        "inverse",
        (8, 8, 8, 128),
        bf16,
        mixed.reshape(8, 4, 16, 128),
        back,
        third[:, :256],
        third[:, 256:],
        partner_table(),
    )
    branch = lax.all_to_all(branch, GZ, split_axis=0, concat_axis=0)
    out = call(output_kernel, "output", (128, 8, 64), f32, branch, latent, joint)
    return out.reshape(1, 8, 16, 8, 64)


def solution(mesh):
    split = Mesh(
        mesh.devices.reshape(mesh.shape["gx"], mesh.shape["gy"], 4, 2), ("gx", "gy", "gz_0", "gz_1")
    )
    return jax.shard_map(
        body,
        mesh=split,
        in_specs=(
            P(None, None, ALL),
            P(None, "gx", "gy", GZ, None),
            P(None, "gx", "gy", GZ),
            P(),
            P(),
            P(),
            P(None, GZ, "gx", "gy", None, None),
            P(),
        ),
        out_specs=P(None, "gx", "gy", GZ, None),
        check_vma=False,
    )
```

```python
import math

import jax
import jax.numpy as jnp
import numpy as np
from jax import lax
from jax.experimental import pallas as pl
from jax.experimental.pallas import tpu as pltpu
from jax.sharding import Mesh
from jax.sharding import PartitionSpec as P

f32 = jnp.float32
bf16 = jnp.bfloat16
i32 = jnp.int32

GRID = 64
NB = 32
NEAR_EARLY = True
ROWS = 8 * NB + 32
LAST = ROWS
CELLS = float(GRID**3)
NORM_FLOOR = 1.0
GZ = ("gz_0", "gz_1")
ALL = ("gx", "gy", "gz_0", "gz_1")
C0 = math.sqrt(2.0 / math.pi)
C1 = C0 * 0.044715
VMEM = pl.BlockSpec(memory_space=pltpu.VMEM)
SMEM = pl.BlockSpec(memory_space=pltpu.SMEM)


def freq(n):
    return np.where(n < 8, n, n - 16)


def angle(f, m):
    return 2.0 * math.pi * ((f * m) % GRID) / GRID


def split_two(a):
    hi = a.astype(bf16)
    lo = (a - hi.astype(a.dtype)).astype(bf16)
    return hi, lo


def third_forward():
    kh, r, kl, c = np.meshgrid(*map(np.arange, (4, 2, 4, 8)), indexing="ij")
    k, r, c = (4 * kh + kl).reshape(-1, 1), r.reshape(-1, 1), c.reshape(-1, 1)
    z = np.repeat(np.arange(64), 8)[None, :]
    cc = np.tile(np.arange(8), 64)[None, :]
    a = angle(k, z)
    v = np.where(r == 0, np.cos(a), -np.sin(a)) * (c == cc)
    return split_two(v)


def third_inverse():
    z = np.repeat(np.arange(64), 8)[:, None]
    o = np.tile(np.arange(8), 64)[:, None]
    s, kh, kl, r, oo = (
        a.reshape(1, -1) for a in np.meshgrid(*map(np.arange, (2, 4, 4, 2, 8)), indexing="ij")
    )
    k = 4 * kh + kl
    a = angle(k, z)
    w = np.where(k == 0, 1.0, 2.0) / CELLS
    cos, sin = np.cos(a), np.sin(a)
    v = np.where(s == 0, np.where(r == 0, cos, -sin), np.where(r == 0, -sin, -cos))
    return (v * w * (o == oo)).astype(bf16)


def plane_tables():
    jl, il, jh, ih = (a.reshape(-1) for a in np.meshgrid(*map(np.arange, (2, 2, 8, 8)), indexing="ij"))
    fwd = freq(2 * ih + il), freq(2 * jh + jl)
    il, jh, ih, jl = (a.reshape(-1) for a in np.meshgrid(*map(np.arange, (2, 8, 8, 2)), indexing="ij"))
    inv = freq(2 * ih + il), freq(2 * jh + jl)
    return fwd, inv, np.repeat(np.arange(8), 16), np.tile(np.arange(16), 8)


def partner_table():
    _, (fi, fj), _, _ = plane_tables()
    hit = (fi[:, None] == -fi[None, :]) & (fj[:, None] == -fj[None, :])
    return hit.astype(np.float32).astype(bf16)


def mode_masks():
    jl, il, kl = (a.reshape(-1, 1) for a in np.meshgrid(*map(np.arange, (2, 2, 4)), indexing="ij"))
    jc, ic, _, kc, _ = (
        a.reshape(1, -1) for a in np.meshgrid(*map(np.arange, (2, 2, 2, 4, 8)), indexing="ij")
    )
    own = ((jl == jc) & (il == ic) & (kl == kc)).astype(np.float32)
    _, ib, kb, _, _ = (
        a.reshape(1, -1) for a in np.meshgrid(*map(np.arange, (8, 2, 4, 2, 8)), indexing="ij")
    )
    place = ((il == ib) & (kl == kb)).astype(np.float32)
    half = np.zeros((8, 16), np.float32)
    half[jl[:, 0], np.arange(16)] = 1.0
    return own, place, half.astype(bf16)


def placing():
    ro, oh, ol = (a.reshape(-1, 1) for a in np.meshgrid(*map(np.arange, (2, 8, 8)), indexing="ij"))
    oc, _, _, rc, lc = (
        a.reshape(1, -1) for a in np.meshgrid(*map(np.arange, (8, 2, 4, 2, 8)), indexing="ij")
    )
    return ((ro == rc) & (oh == oc) & (ol == lc)).astype(np.float32).astype(bf16)


def dot(a, b):
    return jnp.dot(a, b, preferred_element_type=f32)


def dot_t(a, b):
    return lax.dot_general(a, b, (((1,), (1,)), ((), ())), preferred_element_type=f32)


def gelu_twice(v):
    return v * jnp.tanh(v * (v * v * C1 + C0)) + v


def column(line):
    return jnp.broadcast_to(line, (128, 128)).T


def rank_rows(rank, first, count):
    r = lax.broadcasted_iota(i32, (count, 1024), 0) + first
    return jnp.where(r == rank, 1.0, 0.0).astype(bf16)


def sort_kernel(place_ref, nb_ref, cnt_ref, far_ref, near_ref, rank_ref, scnt_ref, tile_ref, lists):
    px, py, pz = place_ref[0], place_ref[1], place_ref[2]
    me = (px * 4 + py) * 8 + pz
    counts = cnt_ref[...]
    nothing = jnp.full((8, 128), -1, i32)
    far = jnp.zeros((8, 128), i32)
    near = jnp.zeros((8, 128), i32)
    codes, far_at, near_at = [], [], []
    for s in range(NB):
        j = nb_ref[s]
        owner = j >> 9
        dz = (owner & 7) - pz + 1
        dy = ((owner >> 3) & 3) - py + 1
        dx = (owner >> 5) - px + 1
        chunk = (((dz * 3 + dy) * 3 + dx) * 4 + ((j >> 7) & 3)) & 127
        codes.append(chunk * 128 + (j & 127))
        valid = counts > s
        mine = owner == me
        is_far = valid & jnp.logical_not(mine)
        is_near = valid & mine
        far_at.append(jnp.where(is_far, far, nothing))
        near_at.append(jnp.where(is_near, near, nothing))
        far = far + is_far.astype(i32)
        near = near + is_near.astype(i32)
    for p in range(NB):
        first = jnp.zeros((8, 128), i32)
        second = jnp.zeros((8, 128), i32)
        for s in range(p, NB):
            first = jnp.where(far_at[s] == p, codes[s], first)
            second = jnp.where(near_at[s] == p, codes[s], second)
        lists[p] = (first >> 7).astype(f32)
        lists[NB + p] = (first & 127).astype(f32)
        lists[2 * NB + p] = ((second >> 7) & 3).astype(f32)
        lists[3 * NB + p] = (second & 127).astype(f32)
    far, near = far.astype(f32), near.astype(f32)
    row8 = lax.broadcasted_iota(i32, (8, 128), 0)
    lane8 = lax.broadcasted_iota(i32, (8, 128), 1)
    key = counts.astype(f32) * 1024.0 - (row8 * 128 + lane8).astype(f32)
    flat = [key[z : z + 1] for z in range(8)]
    ranks = [jnp.zeros((128, 128), f32) for _ in range(8)]
    for z in range(8):
        own = column(flat[z])
        ranks = [r + jnp.where(own > line, 1.0, 0.0) for r, line in zip(ranks, flat)]
    rank = jnp.concatenate([jnp.sum(r, axis=0, keepdims=True) for r in ranks], axis=1).astype(i32)
    rank_ref[...] = jnp.broadcast_to(rank, (8, 1024))
    node = lax.broadcasted_iota(i32, (8, 1024), 1)
    wide = lax.broadcasted_iota(i32, (8, 1024), 0)
    far = jnp.concatenate([far[z : z + 1] for z in range(8)], axis=1)
    near = jnp.concatenate([near[z : z + 1] for z in range(8)], axis=1)
    tail = jnp.where(wide == 2, (node >> 7).astype(f32), (node & 127).astype(f32))
    tail = jnp.where(wide == 0, far, jnp.where(wide == 1, near, tail))
    rows = jnp.concatenate([lists[:, z, :] for z in range(8)], axis=1)
    rows = jnp.concatenate([rows, tail], axis=0).astype(bf16)
    slot = lax.broadcasted_iota(i32, (NB, 128), 0)
    ends = [0, 0]
    for t in range(4):
        found = dot_t(rows, rank_rows(rank, t * 256, 256))
        tail = found[4 * NB : 4 * NB + 8]
        scnt_ref[:, t * 256 : t * 256 + 256] = jnp.broadcast_to(tail[0:1] + tail[1:2], (8, 256))
        for h in range(2):
            part = found[:, h * 128 : h * 128 + 128]
            cell = (tail[2:3] * 128.0 + tail[3:4])[:, h * 128 : h * 128 + 128] * 16384.0
            for n, ref in enumerate((far_ref, near_ref)):
                word = (part[2 * n * NB : (2 * n + 1) * NB] * 128.0 + part[(2 * n + 1) * NB : (2 * n + 2) * NB] + cell).astype(i32)
                length = tail[n : n + 1, h * 128 : h * 128 + 128].astype(i32)
                start = ends[n]
                ref[pl.ds(start, NB), :] = jnp.where(slot < length, word, -1)
                most = jnp.max(length)

                def mark(r, carry):
                    tile_ref[n, start + r] = 2 * t + h
                    return carry

                lax.fori_loop(0, most, mark, 0)
                ends[n] = start + most
    for n, ref in enumerate((far_ref, near_ref)):
        ref[pl.ds(ends[n], 16), :] = jnp.full((16, 128), -1, i32)
        for r in range(16):
            tile_ref[n, ends[n] + r] = 0
        tile_ref[n, LAST] = jnp.maximum((ends[n] + 15) >> 4, 1)


def pair_sums(place_ref, tile_ref, at, code_ref, look_up, ki_ref, km_ref, turn, acc_ref):
    px, py, pz = place_ref[0], place_ref[1], place_ref[2]
    x0 = px.astype(f32) * 8.0 + 0.5
    y0 = py.astype(f32) * 16.0 + 0.5
    z0 = pz.astype(f32) * 8.0 + 0.5
    turn[...] = jnp.zeros(turn.shape, f32)
    steps = tile_ref[at, LAST]

    def gather(b):
        lines = []
        for half in range(2):
            code = code_ref[pl.ds(pl.multiple_of(b * 16 + half * 8, 8), 8), :]
            cell = code >> 14
            centres = (
                (((cell >> 4) & 7).astype(f32) + x0) * (1.0 / GRID),
                ((cell & 15).astype(f32) + y0) * (1.0 / GRID),
                ((cell >> 7).astype(f32) + z0) * (1.0 / GRID),
            )
            values = look_up(code)
            for c in range(6):
                value = values[c]
                if c < 3:
                    value = value - centres[c]
                turn[half, c] = jnp.where(code >= 0, value, 0.0)
            lines += [turn[half, :, n, :] for n in range(8)]
        return jnp.concatenate(lines, axis=1)

    def step(b, pair):
        following = gather(jnp.minimum(b + 1, steps - 1))
        hidden = gelu_twice(dot(ki_ref[...], pair.astype(bf16))).astype(bf16)
        hidden = gelu_twice(dot(km_ref[...], hidden))
        for r in range(16):
            acc_ref[tile_ref[at, b * 16 + r]] += hidden[:, r * 128 : r * 128 + 128]
        return following

    lax.fori_loop(0, steps, step, gather(0))


def lane_gather(line, at):
    return jnp.take_along_axis(jnp.broadcast_to(line, (8, 128)), at, axis=1, mode="promise_in_bounds")


def near_kernel(place_ref, tile_ref, own_ref, code_ref, ki_ref, km_ref, acc_ref, turn):
    acc_ref[...] = jnp.zeros(acc_ref.shape, f32)

    def look_up(code):
        at = code & 127
        low, high = (code & 128) != 0, (code & 256) != 0
        values = []
        for c in range(6):
            found = [lane_gather(own_ref[n, c : c + 1, :], at) for n in range(4)]
            values.append(
                jnp.where(high, jnp.where(low, found[3], found[2]), jnp.where(low, found[1], found[0]))
            )
        return values

    pair_sums(place_ref, tile_ref, 1, code_ref, look_up, ki_ref, km_ref, turn, acc_ref)


def encoder_kernel(
    place_ref,
    tile_ref,
    below_ref,
    own_ref,
    above_ref,
    code_ref,
    rank_ref,
    scnt_ref,
    sum_ref,
    ki_ref,
    km_ref,
    ko_ref,
    out_ref,
    words,
    turn,
    acc_ref,
):
    parts = (below_ref, own_ref, above_ref)
    most = jnp.zeros((8, 128), f32)
    for part in parts:
        most = jnp.maximum(most, jnp.max(jnp.abs(part[...]), axis=0))
    most = jnp.maximum(jnp.max(most, axis=1, keepdims=True), 1e-30)
    scale = jnp.broadcast_to(32767.0 / most, (8, 128))
    unit = jnp.broadcast_to(most * (1.0 / 32767.0), (8, 128))
    for n in range(108):
        q = (parts[n // 36][n % 36] * scale + 32768.5).astype(i32)
        words[n] = (q << 16) | pltpu.roll(q, 5, 0)
    units = [jnp.broadcast_to(unit[c : c + 1], (8, 128)) for c in range(6)]
    acc_ref[...] = sum_ref[...]

    def look_up(code):
        at = code & 127
        bits = [(code & (128 << n)) != 0 for n in range(7)]
        values = [None] * 6
        for c in range(3):

            def pick(lo, level):
                if lo >= 108:
                    return None
                if level == 0:
                    return lane_gather(words[lo, c : c + 1, :], at)
                first = pick(lo, level - 1)
                second = pick(lo + (1 << (level - 1)), level - 1)
                return first if second is None else jnp.where(bits[level - 1], second, first)

            word = pick(0, 7)
            values[c] = (lax.shift_right_logical(word, 16) - 32768).astype(f32) * units[c]
            values[c + 3] = ((word & 65535) - 32768).astype(f32) * units[c + 3]
        return values

    pair_sums(place_ref, tile_ref, 0, code_ref, look_up, ki_ref, km_ref, turn, acc_ref)
    mean = jnp.concatenate([acc_ref[t] for t in range(8)], axis=1) * (0.5 / scnt_ref[0:1])
    upper = mean.astype(bf16)
    lower = (mean - upper.astype(f32)).astype(bf16)
    latent = (dot(ko_ref[...], upper) + dot(ko_ref[...], lower)).astype(bf16)
    rank = rank_ref[0:1]
    spread = jnp.zeros((64, 1024), f32)
    for t in range(4):
        spread = spread + dot(latent[:, t * 256 : t * 256 + 256], rank_rows(rank, t * 256, 256))
    out_ref[...] = spread.astype(bf16).reshape(8, 8, 1024)


def forward_kernel(m_ref, ahi_ref, alo_ref, whi_ref, wlo_ref, out_ref, wide):
    rows = [
        m_ref[s].astype(f32)[:, z * 128 : (z + 1) * 128] for s in range(8) for z in range(8)
    ]
    cells = jnp.concatenate(rows, axis=0).astype(bf16)
    z = dot(ahi_ref[...], cells) + dot(alo_ref[...], cells)
    right = []
    for kh in range(4):
        right += [z[kh * 64 + 32 : kh * 64 + 64], -z[kh * 64 : kh * 64 + 32]]
    both = jnp.concatenate([z, jnp.concatenate(right, axis=0)], axis=1).astype(bf16)
    p = dot_t(whi_ref[...], both) + dot_t(wlo_ref[...], both)
    for kh in range(4):
        for h in range(2):
            line = jnp.concatenate(
                [p[q * 64 : (q + 1) * 64, kh * 64 : (kh + 1) * 64] for q in (2 * h, 2 * h + 1)], axis=1
            )
            for jh in range(8):
                wide[pl.ds(((jh * 4 + kh) * 8) * 2 + h, 8, stride=2), :] = line[jh * 8 : jh * 8 + 8]
    out_ref[...] = wide[...].astype(bf16)


def mix_kernel(r_ref, w_ref, own_ref, sel_ref, place_ref, half_ref, out_ref):
    s = jnp.sum(r_ref[...].astype(f32), axis=0)
    s = s.astype(bf16).astype(f32)
    own = own_ref[...]
    g = jnp.zeros((16, 128), f32)
    for ch in range(8):
        line = jnp.concatenate([s[2 * ch : 2 * ch + 1], s[2 * ch + 1 : 2 * ch + 2]], axis=1)
        g = g + dot((line * own).astype(bf16), w_ref[ch])
    spread = dot(g.astype(bf16), sel_ref[...]) * place_ref[...]
    d = dot(half_ref[...], spread.astype(bf16))
    d = jnp.concatenate([d[0:2, oh * 128 : (oh + 1) * 128] for oh in range(8)], axis=0).astype(bf16)
    for n in range(32):
        out_ref[n] = d


def inverse_kernel(q_ref, v_ref, bc_ref, bs_ref, partner_ref, out_ref):
    blocks = []
    for kh in range(4):
        rows = jnp.concatenate([q_ref[jh, kh] for jh in range(8)], axis=0).astype(f32)
        blocks.append(jnp.concatenate([rows[:, 0:64], rows[:, 64:128]], axis=0))
    x = jnp.concatenate(blocks, axis=1)
    row = lax.broadcasted_iota(i32, (256, 256), 0)
    lane = lax.broadcasted_iota(i32, (256, 256), 1)
    x = jnp.where((row == 0) & (lane < 8), 0.0, x)
    xb = x.astype(bf16)
    twin = dot(partner_ref[...], xb[:, 0:128])
    low = lane[0:1, 0:128]
    side = jnp.where(low < 8, 0.5, jnp.where(low < 16, -0.5, 0.0))
    weight = jnp.where(lane[0:1, :] < 16, 0.5, 2.0)
    power = jnp.sum(x * x, axis=0, keepdims=True) * weight
    cross = jnp.sum(x[:, 0:128] * twin, axis=0, keepdims=True) * side
    power = jnp.broadcast_to(power[:, 0:128] + power[:, 128:256] + cross, (8, 128))
    for shift in (8, 16, 32, 64):
        power = power + pltpu.roll(power, shift, 1)
    scale = lax.rsqrt(power * (1.0 / (CELLS * CELLS)) + NORM_FLOOR)[0:1]
    scale = jnp.concatenate([scale, scale], axis=1)
    g = (dot(v_ref[...], xb) * scale).astype(bf16)
    out = dot_t(bc_ref[...], g[0:128]) + dot_t(bs_ref[...], g[128:256])
    out_ref[...] = out.astype(bf16).reshape(8, 8, 8, 128)


def output_kernel(y_ref, lat_ref, w_ref, out_ref):
    for z in range(8):
        y = jnp.concatenate([y_ref[s, z].astype(f32) for s in range(8)], axis=0)
        lat = jnp.concatenate(
            [lat_ref[s].astype(f32)[:, z * 128 : (z + 1) * 128] for s in range(8)], axis=0
        )
        both = jnp.concatenate([lat, y], axis=0).T.astype(bf16)
        v = dot(both, w_ref[...])
        out_ref[:, z, :] = 0.5 * gelu_twice(v)


def call(kernel, name, shape, dtype, *args, scratch=(), smem=0):
    return pl.pallas_call(
        kernel,
        out_shape=jax.ShapeDtypeStruct(shape, dtype),
        in_specs=[SMEM] * smem + [VMEM] * (len(args) - smem),
        out_specs=VMEM,
        scratch_shapes=list(scratch),
        compiler_params=pltpu.CompilerParams(vmem_limit_bytes=48 * 1024 * 1024),
        name=name,
    )(*args)


def sorted_nodes(place, near, valid):
    shapes = (
        ((ROWS, 128), i32),
        ((ROWS, 128), i32),
        ((8, 1024), i32),
        ((8, 1024), f32),
        ((2, LAST + 1), i32),
    )
    return pl.pallas_call(
        sort_kernel,
        out_shape=[jax.ShapeDtypeStruct(*s) for s in shapes],
        in_specs=[SMEM, VMEM, VMEM],
        out_specs=[VMEM] * 4 + [SMEM],
        scratch_shapes=[pltpu.VMEM((4 * NB, 8, 128), f32)],
        compiler_params=pltpu.CompilerParams(vmem_limit_bytes=48 * 1024 * 1024),
        name="sort",
    )(place, near, valid)


def beside(cells, axis):
    count = lax.axis_size(axis)
    ends = count - 1
    return (
        lax.ppermute(cells, axis, [(i, i + 1) for i in range(ends)]),
        cells,
        lax.ppermute(cells, axis, [(i + 1, i) for i in range(ends)]),
    )


def turned(cos, sin, phase):
    c, s = jnp.cos(phase), jnp.sin(phase)
    return cos * c - sin * s, sin * c + cos * s


def body(point_data, neighbours, counts, kernel_in, kernel_mid, kernel_out, spectral, skip_weight):
    gx = lax.axis_index("gx")
    gy = lax.axis_index("gy")
    gz = lax.axis_index(GZ)
    place = jnp.stack([gx, gy, gz]).astype(i32)

    own = jnp.pad(point_data[0].reshape(6, 4, 128).transpose(1, 0, 2), ((0, 0), (0, 2), (0, 0)))
    near = neighbours[0].transpose(3, 2, 0, 1).reshape(NB, 8, 128)
    valid = counts[0].transpose(2, 0, 1).reshape(8, 128)
    ki = jnp.pad(kernel_in.T, ((0, 0), (0, 2)))
    km = kernel_mid.T * jnp.bfloat16(0.5)

    line = jnp.concatenate(beside(own, "gx"), axis=0)
    tables = sorted_nodes(place, near, valid)
    line, tables = lax.optimization_barrier((line, tables))
    far_code, near_code, rank, sorted_counts, tiles = tables
    plane = jnp.concatenate(beside(line, "gy"), axis=0)
    sums = call(
        near_kernel,
        "near",
        (8, 80, 128),
        f32,
        place,
        tiles,
        own,
        near_code,
        ki,
        km,
        scratch=(pltpu.VMEM((2, 8, 8, 128), f32),),
        smem=2,
    )
    if NEAR_EARLY:
        plane, sums = lax.optimization_barrier((plane, sums))
    below, same, above = beside(plane, GZ)
    latent = call(
        encoder_kernel,
        "encoder",
        (8, 8, 1024),
        bf16,
        place,
        tiles,
        below,
        same,
        above,
        far_code,
        rank,
        sorted_counts,
        sums,
        ki,
        km,
        kernel_out.T,
        scratch=(
            pltpu.VMEM((108, 8, 128), i32),
            pltpu.VMEM((2, 8, 8, 128), f32),
            pltpu.VMEM((8, 80, 128), f32),
        ),
        smem=2,
    )

    (ffi, ffj), (ifi, ifj), xl, yl = plane_tables()
    local = angle(1, ffi[:, None] * xl[None, :] + ffj[:, None] * yl[None, :])
    phase = ((jnp.asarray(ffi, i32) * 8 * gx + jnp.asarray(ffj, i32) * 16 * gy) % GRID).astype(f32)
    cos, sin = turned(
        np.cos(local).astype(np.float32),
        np.sin(local).astype(np.float32),
        (phase * (2.0 * math.pi / GRID))[:, None],
    )
    whi, wlo = split_two(jnp.concatenate([cos, sin], axis=1))
    local = angle(1, ifi[None, :] * xl[:, None] + ifj[None, :] * yl[:, None])
    phase = ((jnp.asarray(ifi, i32) * 8 * gx + jnp.asarray(ifj, i32) * 16 * gy) % GRID).astype(f32)
    cos, sin = turned(
        np.cos(local).astype(np.float32),
        np.sin(local).astype(np.float32),
        (phase * (2.0 * math.pi / GRID))[None, :],
    )
    back = jnp.concatenate([cos, sin], axis=0).astype(bf16)

    w = spectral.reshape(2, 2, 2, 4, 8, 8, 64).transpose(0, 4, 2, 1, 3, 5, 6)
    wr, wi = w[0], w[1]
    mixing = jnp.stack(
        [jnp.concatenate([wr, wi], axis=-1), jnp.concatenate([-wi, wr], axis=-1)], axis=3
    ).reshape(8, 256, 128)
    joint = jnp.concatenate([skip_weight, jnp.eye(64, dtype=bf16)], axis=0)

    depth = lax.all_to_all(latent, GZ, split_axis=0, concat_axis=0)
    ahi, alo = third_forward()
    partial = call(forward_kernel, "forward", (512, 128), bf16, depth, ahi, alo, whi, wlo, scratch=(pltpu.VMEM((512, 128), f32),))
    partial = lax.all_to_all(partial.reshape(256, 2, 128), ALL, split_axis=0, concat_axis=0)
    own_mask, place_mask, half = mode_masks()
    mixed = call(
        mix_kernel,
        "mix",
        (32, 16, 128),
        bf16,
        partial.reshape(32, 16, 128),
        mixing,
        own_mask,
        placing(),
        place_mask,
        half,
    )
    mixed = lax.all_to_all(mixed.reshape(256, 2, 128), ALL, split_axis=0, concat_axis=0)
    third = third_inverse()
    branch = call(
        inverse_kernel,
        "inverse",
        (8, 8, 8, 128),
        bf16,
        mixed.reshape(8, 4, 16, 128),
        back,
        third[:, :256],
        third[:, 256:],
        partner_table(),
    )
    branch = lax.all_to_all(branch, GZ, split_axis=0, concat_axis=0)
    out = call(output_kernel, "output", (128, 8, 64), f32, branch, latent, joint)
    return out.reshape(1, 8, 16, 8, 64)


def solution(mesh):
    split = Mesh(
        mesh.devices.reshape(mesh.shape["gx"], mesh.shape["gy"], 4, 2), ("gx", "gy", "gz_0", "gz_1")
    )
    return jax.shard_map(
        body,
        mesh=split,
        in_specs=(
            P(None, None, ALL),
            P(None, "gx", "gy", GZ, None),
            P(None, "gx", "gy", GZ),
            P(),
            P(),
            P(),
            P(None, GZ, "gx", "gy", None, None),
            P(),
        ),
        out_specs=P(None, "gx", "gy", GZ, None),
        check_vma=False,
    )
```

```python
import math

import jax
import jax.numpy as jnp
import numpy as np
from jax import lax
from jax.experimental import pallas as pl
from jax.experimental.pallas import tpu as pltpu
from jax.sharding import Mesh
from jax.sharding import PartitionSpec as P

f32 = jnp.float32
bf16 = jnp.bfloat16
i32 = jnp.int32

GRID = 64
NB = 32
ROWS = 8 * NB + 32
CELLS = float(GRID**3)
NORM_FLOOR = 1.0
GZ = ("gz_0", "gz_1")
ALL = ("gx", "gy", "gz_0", "gz_1")
C0 = math.sqrt(2.0 / math.pi)
C1 = C0 * 0.044715
VMEM = pl.BlockSpec(memory_space=pltpu.VMEM)
SMEM = pl.BlockSpec(memory_space=pltpu.SMEM)


def freq(n):
    return np.where(n < 8, n, n - 16)


def angle(f, m):
    return 2.0 * math.pi * ((f * m) % GRID) / GRID


def split_two(a):
    hi = a.astype(bf16)
    lo = (a - hi.astype(a.dtype)).astype(bf16)
    return hi, lo


def third_forward():
    kh, r, kl, c = np.meshgrid(*map(np.arange, (4, 2, 4, 8)), indexing="ij")
    k, r, c = (4 * kh + kl).reshape(-1, 1), r.reshape(-1, 1), c.reshape(-1, 1)
    z = np.repeat(np.arange(64), 8)[None, :]
    cc = np.tile(np.arange(8), 64)[None, :]
    a = angle(k, z)
    v = np.where(r == 0, np.cos(a), -np.sin(a)) * (c == cc)
    return split_two(v)


def third_inverse():
    z = np.repeat(np.arange(64), 8)[:, None]
    o = np.tile(np.arange(8), 64)[:, None]
    s, kh, kl, r, oo = (
        a.reshape(1, -1) for a in np.meshgrid(*map(np.arange, (2, 4, 4, 2, 8)), indexing="ij")
    )
    k = 4 * kh + kl
    a = angle(k, z)
    w = np.where(k == 0, 1.0, 2.0) / CELLS
    cos, sin = np.cos(a), np.sin(a)
    v = np.where(s == 0, np.where(r == 0, cos, -sin), np.where(r == 0, -sin, -cos))
    return (v * w * (o == oo)).astype(bf16)


def plane_tables():
    jl, il, jh, ih = (a.reshape(-1) for a in np.meshgrid(*map(np.arange, (2, 2, 8, 8)), indexing="ij"))
    fwd = freq(2 * ih + il), freq(2 * jh + jl)
    il, jh, ih, jl = (a.reshape(-1) for a in np.meshgrid(*map(np.arange, (2, 8, 8, 2)), indexing="ij"))
    inv = freq(2 * ih + il), freq(2 * jh + jl)
    return fwd, inv, np.repeat(np.arange(8), 16), np.tile(np.arange(16), 8)


def partner_table():
    _, (fi, fj), _, _ = plane_tables()
    hit = (fi[:, None] == -fi[None, :]) & (fj[:, None] == -fj[None, :])
    return hit.astype(np.float32).astype(bf16)


def mode_masks():
    jl, il, kl = (a.reshape(-1, 1) for a in np.meshgrid(*map(np.arange, (2, 2, 4)), indexing="ij"))
    jc, ic, _, kc, _ = (
        a.reshape(1, -1) for a in np.meshgrid(*map(np.arange, (2, 2, 2, 4, 8)), indexing="ij")
    )
    own = ((jl == jc) & (il == ic) & (kl == kc)).astype(np.float32)
    _, ib, kb, _, _ = (
        a.reshape(1, -1) for a in np.meshgrid(*map(np.arange, (8, 2, 4, 2, 8)), indexing="ij")
    )
    place = ((il == ib) & (kl == kb)).astype(np.float32)
    half = np.zeros((8, 16), np.float32)
    half[jl[:, 0], np.arange(16)] = 1.0
    return own, place, half.astype(bf16)


def placing():
    ro, oh, ol = (a.reshape(-1, 1) for a in np.meshgrid(*map(np.arange, (2, 8, 8)), indexing="ij"))
    oc, _, _, rc, lc = (
        a.reshape(1, -1) for a in np.meshgrid(*map(np.arange, (8, 2, 4, 2, 8)), indexing="ij")
    )
    return ((ro == rc) & (oh == oc) & (ol == lc)).astype(np.float32).astype(bf16)


def dot(a, b):
    return jnp.dot(a, b, preferred_element_type=f32)


def dot_t(a, b):
    return lax.dot_general(a, b, (((1,), (1,)), ((), ())), preferred_element_type=f32)


def gelu_twice(v):
    return v * jnp.tanh(v * (v * v * C1 + C0)) + v


def column(line):
    return jnp.broadcast_to(line, (128, 128)).T


def rank_rows(rank, first, count):
    r = lax.broadcasted_iota(i32, (count, 1024), 0) + first
    return jnp.where(r == rank, 1.0, 0.0).astype(bf16)


def sort_kernel(place_ref, nb_ref, cnt_ref, far_ref, near_ref, rank_ref, scnt_ref, tile_ref, lists):
    px, py, pz = place_ref[0], place_ref[1], place_ref[2]
    counts = cnt_ref[...]
    nothing = jnp.full((8, 128), -1, i32)
    far = jnp.zeros((8, 128), i32)
    near = jnp.zeros((8, 128), i32)
    codes, far_at, near_at = [], [], []
    for s in range(NB):
        j = nb_ref[s]
        owner = j >> 9
        dz = (owner & 7) - pz + 1
        dy = ((owner >> 3) & 3) - py + 1
        dx = (owner >> 5) - px + 1
        chunk = ((dz >> 1) * 36 + (dy * 3 + dx) * 4 + ((j >> 7) & 3)) & 127
        codes.append(chunk * 128 + (j & 127))
        valid = counts > s
        mine = dz == 1
        is_far = valid & jnp.logical_not(mine)
        is_near = valid & mine
        far_at.append(jnp.where(is_far, far, nothing))
        near_at.append(jnp.where(is_near, near, nothing))
        far = far + is_far.astype(i32)
        near = near + is_near.astype(i32)
    for p in range(NB):
        first = jnp.zeros((8, 128), i32)
        second = jnp.zeros((8, 128), i32)
        for s in range(p, NB):
            first = jnp.where(far_at[s] == p, codes[s], first)
            second = jnp.where(near_at[s] == p, codes[s], second)
        lists[p] = (first >> 7).astype(f32)
        lists[NB + p] = (first & 127).astype(f32)
        lists[2 * NB + p] = (second >> 7).astype(f32)
        lists[3 * NB + p] = (second & 127).astype(f32)
    far, near = far.astype(f32), near.astype(f32)
    row8 = lax.broadcasted_iota(i32, (8, 128), 0)
    lane8 = lax.broadcasted_iota(i32, (8, 128), 1)
    key = counts.astype(f32) * 1024.0 - (row8 * 128 + lane8).astype(f32)
    flat = [key[z : z + 1] for z in range(8)]
    ranks = [jnp.zeros((128, 128), f32) for _ in range(8)]
    for z in range(8):
        own = column(flat[z])
        ranks = [r + jnp.where(own > line, 1.0, 0.0) for r, line in zip(ranks, flat)]
    rank = jnp.concatenate([jnp.sum(r, axis=0, keepdims=True) for r in ranks], axis=1).astype(i32)
    rank_ref[...] = jnp.broadcast_to(rank, (8, 1024))
    node = lax.broadcasted_iota(i32, (8, 1024), 1)
    wide = lax.broadcasted_iota(i32, (8, 1024), 0)
    far = jnp.concatenate([far[z : z + 1] for z in range(8)], axis=1)
    near = jnp.concatenate([near[z : z + 1] for z in range(8)], axis=1)
    tail = jnp.where(wide == 2, (node >> 7).astype(f32), (node & 127).astype(f32))
    tail = jnp.where(wide == 0, far, jnp.where(wide == 1, near, tail))
    rows = jnp.concatenate([lists[:, z, :] for z in range(8)], axis=1)
    rows = jnp.concatenate([rows, tail], axis=0).astype(bf16)
    slot = lax.broadcasted_iota(i32, (NB, 128), 0)
    words, most = [], []
    for t in range(4):
        found = dot_t(rows, rank_rows(rank, t * 256, 256))
        tail = found[4 * NB : 4 * NB + 8]
        scnt_ref[:, t * 256 : t * 256 + 256] = jnp.broadcast_to(tail[0:1] + tail[1:2], (8, 256))
        cell = (tail[2:3] * 128.0 + tail[3:4]) * 16384.0
        for h in range(2):
            at = slice(h * 128, h * 128 + 128)
            for n in range(2):
                upper, lower = found[2 * n * NB : (2 * n + 1) * NB], found[(2 * n + 1) * NB : (2 * n + 2) * NB]
                word = (upper[:, at] * 128.0 + lower[:, at] + cell[:, at]).astype(i32)
                length = tail[n : n + 1, at].astype(i32)
                words.append(jnp.where(slot < length, word, -1))
                most.append(jnp.max(length))
    for n, ref in enumerate((far_ref, near_ref)):
        end = 0
        for t in range(8):
            ref[pl.ds(end, NB), :] = words[2 * t + n]
            end = end + most[2 * t + n]
            tile_ref[n, t] = end
        ref[pl.ds(end, 16), :] = jnp.full((16, 128), -1, i32)
        tile_ref[n, 8] = jnp.maximum((end + 15) >> 4, 1)


def pair_sums(place_ref, tile_ref, at, code_ref, look_up, ki_ref, km_ref, turn, acc_ref):
    px, py, pz = place_ref[0], place_ref[1], place_ref[2]
    x0 = px.astype(f32) * 8.0 + 0.5
    y0 = py.astype(f32) * 16.0 + 0.5
    z0 = pz.astype(f32) * 8.0 + 0.5
    turn[...] = jnp.zeros(turn.shape, f32)
    steps = tile_ref[at, 8]
    ends = [tile_ref[at, t] for t in range(7)]

    def gather(b):
        lines = []
        for half in range(2):
            code = code_ref[pl.ds(pl.multiple_of(b * 16 + half * 8, 8), 8), :]
            cell = code >> 14
            centres = (
                (((cell >> 4) & 7).astype(f32) + x0) * (1.0 / GRID),
                ((cell & 15).astype(f32) + y0) * (1.0 / GRID),
                ((cell >> 7).astype(f32) + z0) * (1.0 / GRID),
            )
            values = look_up(code)
            for c in range(6):
                value = values[c]
                if c < 3:
                    value = value - centres[c]
                turn[half, c] = jnp.where(code >= 0, value, 0.0)
            lines += [turn[half, :, n, :] for n in range(8)]
        return jnp.concatenate(lines, axis=1)

    def add(b, pair):
        hidden = gelu_twice(dot(ki_ref[...], pair.astype(bf16))).astype(bf16)
        hidden = gelu_twice(dot(km_ref[...], hidden))
        for r in range(16):
            tile = sum((b * 16 + r >= end).astype(i32) for end in ends)
            acc_ref[tile] += hidden[:, r * 128 : r * 128 + 128]

    def step(b, pair):
        following = gather(b + 1)
        add(b, pair)
        return following

    add(steps - 1, lax.fori_loop(0, steps - 1, step, gather(0)))


def lane_gather(line, at):
    return jnp.take_along_axis(jnp.broadcast_to(line, (8, 128)), at, axis=1, mode="promise_in_bounds")


def packed(parts, words):
    most = jnp.zeros((8, 128), f32)
    for part in parts:
        most = jnp.maximum(most, jnp.max(jnp.abs(part[...]), axis=0))
    most = jnp.maximum(jnp.max(most, axis=1, keepdims=True), 1e-30)
    scale = jnp.broadcast_to(32767.0 / most, (8, 128))
    unit = jnp.broadcast_to(most * (1.0 / 32767.0), (8, 128))
    for n in range(36 * len(parts)):
        q = (parts[n // 36][n % 36] * scale + 32768.5).astype(i32)
        words[n] = (q << 16) | pltpu.roll(q, 5, 0)
    return [jnp.broadcast_to(unit[c : c + 1], (8, 128)) for c in range(6)]


def looking_up(words, units, count):
    levels = (count - 1).bit_length()

    def look_up(code):
        at = code & 127
        bits = [(code & (128 << n)) != 0 for n in range(levels)]
        values = [None] * 6
        for c in range(3):

            def pick(lo, level):
                if lo >= count:
                    return None
                if level == 0:
                    return lane_gather(words[lo, c : c + 1, :], at)
                first = pick(lo, level - 1)
                second = pick(lo + (1 << (level - 1)), level - 1)
                return first if second is None else jnp.where(bits[level - 1], second, first)

            word = pick(0, levels)
            values[c] = (lax.shift_right_logical(word, 16) - 32768).astype(f32) * units[c]
            values[c + 3] = ((word & 65535) - 32768).astype(f32) * units[c + 3]
        return values

    return look_up


def near_kernel(place_ref, tile_ref, same_ref, code_ref, ki_ref, km_ref, acc_ref, words, turn):
    units = packed((same_ref,), words)
    acc_ref[...] = jnp.zeros(acc_ref.shape, f32)
    look_up = looking_up(words, units, 36)
    pair_sums(place_ref, tile_ref, 1, code_ref, look_up, ki_ref, km_ref, turn, acc_ref)


def encoder_kernel(
    place_ref,
    tile_ref,
    below_ref,
    above_ref,
    code_ref,
    rank_ref,
    scnt_ref,
    sum_ref,
    ki_ref,
    km_ref,
    ko_ref,
    out_ref,
    words,
    turn,
    acc_ref,
):
    units = packed((below_ref, above_ref), words)
    acc_ref[...] = sum_ref[...]
    look_up = looking_up(words, units, 72)
    pair_sums(place_ref, tile_ref, 0, code_ref, look_up, ki_ref, km_ref, turn, acc_ref)
    mean = jnp.concatenate([acc_ref[t] for t in range(8)], axis=1) * (0.5 / scnt_ref[0:1])
    upper = mean.astype(bf16)
    lower = (mean - upper.astype(f32)).astype(bf16)
    latent = (dot(ko_ref[...], upper) + dot(ko_ref[...], lower)).astype(bf16)
    rank = rank_ref[0:1]
    spread = jnp.zeros((64, 1024), f32)
    for t in range(4):
        spread = spread + dot(latent[:, t * 256 : t * 256 + 256], rank_rows(rank, t * 256, 256))
    out_ref[...] = spread.astype(bf16).reshape(8, 8, 1024)


def forward_kernel(m_ref, ahi_ref, alo_ref, whi_ref, wlo_ref, out_ref, wide):
    rows = [
        m_ref[s].astype(f32)[:, z * 128 : (z + 1) * 128] for s in range(8) for z in range(8)
    ]
    cells = jnp.concatenate(rows, axis=0).astype(bf16)
    z = dot(ahi_ref[...], cells) + dot(alo_ref[...], cells)
    right = []
    for kh in range(4):
        right += [z[kh * 64 + 32 : kh * 64 + 64], -z[kh * 64 : kh * 64 + 32]]
    both = jnp.concatenate([z, jnp.concatenate(right, axis=0)], axis=1).astype(bf16)
    p = dot_t(whi_ref[...], both) + dot_t(wlo_ref[...], both)
    for kh in range(4):
        for h in range(2):
            line = jnp.concatenate(
                [p[q * 64 : (q + 1) * 64, kh * 64 : (kh + 1) * 64] for q in (2 * h, 2 * h + 1)], axis=1
            )
            for jh in range(8):
                wide[pl.ds(((jh * 4 + kh) * 8) * 2 + h, 8, stride=2), :] = line[jh * 8 : jh * 8 + 8]
    out_ref[...] = wide[...].astype(bf16)


def mix_kernel(r_ref, w_ref, own_ref, sel_ref, place_ref, half_ref, out_ref):
    s = jnp.sum(r_ref[...].astype(f32), axis=0)
    s = s.astype(bf16).astype(f32)
    own = own_ref[...]
    g = jnp.zeros((16, 128), f32)
    for ch in range(8):
        line = jnp.concatenate([s[2 * ch : 2 * ch + 1], s[2 * ch + 1 : 2 * ch + 2]], axis=1)
        g = g + dot((line * own).astype(bf16), w_ref[ch])
    spread = dot(g.astype(bf16), sel_ref[...]) * place_ref[...]
    d = dot(half_ref[...], spread.astype(bf16))
    d = jnp.concatenate([d[0:2, oh * 128 : (oh + 1) * 128] for oh in range(8)], axis=0).astype(bf16)
    for n in range(32):
        out_ref[n] = d


def inverse_kernel(q_ref, v_ref, bc_ref, bs_ref, partner_ref, out_ref):
    blocks = []
    for kh in range(4):
        rows = jnp.concatenate([q_ref[jh, kh] for jh in range(8)], axis=0).astype(f32)
        blocks.append(jnp.concatenate([rows[:, 0:64], rows[:, 64:128]], axis=0))
    x = jnp.concatenate(blocks, axis=1)
    row = lax.broadcasted_iota(i32, (256, 256), 0)
    lane = lax.broadcasted_iota(i32, (256, 256), 1)
    x = jnp.where((row == 0) & (lane < 8), 0.0, x)
    xb = x.astype(bf16)
    twin = dot(partner_ref[...], xb[:, 0:128])
    low = lane[0:1, 0:128]
    side = jnp.where(low < 8, 0.5, jnp.where(low < 16, -0.5, 0.0))
    weight = jnp.where(lane[0:1, :] < 16, 0.5, 2.0)
    power = jnp.sum(x * x, axis=0, keepdims=True) * weight
    cross = jnp.sum(x[:, 0:128] * twin, axis=0, keepdims=True) * side
    power = jnp.broadcast_to(power[:, 0:128] + power[:, 128:256] + cross, (8, 128))
    for shift in (8, 16, 32, 64):
        power = power + pltpu.roll(power, shift, 1)
    scale = lax.rsqrt(power * (1.0 / (CELLS * CELLS)) + NORM_FLOOR)[0:1]
    scale = jnp.concatenate([scale, scale], axis=1)
    g = (dot(v_ref[...], xb) * scale).astype(bf16)
    out = dot_t(bc_ref[...], g[0:128]) + dot_t(bs_ref[...], g[128:256])
    out_ref[...] = out.astype(bf16).reshape(8, 8, 8, 128)


def output_kernel(y_ref, lat_ref, w_ref, out_ref):
    for z in range(8):
        y = jnp.concatenate([y_ref[s, z].astype(f32) for s in range(8)], axis=0)
        lat = jnp.concatenate(
            [lat_ref[s].astype(f32)[:, z * 128 : (z + 1) * 128] for s in range(8)], axis=0
        )
        both = jnp.concatenate([lat, y], axis=0).T.astype(bf16)
        v = dot(both, w_ref[...])
        out_ref[:, z, :] = 0.5 * gelu_twice(v)


def call(kernel, shape, dtype, *args, scratch=(), smem=0):
    return pl.pallas_call(
        kernel,
        out_shape=jax.ShapeDtypeStruct(shape, dtype),
        in_specs=[SMEM] * smem + [VMEM] * (len(args) - smem),
        out_specs=VMEM,
        scratch_shapes=list(scratch),
        compiler_params=pltpu.CompilerParams(vmem_limit_bytes=48 * 1024 * 1024),
    )(*args)


def sorted_nodes(place, near, valid):
    shapes = (
        ((ROWS, 128), i32),
        ((ROWS, 128), i32),
        ((8, 1024), i32),
        ((8, 1024), f32),
        ((2, 9), i32),
    )
    return pl.pallas_call(
        sort_kernel,
        out_shape=[jax.ShapeDtypeStruct(*s) for s in shapes],
        in_specs=[SMEM, VMEM, VMEM],
        out_specs=[VMEM] * 4 + [SMEM],
        scratch_shapes=[pltpu.VMEM((4 * NB, 8, 128), f32)],
        compiler_params=pltpu.CompilerParams(vmem_limit_bytes=48 * 1024 * 1024),
        name="sort",
    )(place, near, valid)


def beside(cells, axis):
    count = lax.axis_size(axis)
    ends = count - 1
    lower = lax.ppermute(cells, axis, [(i, i + 1) for i in range(ends)])
    upper = lax.ppermute(cells, axis, [(i + 1, i) for i in range(ends)])
    return lower, cells, upper


def turned(cos, sin, phase):
    c, s = jnp.cos(phase), jnp.sin(phase)
    return cos * c - sin * s, sin * c + cos * s


def layer(point_data, neighbours, counts, kernel_in, kernel_mid, kernel_out, spectral, skip_weight):
    gx = lax.axis_index("gx")
    gy = lax.axis_index("gy")
    gz = lax.axis_index(GZ)
    place = jnp.stack([gx, gy, gz]).astype(i32)

    own = jnp.pad(point_data[0].reshape(6, 4, 128).transpose(1, 0, 2), ((0, 0), (0, 2), (0, 0)))
    near = neighbours[0].transpose(3, 2, 0, 1).reshape(NB, 8, 128)
    valid = counts[0].transpose(2, 0, 1).reshape(8, 128)
    ki = jnp.pad(kernel_in.T, ((0, 0), (0, 2)))
    km = kernel_mid.T * jnp.bfloat16(0.5)

    line = jnp.concatenate(beside(own, "gx"), axis=0)
    plane = jnp.concatenate(beside(line, "gy"), axis=0)
    tables = sorted_nodes(place, near, valid)
    plane, tables = lax.optimization_barrier((plane, tables))
    far_code, near_code, rank, sorted_counts, tiles = tables
    below, same, above = beside(plane, GZ)
    sums = call(
        near_kernel,
        (8, 80, 128),
        f32,
        place,
        tiles,
        same,
        near_code,
        ki,
        km,
        scratch=(pltpu.VMEM((36, 8, 128), i32), pltpu.VMEM((2, 8, 8, 128), f32)),
        smem=2,
    )
    latent = call(
        encoder_kernel,
        (8, 8, 1024),
        bf16,
        place,
        tiles,
        below,
        above,
        far_code,
        rank,
        sorted_counts,
        sums,
        ki,
        km,
        kernel_out.T,
        scratch=(
            pltpu.VMEM((72, 8, 128), i32),
            pltpu.VMEM((2, 8, 8, 128), f32),
            pltpu.VMEM((8, 80, 128), f32),
        ),
        smem=2,
    )

    (ffi, ffj), (ifi, ifj), xl, yl = plane_tables()
    local = angle(1, ffi[:, None] * xl[None, :] + ffj[:, None] * yl[None, :])
    phase = ((jnp.asarray(ffi, i32) * 8 * gx + jnp.asarray(ffj, i32) * 16 * gy) % GRID).astype(f32)
    cos, sin = turned(
        np.cos(local).astype(np.float32),
        np.sin(local).astype(np.float32),
        (phase * (2.0 * math.pi / GRID))[:, None],
    )
    whi, wlo = split_two(jnp.concatenate([cos, sin], axis=1))
    local = angle(1, ifi[None, :] * xl[:, None] + ifj[None, :] * yl[:, None])
    phase = ((jnp.asarray(ifi, i32) * 8 * gx + jnp.asarray(ifj, i32) * 16 * gy) % GRID).astype(f32)
    cos, sin = turned(
        np.cos(local).astype(np.float32),
        np.sin(local).astype(np.float32),
        (phase * (2.0 * math.pi / GRID))[None, :],
    )
    back = jnp.concatenate([cos, sin], axis=0).astype(bf16)

    w = spectral.reshape(2, 2, 2, 4, 8, 8, 64).transpose(0, 4, 2, 1, 3, 5, 6)
    wr, wi = w[0], w[1]
    mixing = jnp.stack(
        [jnp.concatenate([wr, wi], axis=-1), jnp.concatenate([-wi, wr], axis=-1)], axis=3
    ).reshape(8, 256, 128)
    joint = jnp.concatenate([skip_weight, jnp.eye(64, dtype=bf16)], axis=0)

    depth = lax.all_to_all(latent, GZ, split_axis=0, concat_axis=0)
    ahi, alo = third_forward()
    partial = call(forward_kernel, (512, 128), bf16, depth, ahi, alo, whi, wlo, scratch=(pltpu.VMEM((512, 128), f32),))
    partial = lax.all_to_all(partial.reshape(256, 2, 128), ALL, split_axis=0, concat_axis=0)
    own_mask, place_mask, half = mode_masks()
    mixed = call(
        mix_kernel, (32, 16, 128), bf16, partial.reshape(32, 16, 128), mixing, own_mask, placing(), place_mask, half
    )
    mixed = lax.all_to_all(mixed.reshape(256, 2, 128), ALL, split_axis=0, concat_axis=0)
    third = third_inverse()
    branch = call(
        inverse_kernel,
        (8, 8, 8, 128),
        bf16,
        mixed.reshape(8, 4, 16, 128),
        back,
        third[:, :256],
        third[:, 256:],
        partner_table(),
    )
    branch = lax.all_to_all(branch, GZ, split_axis=0, concat_axis=0)
    out = call(output_kernel, (128, 8, 64), f32, branch, latent, joint)
    return out.reshape(1, 8, 16, 8, 64)


def solution(mesh):
    split = Mesh(
        mesh.devices.reshape(mesh.shape["gx"], mesh.shape["gy"], 4, 2), ("gx", "gy", "gz_0", "gz_1")
    )
    return jax.shard_map(
        layer,
        mesh=split,
        in_specs=(
            P(None, None, ALL),
            P(None, "gx", "gy", GZ, None),
            P(None, "gx", "gy", GZ),
            P(),
            P(),
            P(),
            P(None, GZ, "gx", "gy", None, None),
            P(),
        ),
        out_specs=P(None, "gx", "gy", GZ, None),
        check_vma=False,
    )
```

```python
import math

import jax
import jax.numpy as jnp
import numpy as np
from jax import lax
from jax.experimental import pallas as pl
from jax.experimental.pallas import tpu as pltpu
from jax.sharding import Mesh
from jax.sharding import PartitionSpec as P

f32 = jnp.float32
bf16 = jnp.bfloat16
i32 = jnp.int32

GRID = 64
NB = 32
ROWS = 8 * NB + 32
CELLS = float(GRID**3)
NORM_FLOOR = 1.0
GZ = ("gz_0", "gz_1")
ALL = ("gx", "gy", "gz_0", "gz_1")
C0 = math.sqrt(2.0 / math.pi)
C1 = C0 * 0.044715
VMEM = pl.BlockSpec(memory_space=pltpu.VMEM)
SMEM = pl.BlockSpec(memory_space=pltpu.SMEM)


def freq(n):
    return np.where(n < 8, n, n - 16)


def angle(f, m):
    return 2.0 * math.pi * ((f * m) % GRID) / GRID


def split_two(a):
    hi = a.astype(bf16)
    lo = (a - hi.astype(a.dtype)).astype(bf16)
    return hi, lo


def third_forward():
    kh, r, kl, c = np.meshgrid(*map(np.arange, (4, 2, 4, 8)), indexing="ij")
    k, r, c = (4 * kh + kl).reshape(-1, 1), r.reshape(-1, 1), c.reshape(-1, 1)
    z = np.repeat(np.arange(64), 8)[None, :]
    cc = np.tile(np.arange(8), 64)[None, :]
    a = angle(k, z)
    v = np.where(r == 0, np.cos(a), -np.sin(a)) * (c == cc)
    return split_two(v)


def third_inverse():
    z = np.repeat(np.arange(64), 8)[:, None]
    o = np.tile(np.arange(8), 64)[:, None]
    s, kh, kl, r, oo = (
        a.reshape(1, -1) for a in np.meshgrid(*map(np.arange, (2, 4, 4, 2, 8)), indexing="ij")
    )
    k = 4 * kh + kl
    a = angle(k, z)
    w = np.where(k == 0, 1.0, 2.0) / CELLS
    cos, sin = np.cos(a), np.sin(a)
    v = np.where(s == 0, np.where(r == 0, cos, -sin), np.where(r == 0, -sin, -cos))
    return (v * w * (o == oo)).astype(bf16)


def plane_tables():
    jl, il, jh, ih = (a.reshape(-1) for a in np.meshgrid(*map(np.arange, (2, 2, 8, 8)), indexing="ij"))
    fwd = freq(2 * ih + il), freq(2 * jh + jl)
    il, jh, ih, jl = (a.reshape(-1) for a in np.meshgrid(*map(np.arange, (2, 8, 8, 2)), indexing="ij"))
    inv = freq(2 * ih + il), freq(2 * jh + jl)
    return fwd, inv, np.repeat(np.arange(8), 16), np.tile(np.arange(16), 8)


def partner_table():
    _, (fi, fj), _, _ = plane_tables()
    hit = (fi[:, None] == -fi[None, :]) & (fj[:, None] == -fj[None, :])
    return hit.astype(np.float32).astype(bf16)


def mode_masks():
    jl, il, kl = (a.reshape(-1, 1) for a in np.meshgrid(*map(np.arange, (2, 2, 4)), indexing="ij"))
    jc, ic, _, kc, _ = (
        a.reshape(1, -1) for a in np.meshgrid(*map(np.arange, (2, 2, 2, 4, 8)), indexing="ij")
    )
    own = ((jl == jc) & (il == ic) & (kl == kc)).astype(np.float32)
    _, ib, kb, _, _ = (
        a.reshape(1, -1) for a in np.meshgrid(*map(np.arange, (8, 2, 4, 2, 8)), indexing="ij")
    )
    place = ((il == ib) & (kl == kb)).astype(np.float32)
    half = np.zeros((8, 16), np.float32)
    half[jl[:, 0], np.arange(16)] = 1.0
    return own, place, half.astype(bf16)


def placing():
    ro, oh, ol = (a.reshape(-1, 1) for a in np.meshgrid(*map(np.arange, (2, 8, 8)), indexing="ij"))
    oc, _, _, rc, lc = (
        a.reshape(1, -1) for a in np.meshgrid(*map(np.arange, (8, 2, 4, 2, 8)), indexing="ij")
    )
    return ((ro == rc) & (oh == oc) & (ol == lc)).astype(np.float32).astype(bf16)


def dot(a, b):
    return jnp.dot(a, b, preferred_element_type=f32)


def dot_t(a, b):
    return lax.dot_general(a, b, (((1,), (1,)), ((), ())), preferred_element_type=f32)


def gelu_twice(v):
    return v * jnp.tanh(v * (v * v * C1 + C0)) + v


def column(line):
    return jnp.broadcast_to(line, (128, 128)).T


def rank_rows(rank, first, count):
    r = lax.broadcasted_iota(i32, (count, 1024), 0) + first
    return jnp.where(r == rank, 1.0, 0.0).astype(bf16)


def sort_kernel(place_ref, nb_ref, cnt_ref, code_ref, rank_ref, scnt_ref, tile_ref):
    px, py, pz = place_ref[0], place_ref[1], place_ref[2]
    j = nb_ref[...]
    owner = j >> 9
    dz = (owner & 7) - pz + 1
    dy = ((owner >> 3) & 3) - py + 1
    dx = (owner >> 5) - px + 1
    group = jnp.where(dz == 1, 72, (dz >> 1) * 36)
    chunk = ((group + (dy * 3 + dx) * 4 + ((j >> 7) & 3)) & 127).astype(f32)
    lane = (j & 127).astype(f32)
    counts = cnt_ref[...].astype(f32)
    row8 = lax.broadcasted_iota(i32, (8, 128), 0)
    lane8 = lax.broadcasted_iota(i32, (8, 128), 1)
    key = counts * 1024.0 - (row8 * 128 + lane8).astype(f32)
    flat = [key[z : z + 1] for z in range(8)]
    ranks = [jnp.zeros((128, 128), f32) for _ in range(8)]
    for z in range(8):
        own = column(flat[z])
        ranks = [r + jnp.where(own > line, 1.0, 0.0) for r, line in zip(ranks, flat)]
    rank = jnp.concatenate([jnp.sum(r, axis=0, keepdims=True) for r in ranks], axis=1).astype(i32)
    rank_ref[...] = jnp.broadcast_to(rank, (8, 1024))
    node = lax.broadcasted_iota(i32, (8, 1024), 1)
    wide = lax.broadcasted_iota(i32, (8, 1024), 0)
    line = jnp.concatenate([counts[z : z + 1] for z in range(8)], axis=1)
    tail = jnp.where(wide == 1, (node >> 7).astype(f32), (node & 127).astype(f32))
    tail = jnp.where(wide == 0, line, tail)
    rows = [jnp.concatenate([a[:, z, :] for z in range(8)], axis=1) for a in (chunk, lane)]
    rows = jnp.concatenate(rows + [tail], axis=0).astype(bf16)
    slot = lax.broadcasted_iota(i32, (NB, 128), 0)
    words, most = [], []
    for t in range(4):
        found = dot_t(rows, rank_rows(rank, t * 256, 256))
        tail = found[2 * NB : 2 * NB + 8]
        scnt_ref[:, t * 256 : t * 256 + 256] = jnp.broadcast_to(tail[0:1], (8, 256))
        cell = (tail[1:2] * 128.0 + tail[2:3]) * 16384.0
        word = (found[0:NB] * 128.0 + found[NB : 2 * NB] + cell).astype(i32)
        length = tail[0:1].astype(i32)
        for h in range(2):
            at = slice(h * 128, h * 128 + 128)
            words.append(jnp.where(slot < length[:, at], word[:, at], -1))
            most.append(jnp.max(length[:, at]))
    end = 0
    for t in range(8):
        code_ref[pl.ds(end, NB), :] = words[t]
        end = end + most[t]
        tile_ref[t] = end
    code_ref[pl.ds(end, 16), :] = jnp.full((16, 128), -1, i32)
    tile_ref[8] = (end + 15) >> 4


def pair_sums(place_ref, tile_ref, code_ref, look_up, ki_ref, km_ref, turn, acc_ref):
    px, py, pz = place_ref[0], place_ref[1], place_ref[2]
    x0 = px.astype(f32) * 8.0 + 0.5
    y0 = py.astype(f32) * 16.0 + 0.5
    z0 = pz.astype(f32) * 8.0 + 0.5
    turn[...] = jnp.zeros(turn.shape, f32)
    steps = tile_ref[8]
    ends = [tile_ref[t] for t in range(7)]

    def gather(b):
        lines = []
        for half in range(2):
            code = code_ref[pl.ds(pl.multiple_of(b * 16 + half * 8, 8), 8), :]
            cell = code >> 14
            centres = (
                (((cell >> 4) & 7).astype(f32) + x0) * (1.0 / GRID),
                ((cell & 15).astype(f32) + y0) * (1.0 / GRID),
                ((cell >> 7).astype(f32) + z0) * (1.0 / GRID),
            )
            values = look_up(code, b * 2 + half)
            for c in range(6):
                value = values[c]
                if c < 3:
                    value = value - centres[c]
                turn[half, c] = jnp.where(code >= 0, value, 0.0)
            lines += [turn[half, :, n, :] for n in range(8)]
        return jnp.concatenate(lines, axis=1)

    def add(b, pair):
        hidden = gelu_twice(dot(ki_ref[...], pair.astype(bf16))).astype(bf16)
        hidden = gelu_twice(dot(km_ref[...], hidden))
        for r in range(16):
            tile = sum((b * 16 + r >= end).astype(i32) for end in ends)
            acc_ref[tile] += hidden[:, r * 128 : r * 128 + 128]

    def step(b, pair):
        following = gather(b + 1)
        add(b, pair)
        return following

    add(steps - 1, lax.fori_loop(0, steps - 1, step, gather(0)))


def lane_gather(line, at):
    return jnp.take_along_axis(jnp.broadcast_to(line, (8, 128)), at, axis=1, mode="promise_in_bounds")


def packed(parts, words):
    most = jnp.zeros((8, 128), f32)
    for part in parts:
        most = jnp.maximum(most, jnp.max(jnp.abs(part[...]), axis=0))
    most = jnp.maximum(jnp.max(most, axis=1, keepdims=True), 1e-30)
    scale = jnp.broadcast_to(32767.0 / most, (8, 128))
    unit = jnp.broadcast_to(most * (1.0 / 32767.0), (8, 128))
    for n in range(36 * len(parts)):
        q = (parts[n // 36][n % 36] * scale + 32768.5).astype(i32)
        words[n] = (q << 16) | pltpu.roll(q, 5, 0)
    return unit


def rows_of(unit):
    return [jnp.broadcast_to(unit[c : c + 1], (8, 128)) for c in range(6)]


def pick_word(words, c, code, count):
    levels = (count - 1).bit_length()
    at = code & 127
    bits = [(code & (128 << n)) != 0 for n in range(levels)]

    def pick(lo, level):
        if lo >= count:
            return None
        if level == 0:
            return lane_gather(words[lo, c : c + 1, :], at)
        first = pick(lo, level - 1)
        second = pick(lo + (1 << (level - 1)), level - 1)
        return first if second is None else jnp.where(bits[level - 1], second, first)

    return pick(0, levels)


def near_kernel(tile_ref, same_ref, code_ref, out_ref, unit_ref, words):
    unit_ref[...] = packed((same_ref,), words)

    def step(b, carry):
        for half in range(2):
            code = code_ref[pl.ds(pl.multiple_of(b * 16 + half * 8, 8), 8), :] - 72 * 128
            for c in range(3):
                out_ref[b * 2 + half, c] = pick_word(words, c, code, 36)
        return carry

    lax.fori_loop(0, tile_ref[8], step, 0)


def encoder_kernel(
    place_ref,
    tile_ref,
    below_ref,
    above_ref,
    code_ref,
    near_ref,
    unit_ref,
    rank_ref,
    scnt_ref,
    ki_ref,
    km_ref,
    ko_ref,
    out_ref,
    words,
    turn,
    acc_ref,
):
    far_units = rows_of(packed((below_ref, above_ref), words))
    near_units = rows_of(unit_ref[...])
    acc_ref[...] = jnp.zeros(acc_ref.shape, f32)

    def look_up(code, block):
        near = (code & 16383) >= 72 * 128
        values = [None] * 6
        for c in range(3):
            word = jnp.where(near, near_ref[block, c], pick_word(words, c, code, 72))
            upper = jnp.where(near, near_units[c], far_units[c])
            lower = jnp.where(near, near_units[c + 3], far_units[c + 3])
            values[c] = (lax.shift_right_logical(word, 16) - 32768).astype(f32) * upper
            values[c + 3] = ((word & 65535) - 32768).astype(f32) * lower
        return values

    pair_sums(place_ref, tile_ref, code_ref, look_up, ki_ref, km_ref, turn, acc_ref)
    mean = jnp.concatenate([acc_ref[t] for t in range(8)], axis=1) * (0.5 / scnt_ref[0:1])
    upper = mean.astype(bf16)
    lower = (mean - upper.astype(f32)).astype(bf16)
    latent = (dot(ko_ref[...], upper) + dot(ko_ref[...], lower)).astype(bf16)
    rank = rank_ref[0:1]
    spread = jnp.zeros((64, 1024), f32)
    for t in range(4):
        spread = spread + dot(latent[:, t * 256 : t * 256 + 256], rank_rows(rank, t * 256, 256))
    out_ref[...] = spread.astype(bf16).reshape(8, 8, 1024)


def forward_kernel(m_ref, ahi_ref, alo_ref, whi_ref, wlo_ref, out_ref, wide):
    rows = [
        m_ref[s].astype(f32)[:, z * 128 : (z + 1) * 128] for s in range(8) for z in range(8)
    ]
    cells = jnp.concatenate(rows, axis=0).astype(bf16)
    z = dot(ahi_ref[...], cells) + dot(alo_ref[...], cells)
    right = []
    for kh in range(4):
        right += [z[kh * 64 + 32 : kh * 64 + 64], -z[kh * 64 : kh * 64 + 32]]
    both = jnp.concatenate([z, jnp.concatenate(right, axis=0)], axis=1).astype(bf16)
    p = dot_t(whi_ref[...], both) + dot_t(wlo_ref[...], both)
    for kh in range(4):
        for h in range(2):
            line = jnp.concatenate(
                [p[q * 64 : (q + 1) * 64, kh * 64 : (kh + 1) * 64] for q in (2 * h, 2 * h + 1)], axis=1
            )
            for jh in range(8):
                wide[pl.ds(((jh * 4 + kh) * 8) * 2 + h, 8, stride=2), :] = line[jh * 8 : jh * 8 + 8]
    out_ref[...] = wide[...].astype(bf16)


def mix_kernel(r_ref, w_ref, own_ref, sel_ref, place_ref, half_ref, out_ref):
    s = jnp.sum(r_ref[...].astype(f32), axis=0)
    s = s.astype(bf16).astype(f32)
    own = own_ref[...]
    g = jnp.zeros((16, 128), f32)
    for ch in range(8):
        line = jnp.concatenate([s[2 * ch : 2 * ch + 1], s[2 * ch + 1 : 2 * ch + 2]], axis=1)
        g = g + dot((line * own).astype(bf16), w_ref[ch])
    spread = dot(g.astype(bf16), sel_ref[...]) * place_ref[...]
    d = dot(half_ref[...], spread.astype(bf16))
    d = jnp.concatenate([d[0:2, oh * 128 : (oh + 1) * 128] for oh in range(8)], axis=0).astype(bf16)
    for n in range(32):
        out_ref[n] = d


def inverse_kernel(q_ref, v_ref, bc_ref, bs_ref, partner_ref, out_ref):
    blocks = []
    for kh in range(4):
        rows = jnp.concatenate([q_ref[jh, kh] for jh in range(8)], axis=0).astype(f32)
        blocks.append(jnp.concatenate([rows[:, 0:64], rows[:, 64:128]], axis=0))
    x = jnp.concatenate(blocks, axis=1)
    row = lax.broadcasted_iota(i32, (256, 256), 0)
    lane = lax.broadcasted_iota(i32, (256, 256), 1)
    x = jnp.where((row == 0) & (lane < 8), 0.0, x)
    xb = x.astype(bf16)
    twin = dot(partner_ref[...], xb[:, 0:128])
    low = lane[0:1, 0:128]
    side = jnp.where(low < 8, 0.5, jnp.where(low < 16, -0.5, 0.0))
    weight = jnp.where(lane[0:1, :] < 16, 0.5, 2.0)
    power = jnp.sum(x * x, axis=0, keepdims=True) * weight
    cross = jnp.sum(x[:, 0:128] * twin, axis=0, keepdims=True) * side
    power = jnp.broadcast_to(power[:, 0:128] + power[:, 128:256] + cross, (8, 128))
    for shift in (8, 16, 32, 64):
        power = power + pltpu.roll(power, shift, 1)
    scale = lax.rsqrt(power * (1.0 / (CELLS * CELLS)) + NORM_FLOOR)[0:1]
    scale = jnp.concatenate([scale, scale], axis=1)
    g = (dot(v_ref[...], xb) * scale).astype(bf16)
    out = dot_t(bc_ref[...], g[0:128]) + dot_t(bs_ref[...], g[128:256])
    out_ref[...] = out.astype(bf16).reshape(8, 8, 8, 128)


def output_kernel(y_ref, lat_ref, w_ref, out_ref):
    for z in range(8):
        y = jnp.concatenate([y_ref[s, z].astype(f32) for s in range(8)], axis=0)
        lat = jnp.concatenate(
            [lat_ref[s].astype(f32)[:, z * 128 : (z + 1) * 128] for s in range(8)], axis=0
        )
        both = jnp.concatenate([lat, y], axis=0).T.astype(bf16)
        v = dot(both, w_ref[...])
        out_ref[:, z, :] = 0.5 * gelu_twice(v)


def call(kernel, shape, dtype, *args, scratch=(), smem=0):
    return pl.pallas_call(
        kernel,
        out_shape=jax.ShapeDtypeStruct(shape, dtype),
        in_specs=[SMEM] * smem + [VMEM] * (len(args) - smem),
        out_specs=VMEM,
        scratch_shapes=list(scratch),
        compiler_params=pltpu.CompilerParams(vmem_limit_bytes=48 * 1024 * 1024),
    )(*args)


def sorted_nodes(place, near, valid):
    shapes = (
        ((ROWS, 128), i32),
        ((8, 1024), i32),
        ((8, 1024), f32),
        ((9,), i32),
    )
    return pl.pallas_call(
        sort_kernel,
        out_shape=[jax.ShapeDtypeStruct(*s) for s in shapes],
        in_specs=[SMEM, VMEM, VMEM],
        out_specs=[VMEM] * 3 + [SMEM],
        compiler_params=pltpu.CompilerParams(vmem_limit_bytes=48 * 1024 * 1024),
        name="sort",
    )(place, near, valid)


def near_words(tiles, same, code):
    shapes = (((ROWS // 8, 3, 8, 128), i32), ((8, 128), f32))
    return pl.pallas_call(
        near_kernel,
        out_shape=[jax.ShapeDtypeStruct(*s) for s in shapes],
        in_specs=[SMEM, VMEM, VMEM],
        out_specs=[VMEM] * 2,
        scratch_shapes=[pltpu.VMEM((36, 8, 128), i32)],
        compiler_params=pltpu.CompilerParams(vmem_limit_bytes=48 * 1024 * 1024),
        name="near",
    )(tiles, same, code)


def beside(cells, axis):
    count = lax.axis_size(axis)
    ends = count - 1
    lower = lax.ppermute(cells, axis, [(i, i + 1) for i in range(ends)])
    upper = lax.ppermute(cells, axis, [(i + 1, i) for i in range(ends)])
    return lower, cells, upper


def turned(cos, sin, phase):
    c, s = jnp.cos(phase), jnp.sin(phase)
    return cos * c - sin * s, sin * c + cos * s


def layer(point_data, neighbours, counts, kernel_in, kernel_mid, kernel_out, spectral, skip_weight):
    gx = lax.axis_index("gx")
    gy = lax.axis_index("gy")
    gz = lax.axis_index(GZ)
    place = jnp.stack([gx, gy, gz]).astype(i32)

    own = jnp.pad(point_data[0].reshape(6, 4, 128).transpose(1, 0, 2), ((0, 0), (0, 2), (0, 0)))
    near = neighbours[0].transpose(3, 2, 0, 1).reshape(NB, 8, 128)
    valid = counts[0].transpose(2, 0, 1).reshape(8, 128)
    ki = jnp.pad(kernel_in.T, ((0, 0), (0, 2)))
    km = kernel_mid.T * jnp.bfloat16(0.5)

    line = jnp.concatenate(beside(own, "gx"), axis=0)
    plane = jnp.concatenate(beside(line, "gy"), axis=0)
    tables = sorted_nodes(place, near, valid)
    plane, tables = lax.optimization_barrier((plane, tables))
    code, rank, sorted_counts, tiles = tables
    below, same, above = beside(plane, GZ)
    words, units = near_words(tiles, same, code)
    latent = call(
        encoder_kernel,
        (8, 8, 1024),
        bf16,
        place,
        tiles,
        below,
        above,
        code,
        words,
        units,
        rank,
        sorted_counts,
        ki,
        km,
        kernel_out.T,
        scratch=(
            pltpu.VMEM((72, 8, 128), i32),
            pltpu.VMEM((2, 8, 8, 128), f32),
            pltpu.VMEM((8, 80, 128), f32),
        ),
        smem=2,
    )

    (ffi, ffj), (ifi, ifj), xl, yl = plane_tables()
    local = angle(1, ffi[:, None] * xl[None, :] + ffj[:, None] * yl[None, :])
    phase = ((jnp.asarray(ffi, i32) * 8 * gx + jnp.asarray(ffj, i32) * 16 * gy) % GRID).astype(f32)
    cos, sin = turned(
        np.cos(local).astype(np.float32),
        np.sin(local).astype(np.float32),
        (phase * (2.0 * math.pi / GRID))[:, None],
    )
    whi, wlo = split_two(jnp.concatenate([cos, sin], axis=1))
    local = angle(1, ifi[None, :] * xl[:, None] + ifj[None, :] * yl[:, None])
    phase = ((jnp.asarray(ifi, i32) * 8 * gx + jnp.asarray(ifj, i32) * 16 * gy) % GRID).astype(f32)
    cos, sin = turned(
        np.cos(local).astype(np.float32),
        np.sin(local).astype(np.float32),
        (phase * (2.0 * math.pi / GRID))[None, :],
    )
    back = jnp.concatenate([cos, sin], axis=0).astype(bf16)

    w = spectral.reshape(2, 2, 2, 4, 8, 8, 64).transpose(0, 4, 2, 1, 3, 5, 6)
    wr, wi = w[0], w[1]
    mixing = jnp.stack(
        [jnp.concatenate([wr, wi], axis=-1), jnp.concatenate([-wi, wr], axis=-1)], axis=3
    ).reshape(8, 256, 128)
    joint = jnp.concatenate([skip_weight, jnp.eye(64, dtype=bf16)], axis=0)

    depth = lax.all_to_all(latent, GZ, split_axis=0, concat_axis=0)
    ahi, alo = third_forward()
    partial = call(forward_kernel, (512, 128), bf16, depth, ahi, alo, whi, wlo, scratch=(pltpu.VMEM((512, 128), f32),))
    partial = lax.all_to_all(partial.reshape(256, 2, 128), ALL, split_axis=0, concat_axis=0)
    own_mask, place_mask, half = mode_masks()
    mixed = call(
        mix_kernel,
        (32, 16, 128),
        bf16,
        partial.reshape(32, 16, 128),
        mixing,
        own_mask,
        placing(),
        place_mask,
        half,
    )
    mixed = lax.all_to_all(mixed.reshape(256, 2, 128), ALL, split_axis=0, concat_axis=0)
    third = third_inverse()
    branch = call(
        inverse_kernel,
        (8, 8, 8, 128),
        bf16,
        mixed.reshape(8, 4, 16, 128),
        back,
        third[:, :256],
        third[:, 256:],
        partner_table(),
    )
    branch = lax.all_to_all(branch, GZ, split_axis=0, concat_axis=0)
    out = call(output_kernel, (128, 8, 64), f32, branch, latent, joint)
    return out.reshape(1, 8, 16, 8, 64)


def solution(mesh):
    split = Mesh(
        mesh.devices.reshape(mesh.shape["gx"], mesh.shape["gy"], 4, 2), ("gx", "gy", "gz_0", "gz_1")
    )
    return jax.shard_map(
        layer,
        mesh=split,
        in_specs=(
            P(None, None, ALL),
            P(None, "gx", "gy", GZ, None),
            P(None, "gx", "gy", GZ),
            P(),
            P(),
            P(),
            P(None, GZ, "gx", "gy", None, None),
            P(),
        ),
        out_specs=P(None, "gx", "gy", GZ, None),
        check_vma=False,
    )
```

```python
import math

import jax
import jax.numpy as jnp
import numpy as np
from jax import lax
from jax.experimental import pallas as pl
from jax.experimental.pallas import tpu as pltpu
from jax.sharding import Mesh
from jax.sharding import PartitionSpec as P

f32 = jnp.float32
bf16 = jnp.bfloat16
i32 = jnp.int32

GRID = 64
NB = 32
ROWS = 8 * NB + 32
CELLS = float(GRID**3)
NORM_FLOOR = 1.0
GZ = ("gz_0", "gz_1")
ALL = ("gx", "gy", "gz_0", "gz_1")
C0 = math.sqrt(2.0 / math.pi)
C1 = C0 * 0.044715
VMEM = pl.BlockSpec(memory_space=pltpu.VMEM)
SMEM = pl.BlockSpec(memory_space=pltpu.SMEM)


def freq(n):
    return np.where(n < 8, n, n - 16)


def angle(f, m):
    return 2.0 * math.pi * ((f * m) % GRID) / GRID


def split_two(a):
    hi = a.astype(bf16)
    lo = (a - hi.astype(a.dtype)).astype(bf16)
    return hi, lo


def third_forward():
    kh, r, kl, c = np.meshgrid(*map(np.arange, (4, 2, 4, 8)), indexing="ij")
    k, r, c = (4 * kh + kl).reshape(-1, 1), r.reshape(-1, 1), c.reshape(-1, 1)
    z = np.repeat(np.arange(64), 8)[None, :]
    cc = np.tile(np.arange(8), 64)[None, :]
    a = angle(k, z)
    v = np.where(r == 0, np.cos(a), -np.sin(a)) * (c == cc)
    return split_two(v)


def third_inverse():
    z = np.repeat(np.arange(64), 8)[:, None]
    o = np.tile(np.arange(8), 64)[:, None]
    s, kh, kl, r, oo = (
        a.reshape(1, -1) for a in np.meshgrid(*map(np.arange, (2, 4, 4, 2, 8)), indexing="ij")
    )
    k = 4 * kh + kl
    a = angle(k, z)
    w = np.where(k == 0, 1.0, 2.0) / CELLS
    cos, sin = np.cos(a), np.sin(a)
    v = np.where(s == 0, np.where(r == 0, cos, -sin), np.where(r == 0, -sin, -cos))
    return (v * w * (o == oo)).astype(bf16)


def plane_tables():
    jl, il, jh, ih = (a.reshape(-1) for a in np.meshgrid(*map(np.arange, (2, 2, 8, 8)), indexing="ij"))
    fwd = freq(2 * ih + il), freq(2 * jh + jl)
    il, jh, ih, jl = (a.reshape(-1) for a in np.meshgrid(*map(np.arange, (2, 8, 8, 2)), indexing="ij"))
    inv = freq(2 * ih + il), freq(2 * jh + jl)
    return fwd, inv, np.repeat(np.arange(8), 16), np.tile(np.arange(16), 8)


def partner_table():
    _, (fi, fj), _, _ = plane_tables()
    hit = (fi[:, None] == -fi[None, :]) & (fj[:, None] == -fj[None, :])
    return hit.astype(np.float32).astype(bf16)


def mode_masks():
    jl, il, kl = (a.reshape(-1, 1) for a in np.meshgrid(*map(np.arange, (2, 2, 4)), indexing="ij"))
    jc, ic, _, kc, _ = (
        a.reshape(1, -1) for a in np.meshgrid(*map(np.arange, (2, 2, 2, 4, 8)), indexing="ij")
    )
    own = ((jl == jc) & (il == ic) & (kl == kc)).astype(np.float32)
    _, ib, kb, _, _ = (
        a.reshape(1, -1) for a in np.meshgrid(*map(np.arange, (8, 2, 4, 2, 8)), indexing="ij")
    )
    place = ((il == ib) & (kl == kb)).astype(np.float32)
    half = np.zeros((8, 16), np.float32)
    half[jl[:, 0], np.arange(16)] = 1.0
    return own, place, half.astype(bf16)


def placing():
    ro, oh, ol = (a.reshape(-1, 1) for a in np.meshgrid(*map(np.arange, (2, 8, 8)), indexing="ij"))
    oc, _, _, rc, lc = (
        a.reshape(1, -1) for a in np.meshgrid(*map(np.arange, (8, 2, 4, 2, 8)), indexing="ij")
    )
    return ((ro == rc) & (oh == oc) & (ol == lc)).astype(np.float32).astype(bf16)


def dot(a, b):
    return jnp.dot(a, b, preferred_element_type=f32)


def dot_t(a, b):
    return lax.dot_general(a, b, (((1,), (1,)), ((), ())), preferred_element_type=f32)


def gelu_twice(v):
    return v * jnp.tanh(v * (v * v * C1 + C0)) + v


def column(line):
    return jnp.broadcast_to(line, (128, 128)).T


def rank_rows(rank, first, count):
    r = lax.broadcasted_iota(i32, (count, 1024), 0) + first
    return jnp.where(r == rank, 1.0, 0.0).astype(bf16)


def sort_kernel(place_ref, nb_ref, cnt_ref, code_ref, rank_ref, scnt_ref, tile_ref):
    px, py, pz = place_ref[0], place_ref[1], place_ref[2]
    j = nb_ref[...]
    owner = j >> 9
    dz = (owner & 7) - pz + 1
    dy = ((owner >> 3) & 3) - py + 1
    dx = (owner >> 5) - px + 1
    group = jnp.where(dz == 1, 72, (dz >> 1) * 36)
    chunk = ((group + (dy * 3 + dx) * 4 + ((j >> 7) & 3)) & 127).astype(f32)
    lane = (j & 127).astype(f32)
    counts = cnt_ref[...].astype(f32)
    row8 = lax.broadcasted_iota(i32, (8, 128), 0)
    lane8 = lax.broadcasted_iota(i32, (8, 128), 1)
    key = counts * 1024.0 - (row8 * 128 + lane8).astype(f32)
    flat = [key[z : z + 1] for z in range(8)]
    ranks = [jnp.zeros((128, 128), f32) for _ in range(8)]
    for z in range(8):
        own = column(flat[z])
        ranks = [r + jnp.where(own > line, 1.0, 0.0) for r, line in zip(ranks, flat)]
    rank = jnp.concatenate([jnp.sum(r, axis=0, keepdims=True) for r in ranks], axis=1).astype(i32)
    rank_ref[...] = jnp.broadcast_to(rank, (8, 1024))
    node = lax.broadcasted_iota(i32, (8, 1024), 1)
    wide = lax.broadcasted_iota(i32, (8, 1024), 0)
    line = jnp.concatenate([counts[z : z + 1] for z in range(8)], axis=1)
    tail = jnp.where(wide == 1, (node >> 7).astype(f32), (node & 127).astype(f32))
    tail = jnp.where(wide == 0, line, tail)
    rows = [jnp.concatenate([a[:, z, :] for z in range(8)], axis=1) for a in (chunk, lane)]
    rows = jnp.concatenate(rows + [tail], axis=0).astype(bf16)
    slot = lax.broadcasted_iota(i32, (NB, 128), 0)
    words, most = [], []
    for t in range(4):
        found = dot_t(rows, rank_rows(rank, t * 256, 256))
        tail = found[2 * NB : 2 * NB + 8]
        scnt_ref[:, t * 256 : t * 256 + 256] = jnp.broadcast_to(tail[0:1], (8, 256))
        cell = (tail[1:2] * 128.0 + tail[2:3]) * 16384.0
        word = (found[0:NB] * 128.0 + found[NB : 2 * NB] + cell).astype(i32)
        length = tail[0:1].astype(i32)
        for h in range(2):
            at = slice(h * 128, h * 128 + 128)
            words.append(jnp.where(slot < length[:, at], word[:, at], -1))
            most.append(jnp.max(length[:, at]))
    end = 0
    for t in range(8):
        code_ref[pl.ds(end, NB), :] = words[t]
        end = end + most[t]
        tile_ref[t] = end
    code_ref[pl.ds(end, 16), :] = jnp.full((16, 128), -1, i32)
    tile_ref[8] = (end + 15) >> 4


def pair_sums(place_ref, tile_ref, code_ref, look_up, ki_ref, km_ref, turn, acc_ref):
    px, py, pz = place_ref[0], place_ref[1], place_ref[2]
    x0 = px.astype(f32) * 8.0 + 0.5
    y0 = py.astype(f32) * 16.0 + 0.5
    z0 = pz.astype(f32) * 8.0 + 0.5
    turn[...] = jnp.zeros(turn.shape, f32)
    steps = tile_ref[8]
    ends = [tile_ref[t] for t in range(7)]

    def gather(b, after=(None,) * 6):
        lines = []
        for half in range(2):
            code = code_ref[pl.ds(pl.multiple_of(b * 16 + half * 8, 8), 8), :]
            cell = code >> 14
            centres = (
                (((cell >> 4) & 7).astype(f32) + x0) * (1.0 / GRID),
                ((cell & 15).astype(f32) + y0) * (1.0 / GRID),
                ((cell >> 7).astype(f32) + z0) * (1.0 / GRID),
            )
            values = look_up(code, b * 2 + half, after[half * 3 : half * 3 + 3])
            for c in range(6):
                value = values[c]
                if c < 3:
                    value = value - centres[c]
                turn[half, c] = jnp.where(code >= 0, value, 0.0)
            lines += [turn[half, :, n, :] for n in range(8)]
        return jnp.concatenate(lines, axis=1)

    def layers(pair):
        first = gelu_twice(dot(ki_ref[...], pair.astype(bf16)))
        return first, gelu_twice(dot(km_ref[...], first.astype(bf16)))

    def add(b, hidden):
        for r in range(16):
            tile = sum((b * 16 + r >= end).astype(i32) for end in ends)
            acc_ref[tile] += hidden[:, r * 128 : r * 128 + 128]

    def step(b, pair):
        first, second = layers(pair)
        after = (None,) + tuple(
            h[0:8, n * 128 : n * 128 + 128]
            for h, n in ((first, 2), (first, 8), (first, 14), (second, 4), (second, 9))
        )
        following = gather(b + 1, after)
        add(b, second)
        return following

    add(steps - 1, layers(lax.fori_loop(0, steps - 1, step, gather(0)))[1])


def lane_gather(line, at):
    return jnp.take_along_axis(jnp.broadcast_to(line, (8, 128)), at, axis=1, mode="promise_in_bounds")


def packed(parts, words):
    most = jnp.zeros((8, 128), f32)
    for part in parts:
        most = jnp.maximum(most, jnp.max(jnp.abs(part[...]), axis=0))
    most = jnp.maximum(jnp.max(most, axis=1, keepdims=True), 1e-30)
    scale = jnp.broadcast_to(32767.0 / most, (8, 128))
    unit = jnp.broadcast_to(most * (1.0 / 32767.0), (8, 128))
    for n in range(36 * len(parts)):
        q = (parts[n // 36][n % 36] * scale + 32768.5).astype(i32)
        words[n] = (q << 16) | pltpu.roll(q, 5, 0)
    return unit


def rows_of(unit):
    return [jnp.broadcast_to(unit[c : c + 1], (8, 128)) for c in range(6)]


def pick_word(words, c, code, count, after=None):
    levels = (count - 1).bit_length()
    at = code & 127
    if after is not None:
        at = jnp.where(after > 3.0e38, 0, at)
    bits = [(code & (128 << n)) != 0 for n in range(levels)]

    def pick(lo, level):
        if lo >= count:
            return None
        if level == 0:
            return lane_gather(words[lo, c : c + 1, :], at)
        first = pick(lo, level - 1)
        second = pick(lo + (1 << (level - 1)), level - 1)
        return first if second is None else jnp.where(bits[level - 1], second, first)

    return pick(0, levels)


def near_kernel(tile_ref, same_ref, code_ref, out_ref, unit_ref, words):
    unit_ref[...] = packed((same_ref,), words)

    def step(b, carry):
        for half in range(2):
            code = code_ref[pl.ds(pl.multiple_of(b * 16 + half * 8, 8), 8), :] - 72 * 128
            for c in range(3):
                out_ref[b * 2 + half, c] = pick_word(words, c, code, 36)
        return carry

    lax.fori_loop(0, tile_ref[8], step, 0)


def encoder_kernel(
    place_ref,
    tile_ref,
    below_ref,
    above_ref,
    code_ref,
    near_ref,
    unit_ref,
    rank_ref,
    scnt_ref,
    ki_ref,
    km_ref,
    ko_ref,
    out_ref,
    words,
    turn,
    acc_ref,
):
    far_units = rows_of(packed((below_ref, above_ref), words))
    near_units = rows_of(unit_ref[...])
    acc_ref[...] = jnp.zeros(acc_ref.shape, f32)

    def look_up(code, block, after):
        near = (code & 16383) >= 72 * 128
        values = [None] * 6
        for c in range(3):
            word = jnp.where(near, near_ref[block, c], pick_word(words, c, code, 72, after[c]))
            upper = jnp.where(near, near_units[c], far_units[c])
            lower = jnp.where(near, near_units[c + 3], far_units[c + 3])
            values[c] = (lax.shift_right_logical(word, 16) - 32768).astype(f32) * upper
            values[c + 3] = ((word & 65535) - 32768).astype(f32) * lower
        return values

    pair_sums(place_ref, tile_ref, code_ref, look_up, ki_ref, km_ref, turn, acc_ref)
    mean = jnp.concatenate([acc_ref[t] for t in range(8)], axis=1) * (0.5 / scnt_ref[0:1])
    upper = mean.astype(bf16)
    lower = (mean - upper.astype(f32)).astype(bf16)
    latent = (dot(ko_ref[...], upper) + dot(ko_ref[...], lower)).astype(bf16)
    rank = rank_ref[0:1]
    spread = jnp.zeros((64, 1024), f32)
    for t in range(4):
        spread = spread + dot(latent[:, t * 256 : t * 256 + 256], rank_rows(rank, t * 256, 256))
    out_ref[...] = spread.astype(bf16).reshape(8, 8, 1024)


def forward_kernel(m_ref, ahi_ref, alo_ref, whi_ref, wlo_ref, out_ref, wide):
    rows = [
        m_ref[s].astype(f32)[:, z * 128 : (z + 1) * 128] for s in range(8) for z in range(8)
    ]
    cells = jnp.concatenate(rows, axis=0).astype(bf16)
    z = dot(ahi_ref[...], cells) + dot(alo_ref[...], cells)
    right = []
    for kh in range(4):
        right += [z[kh * 64 + 32 : kh * 64 + 64], -z[kh * 64 : kh * 64 + 32]]
    both = jnp.concatenate([z, jnp.concatenate(right, axis=0)], axis=1).astype(bf16)
    p = dot_t(whi_ref[...], both) + dot_t(wlo_ref[...], both)
    for kh in range(4):
        for h in range(2):
            line = jnp.concatenate(
                [p[q * 64 : (q + 1) * 64, kh * 64 : (kh + 1) * 64] for q in (2 * h, 2 * h + 1)], axis=1
            )
            for jh in range(8):
                wide[pl.ds(((jh * 4 + kh) * 8) * 2 + h, 8, stride=2), :] = line[jh * 8 : jh * 8 + 8]
    out_ref[...] = wide[...].astype(bf16)


def mix_kernel(r_ref, w_ref, own_ref, sel_ref, place_ref, half_ref, out_ref):
    s = jnp.sum(r_ref[...].astype(f32), axis=0)
    s = s.astype(bf16).astype(f32)
    own = own_ref[...]
    g = jnp.zeros((16, 128), f32)
    for ch in range(8):
        line = jnp.concatenate([s[2 * ch : 2 * ch + 1], s[2 * ch + 1 : 2 * ch + 2]], axis=1)
        g = g + dot((line * own).astype(bf16), w_ref[ch])
    spread = dot(g.astype(bf16), sel_ref[...]) * place_ref[...]
    d = dot(half_ref[...], spread.astype(bf16))
    d = jnp.concatenate([d[0:2, oh * 128 : (oh + 1) * 128] for oh in range(8)], axis=0).astype(bf16)
    for n in range(32):
        out_ref[n] = d


def inverse_kernel(q_ref, v_ref, bc_ref, bs_ref, partner_ref, out_ref):
    blocks = []
    for kh in range(4):
        rows = jnp.concatenate([q_ref[jh, kh] for jh in range(8)], axis=0).astype(f32)
        blocks.append(jnp.concatenate([rows[:, 0:64], rows[:, 64:128]], axis=0))
    x = jnp.concatenate(blocks, axis=1)
    row = lax.broadcasted_iota(i32, (256, 256), 0)
    lane = lax.broadcasted_iota(i32, (256, 256), 1)
    x = jnp.where((row == 0) & (lane < 8), 0.0, x)
    xb = x.astype(bf16)
    twin = dot(partner_ref[...], xb[:, 0:128])
    low = lane[0:1, 0:128]
    side = jnp.where(low < 8, 0.5, jnp.where(low < 16, -0.5, 0.0))
    weight = jnp.where(lane[0:1, :] < 16, 0.5, 2.0)
    power = jnp.sum(x * x, axis=0, keepdims=True) * weight
    cross = jnp.sum(x[:, 0:128] * twin, axis=0, keepdims=True) * side
    power = jnp.broadcast_to(power[:, 0:128] + power[:, 128:256] + cross, (8, 128))
    for shift in (8, 16, 32, 64):
        power = power + pltpu.roll(power, shift, 1)
    scale = lax.rsqrt(power * (1.0 / (CELLS * CELLS)) + NORM_FLOOR)[0:1]
    scale = jnp.concatenate([scale, scale], axis=1)
    g = (dot(v_ref[...], xb) * scale).astype(bf16)
    out = dot_t(bc_ref[...], g[0:128]) + dot_t(bs_ref[...], g[128:256])
    out_ref[...] = out.astype(bf16).reshape(8, 8, 8, 128)


def output_kernel(y_ref, lat_ref, w_ref, out_ref):
    for z in range(8):
        y = jnp.concatenate([y_ref[s, z].astype(f32) for s in range(8)], axis=0)
        lat = jnp.concatenate(
            [lat_ref[s].astype(f32)[:, z * 128 : (z + 1) * 128] for s in range(8)], axis=0
        )
        both = jnp.concatenate([lat, y], axis=0).T.astype(bf16)
        v = dot(both, w_ref[...])
        out_ref[:, z, :] = 0.5 * gelu_twice(v)


def call(kernel, shape, dtype, *args, scratch=(), smem=0):
    return pl.pallas_call(
        kernel,
        out_shape=jax.ShapeDtypeStruct(shape, dtype),
        in_specs=[SMEM] * smem + [VMEM] * (len(args) - smem),
        out_specs=VMEM,
        scratch_shapes=list(scratch),
        compiler_params=pltpu.CompilerParams(vmem_limit_bytes=48 * 1024 * 1024),
    )(*args)


def sorted_nodes(place, near, valid):
    shapes = (
        ((ROWS, 128), i32),
        ((8, 1024), i32),
        ((8, 1024), f32),
        ((9,), i32),
    )
    return pl.pallas_call(
        sort_kernel,
        out_shape=[jax.ShapeDtypeStruct(*s) for s in shapes],
        in_specs=[SMEM, VMEM, VMEM],
        out_specs=[VMEM] * 3 + [SMEM],
        compiler_params=pltpu.CompilerParams(vmem_limit_bytes=48 * 1024 * 1024),
        name="sort",
    )(place, near, valid)


def near_words(tiles, same, code):
    shapes = (((ROWS // 8, 3, 8, 128), i32), ((8, 128), f32))
    return pl.pallas_call(
        near_kernel,
        out_shape=[jax.ShapeDtypeStruct(*s) for s in shapes],
        in_specs=[SMEM, VMEM, VMEM],
        out_specs=[VMEM] * 2,
        scratch_shapes=[pltpu.VMEM((36, 8, 128), i32)],
        compiler_params=pltpu.CompilerParams(vmem_limit_bytes=48 * 1024 * 1024),
        name="near",
    )(tiles, same, code)


def beside(cells, axis):
    count = lax.axis_size(axis)
    ends = count - 1
    lower = lax.ppermute(cells, axis, [(i, i + 1) for i in range(ends)])
    upper = lax.ppermute(cells, axis, [(i + 1, i) for i in range(ends)])
    return lower, cells, upper


def turned(cos, sin, phase):
    c, s = jnp.cos(phase), jnp.sin(phase)
    return cos * c - sin * s, sin * c + cos * s


def layer(point_data, neighbours, counts, kernel_in, kernel_mid, kernel_out, spectral, skip_weight):
    gx = lax.axis_index("gx")
    gy = lax.axis_index("gy")
    gz = lax.axis_index(GZ)
    place = jnp.stack([gx, gy, gz]).astype(i32)

    own = jnp.pad(point_data[0].reshape(6, 4, 128).transpose(1, 0, 2), ((0, 0), (0, 2), (0, 0)))
    near = neighbours[0].transpose(3, 2, 0, 1).reshape(NB, 8, 128)
    valid = counts[0].transpose(2, 0, 1).reshape(8, 128)
    ki = jnp.pad(kernel_in.T, ((0, 0), (0, 2)))
    km = kernel_mid.T * jnp.bfloat16(0.5)

    line = jnp.concatenate(beside(own, "gx"), axis=0)
    plane = jnp.concatenate(beside(line, "gy"), axis=0)
    tables = sorted_nodes(place, near, valid)
    plane, tables = lax.optimization_barrier((plane, tables))
    code, rank, sorted_counts, tiles = tables
    below, same, above = beside(plane, GZ)
    words, units = near_words(tiles, same, code)
    latent = call(
        encoder_kernel,
        (8, 8, 1024),
        bf16,
        place,
        tiles,
        below,
        above,
        code,
        words,
        units,
        rank,
        sorted_counts,
        ki,
        km,
        kernel_out.T,
        scratch=(
            pltpu.VMEM((72, 8, 128), i32),
            pltpu.VMEM((2, 8, 8, 128), f32),
            pltpu.VMEM((8, 80, 128), f32),
        ),
        smem=2,
    )

    (ffi, ffj), (ifi, ifj), xl, yl = plane_tables()
    local = angle(1, ffi[:, None] * xl[None, :] + ffj[:, None] * yl[None, :])
    phase = ((jnp.asarray(ffi, i32) * 8 * gx + jnp.asarray(ffj, i32) * 16 * gy) % GRID).astype(f32)
    cos, sin = turned(
        np.cos(local).astype(np.float32),
        np.sin(local).astype(np.float32),
        (phase * (2.0 * math.pi / GRID))[:, None],
    )
    whi, wlo = split_two(jnp.concatenate([cos, sin], axis=1))
    local = angle(1, ifi[None, :] * xl[:, None] + ifj[None, :] * yl[:, None])
    phase = ((jnp.asarray(ifi, i32) * 8 * gx + jnp.asarray(ifj, i32) * 16 * gy) % GRID).astype(f32)
    cos, sin = turned(
        np.cos(local).astype(np.float32),
        np.sin(local).astype(np.float32),
        (phase * (2.0 * math.pi / GRID))[None, :],
    )
    back = jnp.concatenate([cos, sin], axis=0).astype(bf16)

    w = spectral.reshape(2, 2, 2, 4, 8, 8, 64).transpose(0, 4, 2, 1, 3, 5, 6)
    wr, wi = w[0], w[1]
    mixing = jnp.stack(
        [jnp.concatenate([wr, wi], axis=-1), jnp.concatenate([-wi, wr], axis=-1)], axis=3
    ).reshape(8, 256, 128)
    joint = jnp.concatenate([skip_weight, jnp.eye(64, dtype=bf16)], axis=0)

    depth = lax.all_to_all(latent, GZ, split_axis=0, concat_axis=0)
    ahi, alo = third_forward()
    partial = call(forward_kernel, (512, 128), bf16, depth, ahi, alo, whi, wlo, scratch=(pltpu.VMEM((512, 128), f32),))
    partial = lax.all_to_all(partial.reshape(256, 2, 128), ALL, split_axis=0, concat_axis=0)
    own_mask, place_mask, half = mode_masks()
    mixed = call(
        mix_kernel,
        (32, 16, 128),
        bf16,
        partial.reshape(32, 16, 128),
        mixing,
        own_mask,
        placing(),
        place_mask,
        half,
    )
    mixed = lax.all_to_all(mixed.reshape(256, 2, 128), ALL, split_axis=0, concat_axis=0)
    third = third_inverse()
    branch = call(
        inverse_kernel,
        (8, 8, 8, 128),
        bf16,
        mixed.reshape(8, 4, 16, 128),
        back,
        third[:, :256],
        third[:, 256:],
        partner_table(),
    )
    branch = lax.all_to_all(branch, GZ, split_axis=0, concat_axis=0)
    out = call(output_kernel, (128, 8, 64), f32, branch, latent, joint)
    return out.reshape(1, 8, 16, 8, 64)


def solution(mesh):
    split = Mesh(
        mesh.devices.reshape(mesh.shape["gx"], mesh.shape["gy"], 4, 2), ("gx", "gy", "gz_0", "gz_1")
    )
    return jax.shard_map(
        layer,
        mesh=split,
        in_specs=(
            P(None, None, ALL),
            P(None, "gx", "gy", GZ, None),
            P(None, "gx", "gy", GZ),
            P(),
            P(),
            P(),
            P(None, GZ, "gx", "gy", None, None),
            P(),
        ),
        out_specs=P(None, "gx", "gy", GZ, None),
        check_vma=False,
    )
```

```python
import math

import jax
import jax.numpy as jnp
import numpy as np
from jax import lax
from jax.experimental import pallas as pl
from jax.experimental.pallas import tpu as pltpu
from jax.sharding import Mesh
from jax.sharding import PartitionSpec as P

f32 = jnp.float32
bf16 = jnp.bfloat16
i32 = jnp.int32

GRID = 64
NB = 32
ROWS = 8 * NB + 32
CELLS = float(GRID**3)
NORM_FLOOR = 1.0
GZ = ("gz_0", "gz_1")
ALL = ("gx", "gy", "gz_0", "gz_1")
C0 = math.sqrt(2.0 / math.pi)
C1 = C0 * 0.044715
VMEM = pl.BlockSpec(memory_space=pltpu.VMEM)
SMEM = pl.BlockSpec(memory_space=pltpu.SMEM)


def freq(n):
    return np.where(n < 8, n, n - 16)


def angle(f, m):
    return 2.0 * math.pi * ((f * m) % GRID) / GRID


def split_two(a):
    hi = a.astype(bf16)
    lo = (a - hi.astype(a.dtype)).astype(bf16)
    return hi, lo


def third_forward():
    kh, r, kl, c = np.meshgrid(*map(np.arange, (4, 2, 4, 8)), indexing="ij")
    k, r, c = (4 * kh + kl).reshape(-1, 1), r.reshape(-1, 1), c.reshape(-1, 1)
    z = np.repeat(np.arange(64), 8)[None, :]
    cc = np.tile(np.arange(8), 64)[None, :]
    a = angle(k, z)
    v = np.where(r == 0, np.cos(a), -np.sin(a)) * (c == cc)
    return split_two(v)


def third_inverse():
    z = np.repeat(np.arange(64), 8)[:, None]
    o = np.tile(np.arange(8), 64)[:, None]
    s, kh, kl, r, oo = (
        a.reshape(1, -1) for a in np.meshgrid(*map(np.arange, (2, 4, 4, 2, 8)), indexing="ij")
    )
    k = 4 * kh + kl
    a = angle(k, z)
    w = np.where(k == 0, 1.0, 2.0) / CELLS
    cos, sin = np.cos(a), np.sin(a)
    v = np.where(s == 0, np.where(r == 0, cos, -sin), np.where(r == 0, -sin, -cos))
    return (v * w * (o == oo)).astype(bf16)


def plane_tables():
    jl, il, jh, ih = (a.reshape(-1) for a in np.meshgrid(*map(np.arange, (2, 2, 8, 8)), indexing="ij"))
    fwd = freq(2 * ih + il), freq(2 * jh + jl)
    il, jh, ih, jl = (a.reshape(-1) for a in np.meshgrid(*map(np.arange, (2, 8, 8, 2)), indexing="ij"))
    inv = freq(2 * ih + il), freq(2 * jh + jl)
    return fwd, inv, np.repeat(np.arange(8), 16), np.tile(np.arange(16), 8)


def partner_table():
    _, (fi, fj), _, _ = plane_tables()
    hit = (fi[:, None] == -fi[None, :]) & (fj[:, None] == -fj[None, :])
    return hit.astype(np.float32).astype(bf16)


def mode_masks():
    jl, il, kl = (a.reshape(-1, 1) for a in np.meshgrid(*map(np.arange, (2, 2, 4)), indexing="ij"))
    jc, ic, _, kc, _ = (
        a.reshape(1, -1) for a in np.meshgrid(*map(np.arange, (2, 2, 2, 4, 8)), indexing="ij")
    )
    own = ((jl == jc) & (il == ic) & (kl == kc)).astype(np.float32)
    _, ib, kb, _, _ = (
        a.reshape(1, -1) for a in np.meshgrid(*map(np.arange, (8, 2, 4, 2, 8)), indexing="ij")
    )
    place = ((il == ib) & (kl == kb)).astype(np.float32)
    half = np.zeros((8, 16), np.float32)
    half[jl[:, 0], np.arange(16)] = 1.0
    return own, place, half.astype(bf16)


def placing():
    ro, oh, ol = (a.reshape(-1, 1) for a in np.meshgrid(*map(np.arange, (2, 8, 8)), indexing="ij"))
    oc, _, _, rc, lc = (
        a.reshape(1, -1) for a in np.meshgrid(*map(np.arange, (8, 2, 4, 2, 8)), indexing="ij")
    )
    return ((ro == rc) & (oh == oc) & (ol == lc)).astype(np.float32).astype(bf16)


def dot(a, b):
    return jnp.dot(a, b, preferred_element_type=f32)


def dot_t(a, b):
    return lax.dot_general(a, b, (((1,), (1,)), ((), ())), preferred_element_type=f32)


def gelu_twice(v):
    return v * jnp.tanh(v * (v * v * C1 + C0)) + v


def column(line):
    return jnp.broadcast_to(line, (128, 128)).T


def rank_rows(rank, first, count):
    r = lax.broadcasted_iota(i32, (count, 1024), 0) + first
    return jnp.where(r == rank, 1.0, 0.0).astype(bf16)


def sort_kernel(place_ref, nb_ref, cnt_ref, code_ref, rank_ref, scnt_ref, tile_ref):
    px, py, pz = place_ref[0], place_ref[1], place_ref[2]
    j = nb_ref[...]
    owner = j >> 9
    dz = (owner & 7) - pz + 1
    dy = ((owner >> 3) & 3) - py + 1
    dx = (owner >> 5) - px + 1
    group = jnp.where(dz == 1, 72, (dz >> 1) * 36)
    chunk = ((group + (dy * 3 + dx) * 4 + ((j >> 7) & 3)) & 127).astype(f32)
    lane = (j & 127).astype(f32)
    counts = cnt_ref[...].astype(f32)
    row8 = lax.broadcasted_iota(i32, (8, 128), 0)
    lane8 = lax.broadcasted_iota(i32, (8, 128), 1)
    key = counts * 1024.0 - (row8 * 128 + lane8).astype(f32)
    flat = [key[z : z + 1] for z in range(8)]
    ranks = [jnp.zeros((128, 128), f32) for _ in range(8)]
    for z in range(8):
        own = column(flat[z])
        ranks = [r + jnp.where(own > line, 1.0, 0.0) for r, line in zip(ranks, flat)]
    rank = jnp.concatenate([jnp.sum(r, axis=0, keepdims=True) for r in ranks], axis=1).astype(i32)
    rank_ref[...] = jnp.broadcast_to(rank, (8, 1024))
    node = lax.broadcasted_iota(i32, (8, 1024), 1)
    wide = lax.broadcasted_iota(i32, (8, 1024), 0)
    line = jnp.concatenate([counts[z : z + 1] for z in range(8)], axis=1)
    tail = jnp.where(wide == 1, (node >> 7).astype(f32), (node & 127).astype(f32))
    tail = jnp.where(wide == 0, line, tail)
    rows = [jnp.concatenate([a[:, z, :] for z in range(8)], axis=1) for a in (chunk, lane)]
    rows = jnp.concatenate(rows + [tail], axis=0).astype(bf16)
    slot = lax.broadcasted_iota(i32, (NB, 128), 0)
    words, most = [], []
    for t in range(4):
        found = dot_t(rows, rank_rows(rank, t * 256, 256))
        tail = found[2 * NB : 2 * NB + 8]
        scnt_ref[:, t * 256 : t * 256 + 256] = jnp.broadcast_to(tail[0:1], (8, 256))
        cell = (tail[1:2] * 128.0 + tail[2:3]) * 16384.0
        word = (found[0:NB] * 128.0 + found[NB : 2 * NB] + cell).astype(i32)
        length = tail[0:1].astype(i32)
        for h in range(2):
            at = slice(h * 128, h * 128 + 128)
            words.append(jnp.where(slot < length[:, at], word[:, at], -1))
            most.append(jnp.max(length[:, at]))
    end = 0
    for t in range(8):
        code_ref[pl.ds(end, NB), :] = words[t]
        end = end + most[t]
        tile_ref[t] = end
    code_ref[pl.ds(end, 16), :] = jnp.full((16, 128), -1, i32)
    tile_ref[8] = (end + 15) >> 4


def pair_sums(place_ref, tile_ref, code_ref, look_up, ki_ref, km_ref, turn, acc_ref):
    px, py, pz = place_ref[0], place_ref[1], place_ref[2]
    x0 = px.astype(f32) * 8.0 + 0.5
    y0 = py.astype(f32) * 16.0 + 0.5
    z0 = pz.astype(f32) * 8.0 + 0.5
    turn[...] = jnp.zeros(turn.shape, f32)
    steps = tile_ref[8]
    ends = [tile_ref[t] for t in range(7)]

    def gather(b):
        lines = []
        for half in range(2):
            code = code_ref[pl.ds(pl.multiple_of(b * 16 + half * 8, 8), 8), :]
            cell = code >> 14
            centres = (
                (((cell >> 4) & 7).astype(f32) + x0) * (1.0 / GRID),
                ((cell & 15).astype(f32) + y0) * (1.0 / GRID),
                ((cell >> 7).astype(f32) + z0) * (1.0 / GRID),
            )
            values = look_up(code, b * 2 + half)
            for c in range(6):
                value = values[c]
                if c < 3:
                    value = value - centres[c]
                turn[half, c] = jnp.where(code >= 0, value, 0.0)
            lines += [turn[half, :, n, :] for n in range(8)]
        return jnp.concatenate(lines, axis=1)

    def add(b, pair):
        hidden = gelu_twice(dot(ki_ref[...], pair.astype(bf16))).astype(bf16)
        hidden = gelu_twice(dot(km_ref[...], hidden))
        for r in range(16):
            tile = sum((b * 16 + r >= end).astype(i32) for end in ends)
            acc_ref[tile] += hidden[:, r * 128 : r * 128 + 128]

    def step(b, pair):
        following = gather(b + 1)
        add(b, pair)
        return following

    add(steps - 1, lax.fori_loop(0, steps - 1, step, gather(0)))


def lane_gather(line, at):
    return jnp.take_along_axis(jnp.broadcast_to(line, (8, 128)), at, axis=1, mode="promise_in_bounds")


def packed(parts, words):
    most = jnp.zeros((24, 128), f32)
    for part in parts:
        most = jnp.maximum(most, jnp.max(jnp.abs(part[...]), axis=0))
    most = jnp.maximum(jnp.max(most, axis=1, keepdims=True), 1e-30)
    place = jnp.broadcast_to(jnp.max(most[0:12], axis=0, keepdims=True), (12, 128))
    normal = jnp.broadcast_to(jnp.max(most[12:24], axis=0, keepdims=True), (12, 128))
    upper, lower = 32767.0 / place, 32767.0 / normal
    for n in range(9 * len(parts)):
        part = parts[n // 9]
        p = (part[n % 9, 0:12] * upper + 32768.5).astype(i32)
        q = (part[n % 9, 12:24] * lower + 32768.5).astype(i32)
        words[n] = (p << 16) | q
    return place[0:8] * (1.0 / 32767.0), normal[0:8] * (1.0 / 32767.0)


def pick_word(words, c, code, count):
    levels = (count - 1).bit_length()
    at = code & 127
    bits = [(code & (128 << n)) != 0 for n in range(levels)]

    def pick(lo, level):
        if lo >= count:
            return None
        if level == 0:
            row = c * 4 + lo % 4
            return lane_gather(words[lo // 4, row : row + 1, :], at)
        first = pick(lo, level - 1)
        second = pick(lo + (1 << (level - 1)), level - 1)
        return first if second is None else jnp.where(bits[level - 1], second, first)

    return pick(0, levels)


def near_kernel(tile_ref, same_ref, code_ref, out_ref, unit_ref, words):
    unit_ref[0], unit_ref[1] = packed((same_ref,), words)

    def step(b, carry):
        for half in range(2):
            code = code_ref[pl.ds(pl.multiple_of(b * 16 + half * 8, 8), 8), :] - 72 * 128
            for c in range(3):
                out_ref[b * 2 + half, c] = pick_word(words, c, code, 36)
        return carry

    lax.fori_loop(0, tile_ref[8], step, 0)


def encoder_kernel(
    place_ref,
    tile_ref,
    below_ref,
    above_ref,
    code_ref,
    near_ref,
    unit_ref,
    rank_ref,
    scnt_ref,
    ki_ref,
    km_ref,
    ko_ref,
    out_ref,
    words,
    turn,
    acc_ref,
):
    far_place, far_normal = packed((below_ref, above_ref), words)
    near_place, near_normal = unit_ref[0], unit_ref[1]
    acc_ref[...] = jnp.zeros(acc_ref.shape, f32)

    def look_up(code, block):
        near = (code & 16383) >= 72 * 128
        upper = jnp.where(near, near_place, far_place)
        lower = jnp.where(near, near_normal, far_normal)
        values = [None] * 6
        for c in range(3):
            word = jnp.where(near, near_ref[block, c], pick_word(words, c, code, 72))
            values[c] = (lax.shift_right_logical(word, 16) - 32768).astype(f32) * upper
            values[c + 3] = ((word & 65535) - 32768).astype(f32) * lower
        return values

    pair_sums(place_ref, tile_ref, code_ref, look_up, ki_ref, km_ref, turn, acc_ref)
    mean = jnp.concatenate([acc_ref[t] for t in range(8)], axis=1) * (0.5 / scnt_ref[0:1])
    upper = mean.astype(bf16)
    lower = (mean - upper.astype(f32)).astype(bf16)
    latent = (dot(ko_ref[...], upper) + dot(ko_ref[...], lower)).astype(bf16)
    rank = rank_ref[0:1]
    spread = jnp.zeros((64, 1024), f32)
    for t in range(4):
        spread = spread + dot(latent[:, t * 256 : t * 256 + 256], rank_rows(rank, t * 256, 256))
    out_ref[...] = spread.astype(bf16).reshape(8, 8, 1024)


def forward_kernel(m_ref, ahi_ref, alo_ref, whi_ref, wlo_ref, out_ref, wide):
    rows = [
        m_ref[s].astype(f32)[:, z * 128 : (z + 1) * 128] for s in range(8) for z in range(8)
    ]
    cells = jnp.concatenate(rows, axis=0).astype(bf16)
    z = dot(ahi_ref[...], cells) + dot(alo_ref[...], cells)
    right = []
    for kh in range(4):
        right += [z[kh * 64 + 32 : kh * 64 + 64], -z[kh * 64 : kh * 64 + 32]]
    both = jnp.concatenate([z, jnp.concatenate(right, axis=0)], axis=1).astype(bf16)
    p = dot_t(whi_ref[...], both) + dot_t(wlo_ref[...], both)
    for kh in range(4):
        for h in range(2):
            line = jnp.concatenate(
                [p[q * 64 : (q + 1) * 64, kh * 64 : (kh + 1) * 64] for q in (2 * h, 2 * h + 1)], axis=1
            )
            for jh in range(8):
                wide[pl.ds(((jh * 4 + kh) * 8) * 2 + h, 8, stride=2), :] = line[jh * 8 : jh * 8 + 8]
    out_ref[...] = wide[...].astype(bf16)


def mix_kernel(r_ref, w_ref, own_ref, sel_ref, place_ref, half_ref, out_ref):
    s = jnp.sum(r_ref[...].astype(f32), axis=0)
    s = s.astype(bf16).astype(f32)
    own = own_ref[...]
    g = jnp.zeros((16, 128), f32)
    for ch in range(8):
        line = jnp.concatenate([s[2 * ch : 2 * ch + 1], s[2 * ch + 1 : 2 * ch + 2]], axis=1)
        g = g + dot((line * own).astype(bf16), w_ref[ch])
    spread = dot(g.astype(bf16), sel_ref[...]) * place_ref[...]
    d = dot(half_ref[...], spread.astype(bf16))
    d = jnp.concatenate([d[0:2, oh * 128 : (oh + 1) * 128] for oh in range(8)], axis=0).astype(bf16)
    for n in range(32):
        out_ref[n] = d


def inverse_kernel(q_ref, v_ref, bc_ref, bs_ref, partner_ref, out_ref):
    blocks = []
    for kh in range(4):
        rows = jnp.concatenate([q_ref[jh, kh] for jh in range(8)], axis=0).astype(f32)
        blocks.append(jnp.concatenate([rows[:, 0:64], rows[:, 64:128]], axis=0))
    x = jnp.concatenate(blocks, axis=1)
    row = lax.broadcasted_iota(i32, (256, 256), 0)
    lane = lax.broadcasted_iota(i32, (256, 256), 1)
    x = jnp.where((row == 0) & (lane < 8), 0.0, x)
    xb = x.astype(bf16)
    twin = dot(partner_ref[...], xb[:, 0:128])
    low = lane[0:1, 0:128]
    side = jnp.where(low < 8, 0.5, jnp.where(low < 16, -0.5, 0.0))
    weight = jnp.where(lane[0:1, :] < 16, 0.5, 2.0)
    power = jnp.sum(x * x, axis=0, keepdims=True) * weight
    cross = jnp.sum(x[:, 0:128] * twin, axis=0, keepdims=True) * side
    power = jnp.broadcast_to(power[:, 0:128] + power[:, 128:256] + cross, (8, 128))
    for shift in (8, 16, 32, 64):
        power = power + pltpu.roll(power, shift, 1)
    scale = lax.rsqrt(power * (1.0 / (CELLS * CELLS)) + NORM_FLOOR)[0:1]
    scale = jnp.concatenate([scale, scale], axis=1)
    g = (dot(v_ref[...], xb) * scale).astype(bf16)
    out = dot_t(bc_ref[...], g[0:128]) + dot_t(bs_ref[...], g[128:256])
    out_ref[...] = out.astype(bf16).reshape(8, 8, 8, 128)


def output_kernel(y_ref, lat_ref, w_ref, out_ref):
    for z in range(8):
        y = jnp.concatenate([y_ref[s, z].astype(f32) for s in range(8)], axis=0)
        lat = jnp.concatenate(
            [lat_ref[s].astype(f32)[:, z * 128 : (z + 1) * 128] for s in range(8)], axis=0
        )
        both = jnp.concatenate([lat, y], axis=0).T.astype(bf16)
        v = dot(both, w_ref[...])
        out_ref[:, z, :] = 0.5 * gelu_twice(v)


def call(kernel, shape, dtype, *args, scratch=(), smem=0):
    return pl.pallas_call(
        kernel,
        out_shape=jax.ShapeDtypeStruct(shape, dtype),
        in_specs=[SMEM] * smem + [VMEM] * (len(args) - smem),
        out_specs=VMEM,
        scratch_shapes=list(scratch),
        compiler_params=pltpu.CompilerParams(vmem_limit_bytes=48 * 1024 * 1024),
    )(*args)


def sorted_nodes(place, near, valid):
    shapes = (
        ((ROWS, 128), i32),
        ((8, 1024), i32),
        ((8, 1024), f32),
        ((9,), i32),
    )
    return pl.pallas_call(
        sort_kernel,
        out_shape=[jax.ShapeDtypeStruct(*s) for s in shapes],
        in_specs=[SMEM, VMEM, VMEM],
        out_specs=[VMEM] * 3 + [SMEM],
        compiler_params=pltpu.CompilerParams(vmem_limit_bytes=48 * 1024 * 1024),
        name="sort",
    )(place, near, valid)


def near_words(tiles, same, code):
    shapes = (((ROWS // 8, 3, 8, 128), i32), ((2, 8, 128), f32))
    return pl.pallas_call(
        near_kernel,
        out_shape=[jax.ShapeDtypeStruct(*s) for s in shapes],
        in_specs=[SMEM, VMEM, VMEM],
        out_specs=[VMEM] * 2,
        scratch_shapes=[pltpu.VMEM((9, 12, 128), i32)],
        compiler_params=pltpu.CompilerParams(vmem_limit_bytes=48 * 1024 * 1024),
        name="near",
    )(tiles, same, code)


def beside(cells, axis):
    count = lax.axis_size(axis)
    ends = count - 1
    lower = lax.ppermute(cells, axis, [(i, i + 1) for i in range(ends)])
    upper = lax.ppermute(cells, axis, [(i + 1, i) for i in range(ends)])
    return lower, cells, upper


def turned(cos, sin, phase):
    c, s = jnp.cos(phase), jnp.sin(phase)
    return cos * c - sin * s, sin * c + cos * s


def layer(point_data, neighbours, counts, kernel_in, kernel_mid, kernel_out, spectral, skip_weight):
    gx = lax.axis_index("gx")
    gy = lax.axis_index("gy")
    gz = lax.axis_index(GZ)
    place = jnp.stack([gx, gy, gz]).astype(i32)

    own = point_data.reshape(1, 24, 128)
    near = neighbours[0].transpose(3, 2, 0, 1).reshape(NB, 8, 128)
    valid = counts[0].transpose(2, 0, 1).reshape(8, 128)
    ki = jnp.pad(kernel_in.T, ((0, 0), (0, 2)))
    km = kernel_mid.T * jnp.bfloat16(0.5)

    line = jnp.concatenate(beside(own, "gx"), axis=0)
    plane = jnp.concatenate(beside(line, "gy"), axis=0)
    tables = sorted_nodes(place, near, valid)
    plane, tables = lax.optimization_barrier((plane, tables))
    code, rank, sorted_counts, tiles = tables
    below, same, above = beside(plane, GZ)
    words, units = near_words(tiles, same, code)
    latent = call(
        encoder_kernel,
        (8, 8, 1024),
        bf16,
        place,
        tiles,
        below,
        above,
        code,
        words,
        units,
        rank,
        sorted_counts,
        ki,
        km,
        kernel_out.T,
        scratch=(
            pltpu.VMEM((18, 12, 128), i32),
            pltpu.VMEM((2, 8, 8, 128), f32),
            pltpu.VMEM((8, 80, 128), f32),
        ),
        smem=2,
    )

    (ffi, ffj), (ifi, ifj), xl, yl = plane_tables()
    local = angle(1, ffi[:, None] * xl[None, :] + ffj[:, None] * yl[None, :])
    phase = ((jnp.asarray(ffi, i32) * 8 * gx + jnp.asarray(ffj, i32) * 16 * gy) % GRID).astype(f32)
    cos, sin = turned(
        np.cos(local).astype(np.float32),
        np.sin(local).astype(np.float32),
        (phase * (2.0 * math.pi / GRID))[:, None],
    )
    whi, wlo = split_two(jnp.concatenate([cos, sin], axis=1))
    local = angle(1, ifi[None, :] * xl[:, None] + ifj[None, :] * yl[:, None])
    phase = ((jnp.asarray(ifi, i32) * 8 * gx + jnp.asarray(ifj, i32) * 16 * gy) % GRID).astype(f32)
    cos, sin = turned(
        np.cos(local).astype(np.float32),
        np.sin(local).astype(np.float32),
        (phase * (2.0 * math.pi / GRID))[None, :],
    )
    back = jnp.concatenate([cos, sin], axis=0).astype(bf16)

    w = spectral.reshape(2, 2, 2, 4, 8, 8, 64).transpose(0, 4, 2, 1, 3, 5, 6)
    wr, wi = w[0], w[1]
    mixing = jnp.stack(
        [jnp.concatenate([wr, wi], axis=-1), jnp.concatenate([-wi, wr], axis=-1)], axis=3
    ).reshape(8, 256, 128)
    joint = jnp.concatenate([skip_weight, jnp.eye(64, dtype=bf16)], axis=0)

    depth = lax.all_to_all(latent, GZ, split_axis=0, concat_axis=0)
    ahi, alo = third_forward()
    partial = call(forward_kernel, (512, 128), bf16, depth, ahi, alo, whi, wlo, scratch=(pltpu.VMEM((512, 128), f32),))
    partial = lax.all_to_all(partial.reshape(256, 2, 128), ALL, split_axis=0, concat_axis=0)
    own_mask, place_mask, half = mode_masks()
    mixed = call(
        mix_kernel,
        (32, 16, 128),
        bf16,
        partial.reshape(32, 16, 128),
        mixing,
        own_mask,
        placing(),
        place_mask,
        half,
    )
    mixed = lax.all_to_all(mixed.reshape(256, 2, 128), ALL, split_axis=0, concat_axis=0)
    third = third_inverse()
    branch = call(
        inverse_kernel,
        (8, 8, 8, 128),
        bf16,
        mixed.reshape(8, 4, 16, 128),
        back,
        third[:, :256],
        third[:, 256:],
        partner_table(),
    )
    branch = lax.all_to_all(branch, GZ, split_axis=0, concat_axis=0)
    out = call(output_kernel, (128, 8, 64), f32, branch, latent, joint)
    return out.reshape(1, 8, 16, 8, 64)


def solution(mesh):
    split = Mesh(
        mesh.devices.reshape(mesh.shape["gx"], mesh.shape["gy"], 4, 2), ("gx", "gy", "gz_0", "gz_1")
    )
    return jax.shard_map(
        layer,
        mesh=split,
        in_specs=(
            P(None, None, ALL),
            P(None, "gx", "gy", GZ, None),
            P(None, "gx", "gy", GZ),
            P(),
            P(),
            P(),
            P(None, GZ, "gx", "gy", None, None),
            P(),
        ),
        out_specs=P(None, "gx", "gy", GZ, None),
        check_vma=False,
    )
```

```python
import math

import jax
import jax.numpy as jnp
import numpy as np
from jax import lax
from jax.experimental import pallas as pl
from jax.experimental.pallas import tpu as pltpu
from jax.sharding import Mesh
from jax.sharding import PartitionSpec as P

f32 = jnp.float32
bf16 = jnp.bfloat16
i32 = jnp.int32

GRID = 64
NB = 32
ROWS = 8 * NB + 32
CELLS = float(GRID**3)
NORM_FLOOR = 1.0
GZ = ("gz_0", "gz_1")
ALL = ("gx", "gy", "gz_0", "gz_1")
C0 = math.sqrt(2.0 / math.pi)
C1 = C0 * 0.044715
VMEM = pl.BlockSpec(memory_space=pltpu.VMEM)
SMEM = pl.BlockSpec(memory_space=pltpu.SMEM)


def freq(n):
    return np.where(n < 8, n, n - 16)


def angle(f, m):
    return 2.0 * math.pi * ((f * m) % GRID) / GRID


def split_two(a):
    hi = a.astype(bf16)
    lo = (a - hi.astype(a.dtype)).astype(bf16)
    return hi, lo


def third_forward():
    kh, r, kl, c = np.meshgrid(*map(np.arange, (4, 2, 4, 8)), indexing="ij")
    k, r, c = (4 * kh + kl).reshape(-1, 1), r.reshape(-1, 1), c.reshape(-1, 1)
    z = np.repeat(np.arange(64), 8)[None, :]
    cc = np.tile(np.arange(8), 64)[None, :]
    a = angle(k, z)
    v = np.where(r == 0, np.cos(a), -np.sin(a)) * (c == cc)
    return split_two(v)


def third_inverse():
    z = np.repeat(np.arange(64), 8)[:, None]
    o = np.tile(np.arange(8), 64)[:, None]
    s, kh, kl, r, oo = (
        a.reshape(1, -1) for a in np.meshgrid(*map(np.arange, (2, 4, 4, 2, 8)), indexing="ij")
    )
    k = 4 * kh + kl
    a = angle(k, z)
    w = np.where(k == 0, 1.0, 2.0) / CELLS
    cos, sin = np.cos(a), np.sin(a)
    v = np.where(s == 0, np.where(r == 0, cos, -sin), np.where(r == 0, -sin, -cos))
    return (v * w * (o == oo)).astype(bf16)


def plane_tables():
    jl, il, jh, ih = (a.reshape(-1) for a in np.meshgrid(*map(np.arange, (2, 2, 8, 8)), indexing="ij"))
    fwd = freq(2 * ih + il), freq(2 * jh + jl)
    il, jh, ih, jl = (a.reshape(-1) for a in np.meshgrid(*map(np.arange, (2, 8, 8, 2)), indexing="ij"))
    inv = freq(2 * ih + il), freq(2 * jh + jl)
    return fwd, inv, np.repeat(np.arange(8), 16), np.tile(np.arange(16), 8)


def partner_table():
    _, (fi, fj), _, _ = plane_tables()
    hit = (fi[:, None] == -fi[None, :]) & (fj[:, None] == -fj[None, :])
    return hit.astype(np.float32).astype(bf16)


def mode_masks():
    jl, il, kl = (a.reshape(-1, 1) for a in np.meshgrid(*map(np.arange, (2, 2, 4)), indexing="ij"))
    jc, ic, _, kc, _ = (
        a.reshape(1, -1) for a in np.meshgrid(*map(np.arange, (2, 2, 2, 4, 8)), indexing="ij")
    )
    own = ((jl == jc) & (il == ic) & (kl == kc)).astype(np.float32)
    _, ib, kb, _, _ = (
        a.reshape(1, -1) for a in np.meshgrid(*map(np.arange, (8, 2, 4, 2, 8)), indexing="ij")
    )
    place = ((il == ib) & (kl == kb)).astype(np.float32)
    half = np.zeros((8, 16), np.float32)
    half[jl[:, 0], np.arange(16)] = 1.0
    return own, place, half.astype(bf16)


def placing():
    ro, oh, ol = (a.reshape(-1, 1) for a in np.meshgrid(*map(np.arange, (2, 8, 8)), indexing="ij"))
    oc, _, _, rc, lc = (
        a.reshape(1, -1) for a in np.meshgrid(*map(np.arange, (8, 2, 4, 2, 8)), indexing="ij")
    )
    return ((ro == rc) & (oh == oc) & (ol == lc)).astype(np.float32).astype(bf16)


def dot(a, b):
    return jnp.dot(a, b, preferred_element_type=f32)


def dot_t(a, b):
    return lax.dot_general(a, b, (((1,), (1,)), ((), ())), preferred_element_type=f32)


def gelu_twice(v):
    return v * jnp.tanh(v * (v * v * C1 + C0)) + v


def column(line):
    return jnp.broadcast_to(line, (128, 128)).T


def rank_rows(rank, first, count):
    r = lax.broadcasted_iota(i32, (count, 1024), 0) + first
    return jnp.where(r == rank, 1.0, 0.0).astype(bf16)


def sort_kernel(place_ref, nb_ref, cnt_ref, code_ref, rank_ref, scnt_ref, tile_ref):
    px, py, pz = place_ref[0], place_ref[1], place_ref[2]
    j = nb_ref[...]
    owner = j >> 9
    dz = (owner & 7) - pz + 1
    dy = ((owner >> 3) & 3) - py + 1
    dx = (owner >> 5) - px + 1
    group = jnp.where(dz == 1, 72, (dz >> 1) * 36)
    chunk = ((group + (dy * 3 + dx) * 4 + ((j >> 7) & 3)) & 127).astype(f32)
    lane = (j & 127).astype(f32)
    counts = cnt_ref[...].astype(f32)
    row8 = lax.broadcasted_iota(i32, (8, 128), 0)
    lane8 = lax.broadcasted_iota(i32, (8, 128), 1)
    key = counts * 1024.0 - (row8 * 128 + lane8).astype(f32)
    flat = [key[z : z + 1] for z in range(8)]
    ranks = [jnp.zeros((128, 128), f32) for _ in range(8)]
    for z in range(8):
        own = column(flat[z])
        ranks = [r + jnp.where(own > line, 1.0, 0.0) for r, line in zip(ranks, flat)]
    rank = jnp.concatenate([jnp.sum(r, axis=0, keepdims=True) for r in ranks], axis=1).astype(i32)
    rank_ref[...] = jnp.broadcast_to(rank, (8, 1024))
    node = lax.broadcasted_iota(i32, (8, 1024), 1)
    wide = lax.broadcasted_iota(i32, (8, 1024), 0)
    line = jnp.concatenate([counts[z : z + 1] for z in range(8)], axis=1)
    tail = jnp.where(wide == 1, (node >> 7).astype(f32), (node & 127).astype(f32))
    tail = jnp.where(wide == 0, line, tail)
    rows = [jnp.concatenate([a[:, z, :] for z in range(8)], axis=1) for a in (chunk, lane)]
    rows = jnp.concatenate(rows + [tail], axis=0).astype(bf16)
    slot = lax.broadcasted_iota(i32, (NB, 128), 0)
    words, most = [], []
    for t in range(4):
        found = dot_t(rows, rank_rows(rank, t * 256, 256))
        tail = found[2 * NB : 2 * NB + 8]
        scnt_ref[:, t * 256 : t * 256 + 256] = jnp.broadcast_to(tail[0:1], (8, 256))
        cell = (tail[1:2] * 128.0 + tail[2:3]) * 16384.0
        word = (found[0:NB] * 128.0 + found[NB : 2 * NB] + cell).astype(i32)
        length = tail[0:1].astype(i32)
        for h in range(2):
            at = slice(h * 128, h * 128 + 128)
            words.append(jnp.where(slot < length[:, at], word[:, at], -1))
            most.append(jnp.max(length[:, at]))
    end = 0
    for t in range(8):
        code_ref[pl.ds(end, NB), :] = words[t]
        end = end + most[t]
        tile_ref[t] = end
    code_ref[pl.ds(end, 16), :] = jnp.full((16, 128), -1, i32)
    tile_ref[8] = (end + 15) >> 4


def pair_sums(place_ref, tile_ref, code_ref, look_up, ki_ref, km_ref, turn, acc_ref):
    px, py, pz = place_ref[0], place_ref[1], place_ref[2]
    x0 = px.astype(f32) * 8.0 + 0.5
    y0 = py.astype(f32) * 16.0 + 0.5
    z0 = pz.astype(f32) * 8.0 + 0.5
    turn[...] = jnp.zeros(turn.shape, f32)
    steps = tile_ref[8]
    ends = [tile_ref[t] for t in range(7)]

    def gather(b):
        lines = []
        for half in range(2):
            code = code_ref[pl.ds(pl.multiple_of(b * 16 + half * 8, 8), 8), :]
            cell = code >> 14
            centres = (
                (((cell >> 4) & 7).astype(f32) + x0) * (1.0 / GRID),
                ((cell & 15).astype(f32) + y0) * (1.0 / GRID),
                ((cell >> 7).astype(f32) + z0) * (1.0 / GRID),
            )
            values = look_up(code, b * 2 + half)
            for c in range(6):
                value = values[c]
                if c < 3:
                    value = value - centres[c]
                turn[half, c] = jnp.where(code >= 0, value, 0.0)
            lines += [turn[half, :, n, :] for n in range(8)]
        return jnp.concatenate(lines, axis=1)

    def add(b, pair):
        hidden = gelu_twice(dot(ki_ref[...], pair.astype(bf16))).astype(bf16)
        hidden = gelu_twice(dot(km_ref[...], hidden))
        for r in range(16):
            tile = sum((b * 16 + r >= end).astype(i32) for end in ends)
            acc_ref[tile] += hidden[:, r * 128 : r * 128 + 128]

    def step(b, pair):
        following = gather(b + 1)
        add(b, pair)
        return following

    add(steps - 1, lax.fori_loop(0, steps - 1, step, gather(0)))


def lane_gather(line, at):
    return jnp.take_along_axis(jnp.broadcast_to(line, (8, 128)), at, axis=1, mode="promise_in_bounds")


def packed(parts, words):
    most = jnp.zeros((24, 128), f32)
    for part in parts:
        most = jnp.maximum(most, jnp.max(jnp.abs(part[...]), axis=0))
    most = jnp.maximum(jnp.max(most, axis=1, keepdims=True), 1e-30)
    place = jnp.broadcast_to(jnp.max(most[0:12], axis=0, keepdims=True), (12, 128))
    normal = jnp.broadcast_to(jnp.max(most[12:24], axis=0, keepdims=True), (12, 128))
    upper, lower = 32767.0 / place, 32767.0 / normal
    for n in range(9 * len(parts)):
        part = parts[n // 9]
        p = (part[n % 9, 0:12] * upper + 32768.5).astype(i32)
        q = (part[n % 9, 12:24] * lower + 32768.5).astype(i32)
        words[n] = (p << 16) | q
    return place[0:8] * (1.0 / 32767.0), normal[0:8] * (1.0 / 32767.0)


def pick_word(words, c, code, count):
    levels = (count - 1).bit_length()
    at = code & 127
    bits = [(code & (128 << n)) != 0 for n in range(levels)]

    def pick(lo, level):
        if lo >= count:
            return None
        if level == 0:
            row = c * 4 + lo % 4
            return lane_gather(words[lo // 4, row : row + 1, :], at)
        first = pick(lo, level - 1)
        second = pick(lo + (1 << (level - 1)), level - 1)
        return first if second is None else jnp.where(bits[level - 1], second, first)

    return pick(0, levels)


def near_kernel(tile_ref, same_ref, code_ref, out_ref, unit_ref, words):
    unit_ref[0], unit_ref[1] = packed((same_ref,), words)

    def step(b, carry):
        for half in range(2):
            code = code_ref[pl.ds(pl.multiple_of(b * 16 + half * 8, 8), 8), :] - 72 * 128
            for c in range(3):
                out_ref[b * 2 + half, c] = pick_word(words, c, code, 36)
        return carry

    lax.fori_loop(0, tile_ref[8], step, 0)


def encoder_kernel(
    place_ref,
    tile_ref,
    below_ref,
    above_ref,
    code_ref,
    near_ref,
    unit_ref,
    rank_ref,
    scnt_ref,
    kernel_in_ref,
    kernel_mid_ref,
    ko_ref,
    out_ref,
    ki_ref,
    km_ref,
    words,
    turn,
    acc_ref,
):
    ki = jnp.concatenate([kernel_in_ref[...].astype(f32), jnp.zeros((2, 80), f32)], axis=0)
    ki_ref[...] = jnp.concatenate([ki, jnp.zeros((8, 48), f32)], axis=1).T[0:80].astype(bf16)
    km = jnp.concatenate([kernel_mid_ref[...].astype(f32) * 0.5, jnp.zeros((80, 48), f32)], axis=1)
    km_ref[...] = km.T[0:80].astype(bf16)
    far_place, far_normal = packed((below_ref, above_ref), words)
    near_place, near_normal = unit_ref[0], unit_ref[1]
    acc_ref[...] = jnp.zeros(acc_ref.shape, f32)

    def look_up(code, block):
        near = (code & 16383) >= 72 * 128
        upper = jnp.where(near, near_place, far_place)
        lower = jnp.where(near, near_normal, far_normal)
        values = [None] * 6
        for c in range(3):
            word = jnp.where(near, near_ref[block, c], pick_word(words, c, code, 72))
            values[c] = (lax.shift_right_logical(word, 16) - 32768).astype(f32) * upper
            values[c + 3] = ((word & 65535) - 32768).astype(f32) * lower
        return values

    pair_sums(place_ref, tile_ref, code_ref, look_up, ki_ref, km_ref, turn, acc_ref)
    mean = jnp.concatenate([acc_ref[t] for t in range(8)], axis=1) * (0.5 / scnt_ref[0:1])
    upper = mean.astype(bf16)
    lower = (mean - upper.astype(f32)).astype(bf16)
    latent = (dot(ko_ref[...], upper) + dot(ko_ref[...], lower)).astype(bf16)
    rank = rank_ref[0:1]
    spread = jnp.zeros((64, 1024), f32)
    for t in range(4):
        spread = spread + dot(latent[:, t * 256 : t * 256 + 256], rank_rows(rank, t * 256, 256))
    out_ref[...] = spread.astype(bf16).reshape(8, 8, 1024)


def forward_kernel(m_ref, ahi_ref, alo_ref, whi_ref, wlo_ref, out_ref, wide):
    rows = [
        m_ref[s].astype(f32)[:, z * 128 : (z + 1) * 128] for s in range(8) for z in range(8)
    ]
    cells = jnp.concatenate(rows, axis=0).astype(bf16)
    z = dot(ahi_ref[...], cells) + dot(alo_ref[...], cells)
    right = []
    for kh in range(4):
        right += [z[kh * 64 + 32 : kh * 64 + 64], -z[kh * 64 : kh * 64 + 32]]
    both = jnp.concatenate([z, jnp.concatenate(right, axis=0)], axis=1).astype(bf16)
    p = dot_t(whi_ref[...], both) + dot_t(wlo_ref[...], both)
    for kh in range(4):
        for h in range(2):
            line = jnp.concatenate(
                [p[q * 64 : (q + 1) * 64, kh * 64 : (kh + 1) * 64] for q in (2 * h, 2 * h + 1)], axis=1
            )
            for jh in range(8):
                wide[pl.ds(((jh * 4 + kh) * 8) * 2 + h, 8, stride=2), :] = line[jh * 8 : jh * 8 + 8]
    out_ref[...] = wide[...].astype(bf16)


def mix_kernel(r_ref, w_ref, own_ref, sel_ref, place_ref, half_ref, out_ref):
    s = jnp.sum(r_ref[...].astype(f32), axis=0)
    s = s.astype(bf16).astype(f32)
    own = own_ref[...]
    g = jnp.zeros((16, 128), f32)
    for ch in range(8):
        line = jnp.concatenate([s[2 * ch : 2 * ch + 1], s[2 * ch + 1 : 2 * ch + 2]], axis=1)
        g = g + dot((line * own).astype(bf16), w_ref[ch])
    spread = dot(g.astype(bf16), sel_ref[...]) * place_ref[...]
    d = dot(half_ref[...], spread.astype(bf16))
    d = jnp.concatenate([d[0:2, oh * 128 : (oh + 1) * 128] for oh in range(8)], axis=0).astype(bf16)
    for n in range(32):
        out_ref[n] = d


def inverse_kernel(q_ref, v_ref, bc_ref, bs_ref, partner_ref, out_ref):
    blocks = []
    for kh in range(4):
        rows = jnp.concatenate([q_ref[jh, kh] for jh in range(8)], axis=0).astype(f32)
        blocks.append(jnp.concatenate([rows[:, 0:64], rows[:, 64:128]], axis=0))
    x = jnp.concatenate(blocks, axis=1)
    row = lax.broadcasted_iota(i32, (256, 256), 0)
    lane = lax.broadcasted_iota(i32, (256, 256), 1)
    x = jnp.where((row == 0) & (lane < 8), 0.0, x)
    xb = x.astype(bf16)
    twin = dot(partner_ref[...], xb[:, 0:128])
    low = lane[0:1, 0:128]
    side = jnp.where(low < 8, 0.5, jnp.where(low < 16, -0.5, 0.0))
    weight = jnp.where(lane[0:1, :] < 16, 0.5, 2.0)
    power = jnp.sum(x * x, axis=0, keepdims=True) * weight
    cross = jnp.sum(x[:, 0:128] * twin, axis=0, keepdims=True) * side
    power = jnp.broadcast_to(power[:, 0:128] + power[:, 128:256] + cross, (8, 128))
    for shift in (8, 16, 32, 64):
        power = power + pltpu.roll(power, shift, 1)
    scale = lax.rsqrt(power * (1.0 / (CELLS * CELLS)) + NORM_FLOOR)[0:1]
    scale = jnp.concatenate([scale, scale], axis=1)
    g = (dot(v_ref[...], xb) * scale).astype(bf16)
    out = dot_t(bc_ref[...], g[0:128]) + dot_t(bs_ref[...], g[128:256])
    out_ref[...] = out.astype(bf16).reshape(8, 8, 8, 128)


def output_kernel(y_ref, lat_ref, w_ref, out_ref):
    for z in range(8):
        y = jnp.concatenate([y_ref[s, z].astype(f32) for s in range(8)], axis=0)
        lat = jnp.concatenate(
            [lat_ref[s].astype(f32)[:, z * 128 : (z + 1) * 128] for s in range(8)], axis=0
        )
        both = jnp.concatenate([lat, y], axis=0).T.astype(bf16)
        v = dot(both, w_ref[...])
        out_ref[:, z, :] = 0.5 * gelu_twice(v)


def call(kernel, shape, dtype, *args, scratch=(), smem=0):
    return pl.pallas_call(
        kernel,
        out_shape=jax.ShapeDtypeStruct(shape, dtype),
        in_specs=[SMEM] * smem + [VMEM] * (len(args) - smem),
        out_specs=VMEM,
        scratch_shapes=list(scratch),
        compiler_params=pltpu.CompilerParams(vmem_limit_bytes=48 * 1024 * 1024),
    )(*args)


def sorted_nodes(place, near, valid):
    shapes = (
        ((ROWS, 128), i32),
        ((8, 1024), i32),
        ((8, 1024), f32),
        ((9,), i32),
    )
    return pl.pallas_call(
        sort_kernel,
        out_shape=[jax.ShapeDtypeStruct(*s) for s in shapes],
        in_specs=[SMEM, VMEM, VMEM],
        out_specs=[VMEM] * 3 + [SMEM],
        compiler_params=pltpu.CompilerParams(vmem_limit_bytes=48 * 1024 * 1024),
        name="sort",
    )(place, near, valid)


def near_words(tiles, same, code):
    shapes = (((ROWS // 8, 3, 8, 128), i32), ((2, 8, 128), f32))
    return pl.pallas_call(
        near_kernel,
        out_shape=[jax.ShapeDtypeStruct(*s) for s in shapes],
        in_specs=[SMEM, VMEM, VMEM],
        out_specs=[VMEM] * 2,
        scratch_shapes=[pltpu.VMEM((9, 12, 128), i32)],
        compiler_params=pltpu.CompilerParams(vmem_limit_bytes=48 * 1024 * 1024),
        name="near",
    )(tiles, same, code)


def beside(cells, axis):
    count = lax.axis_size(axis)
    ends = count - 1
    lower = lax.ppermute(cells, axis, [(i, i + 1) for i in range(ends)])
    upper = lax.ppermute(cells, axis, [(i + 1, i) for i in range(ends)])
    return lower, cells, upper


def turned(cos, sin, phase):
    c, s = jnp.cos(phase), jnp.sin(phase)
    return cos * c - sin * s, sin * c + cos * s


def layer(point_data, neighbours, counts, kernel_in, kernel_mid, kernel_out, spectral, skip_weight):
    gx = lax.axis_index("gx")
    gy = lax.axis_index("gy")
    gz = lax.axis_index(GZ)
    place = jnp.stack([gx, gy, gz]).astype(i32)

    own = point_data.reshape(1, 24, 128)
    near = neighbours[0].transpose(3, 2, 0, 1).reshape(NB, 8, 128)
    valid = counts[0].transpose(2, 0, 1).reshape(8, 128)

    line = jnp.concatenate(beside(own, "gx"), axis=0)
    plane = jnp.concatenate(beside(line, "gy"), axis=0)
    tables = sorted_nodes(place, near, valid)
    plane, tables = lax.optimization_barrier((plane, tables))
    code, rank, sorted_counts, tiles = tables
    below, same, above = beside(plane, GZ)
    words, units = near_words(tiles, same, code)
    latent = call(
        encoder_kernel,
        (8, 8, 1024),
        bf16,
        place,
        tiles,
        below,
        above,
        code,
        words,
        units,
        rank,
        sorted_counts,
        kernel_in,
        kernel_mid,
        kernel_out.T,
        scratch=(
            pltpu.VMEM((80, 8), bf16),
            pltpu.VMEM((80, 80), bf16),
            pltpu.VMEM((18, 12, 128), i32),
            pltpu.VMEM((2, 8, 8, 128), f32),
            pltpu.VMEM((8, 80, 128), f32),
        ),
        smem=2,
    )

    latent, spectral, gx, gy = lax.optimization_barrier((latent, spectral, gx, gy))
    (ffi, ffj), (ifi, ifj), xl, yl = plane_tables()
    local = angle(1, ffi[:, None] * xl[None, :] + ffj[:, None] * yl[None, :])
    phase = ((jnp.asarray(ffi, i32) * 8 * gx + jnp.asarray(ffj, i32) * 16 * gy) % GRID).astype(f32)
    cos, sin = turned(
        np.cos(local).astype(np.float32),
        np.sin(local).astype(np.float32),
        (phase * (2.0 * math.pi / GRID))[:, None],
    )
    whi, wlo = split_two(jnp.concatenate([cos, sin], axis=1))
    local = angle(1, ifi[None, :] * xl[:, None] + ifj[None, :] * yl[:, None])
    phase = ((jnp.asarray(ifi, i32) * 8 * gx + jnp.asarray(ifj, i32) * 16 * gy) % GRID).astype(f32)
    cos, sin = turned(
        np.cos(local).astype(np.float32),
        np.sin(local).astype(np.float32),
        (phase * (2.0 * math.pi / GRID))[None, :],
    )
    back = jnp.concatenate([cos, sin], axis=0).astype(bf16)

    w = spectral.reshape(2, 2, 2, 4, 8, 8, 64).transpose(0, 4, 2, 1, 3, 5, 6)
    wr, wi = w[0], w[1]
    mixing = jnp.stack(
        [jnp.concatenate([wr, wi], axis=-1), jnp.concatenate([-wi, wr], axis=-1)], axis=3
    ).reshape(8, 256, 128)
    joint = jnp.concatenate([skip_weight, jnp.eye(64, dtype=bf16)], axis=0)

    depth = lax.all_to_all(latent, GZ, split_axis=0, concat_axis=0)
    ahi, alo = third_forward()
    partial = call(forward_kernel, (512, 128), bf16, depth, ahi, alo, whi, wlo, scratch=(pltpu.VMEM((512, 128), f32),))
    partial = lax.all_to_all(partial.reshape(256, 2, 128), ALL, split_axis=0, concat_axis=0)
    own_mask, place_mask, half = mode_masks()
    mixed = call(
        mix_kernel,
        (32, 16, 128),
        bf16,
        partial.reshape(32, 16, 128),
        mixing,
        own_mask,
        placing(),
        place_mask,
        half,
    )
    mixed = lax.all_to_all(mixed.reshape(256, 2, 128), ALL, split_axis=0, concat_axis=0)
    third = third_inverse()
    branch = call(
        inverse_kernel,
        (8, 8, 8, 128),
        bf16,
        mixed.reshape(8, 4, 16, 128),
        back,
        third[:, :256],
        third[:, 256:],
        partner_table(),
    )
    branch = lax.all_to_all(branch, GZ, split_axis=0, concat_axis=0)
    out = call(output_kernel, (128, 8, 64), f32, branch, latent, joint)
    return out.reshape(1, 8, 16, 8, 64)


def solution(mesh):
    split = Mesh(
        mesh.devices.reshape(mesh.shape["gx"], mesh.shape["gy"], 4, 2), ("gx", "gy", "gz_0", "gz_1")
    )
    return jax.shard_map(
        layer,
        mesh=split,
        in_specs=(
            P(None, None, ALL),
            P(None, "gx", "gy", GZ, None),
            P(None, "gx", "gy", GZ),
            P(),
            P(),
            P(),
            P(None, GZ, "gx", "gy", None, None),
            P(),
        ),
        out_specs=P(None, "gx", "gy", GZ, None),
        check_vma=False,
    )
```

```python
import math

import jax
import jax.numpy as jnp
import numpy as np
from jax import lax
from jax.experimental import pallas as pl
from jax.experimental.pallas import tpu as pltpu
from jax.sharding import Mesh
from jax.sharding import PartitionSpec as P

f32 = jnp.float32
bf16 = jnp.bfloat16
i32 = jnp.int32

GRID = 64
NB = 32
ROWS = 8 * NB + 32
CELLS = float(GRID**3)
NORM_FLOOR = 1.0
GZ = ("gz_0", "gz_1")
ALL = ("gx", "gy", "gz_0", "gz_1")
C0 = math.sqrt(2.0 / math.pi)
C1 = C0 * 0.044715
VMEM = pl.BlockSpec(memory_space=pltpu.VMEM)
SMEM = pl.BlockSpec(memory_space=pltpu.SMEM)


def freq(n):
    return np.where(n < 8, n, n - 16)


def angle(f, m):
    return 2.0 * math.pi * ((f * m) % GRID) / GRID


def split_two(a):
    hi = a.astype(bf16)
    lo = (a - hi.astype(a.dtype)).astype(bf16)
    return hi, lo


def third_forward():
    kh, r, kl, c = np.meshgrid(*map(np.arange, (4, 2, 4, 8)), indexing="ij")
    k, r, c = (4 * kh + kl).reshape(-1, 1), r.reshape(-1, 1), c.reshape(-1, 1)
    z = np.repeat(np.arange(64), 8)[None, :]
    cc = np.tile(np.arange(8), 64)[None, :]
    a = angle(k, z)
    v = np.where(r == 0, np.cos(a), -np.sin(a)) * (c == cc)
    return split_two(v)


def third_inverse():
    z = np.repeat(np.arange(64), 8)[:, None]
    o = np.tile(np.arange(8), 64)[:, None]
    s, kh, kl, r, oo = (
        a.reshape(1, -1) for a in np.meshgrid(*map(np.arange, (2, 4, 4, 2, 8)), indexing="ij")
    )
    k = 4 * kh + kl
    a = angle(k, z)
    w = np.where(k == 0, 1.0, 2.0) / CELLS
    cos, sin = np.cos(a), np.sin(a)
    v = np.where(s == 0, np.where(r == 0, cos, -sin), np.where(r == 0, -sin, -cos))
    return (v * w * (o == oo)).astype(bf16)


def plane_tables():
    jl, il, jh, ih = (a.reshape(-1) for a in np.meshgrid(*map(np.arange, (2, 2, 8, 8)), indexing="ij"))
    fwd = freq(2 * ih + il), freq(2 * jh + jl)
    il, jh, ih, jl = (a.reshape(-1) for a in np.meshgrid(*map(np.arange, (2, 8, 8, 2)), indexing="ij"))
    inv = freq(2 * ih + il), freq(2 * jh + jl)
    return fwd, inv, np.repeat(np.arange(8), 16), np.tile(np.arange(16), 8)


def partner_table():
    _, (fi, fj), _, _ = plane_tables()
    hit = (fi[:, None] == -fi[None, :]) & (fj[:, None] == -fj[None, :])
    return hit.astype(np.float32).astype(bf16)


def mode_masks():
    jl, il, kl = (a.reshape(-1, 1) for a in np.meshgrid(*map(np.arange, (2, 2, 4)), indexing="ij"))
    jc, ic, _, kc, _ = (
        a.reshape(1, -1) for a in np.meshgrid(*map(np.arange, (2, 2, 2, 4, 8)), indexing="ij")
    )
    own = ((jl == jc) & (il == ic) & (kl == kc)).astype(np.float32)
    _, ib, kb, _, _ = (
        a.reshape(1, -1) for a in np.meshgrid(*map(np.arange, (8, 2, 4, 2, 8)), indexing="ij")
    )
    place = ((il == ib) & (kl == kb)).astype(np.float32)
    half = np.zeros((8, 16), np.float32)
    half[jl[:, 0], np.arange(16)] = 1.0
    return own, place, half.astype(bf16)


def placing():
    ro, oh, ol = (a.reshape(-1, 1) for a in np.meshgrid(*map(np.arange, (2, 8, 8)), indexing="ij"))
    oc, _, _, rc, lc = (
        a.reshape(1, -1) for a in np.meshgrid(*map(np.arange, (8, 2, 4, 2, 8)), indexing="ij")
    )
    return ((ro == rc) & (oh == oc) & (ol == lc)).astype(np.float32).astype(bf16)


def dot(a, b):
    return jnp.dot(a, b, preferred_element_type=f32)


def dot_t(a, b):
    return lax.dot_general(a, b, (((1,), (1,)), ((), ())), preferred_element_type=f32)


def gelu_twice(v):
    return v * jnp.tanh(v * (v * v * C1 + C0)) + v


def column(line):
    return jnp.broadcast_to(line, (128, 128)).T


def rank_rows(rank, first, count):
    r = lax.broadcasted_iota(i32, (count, 1024), 0) + first
    return jnp.where(r == rank, 1.0, 0.0).astype(bf16)


def sort_kernel(
    place_ref, nb_ref, cnt_ref, kernel_in_ref, kernel_mid_ref, code_ref, rank_ref, scnt_ref, ki_ref, km_ref, tile_ref
):
    ki = jnp.concatenate([kernel_in_ref[...].astype(f32), jnp.zeros((2, 80), f32)], axis=0)
    ki_ref[...] = jnp.concatenate([ki, jnp.zeros((8, 48), f32)], axis=1).T[0:80].astype(bf16)
    km = jnp.concatenate([kernel_mid_ref[...].astype(f32) * 0.5, jnp.zeros((80, 48), f32)], axis=1)
    km_ref[...] = km.T[0:80].astype(bf16)
    px, py, pz = place_ref[0], place_ref[1], place_ref[2]
    j = nb_ref[...]
    owner = j >> 9
    dz = (owner & 7) - pz + 1
    dy = ((owner >> 3) & 3) - py + 1
    dx = (owner >> 5) - px + 1
    group = jnp.where(dz == 1, 72, (dz >> 1) * 36)
    chunk = ((group + (dy * 3 + dx) * 4 + ((j >> 7) & 3)) & 127).astype(f32)
    lane = (j & 127).astype(f32)
    counts = cnt_ref[...].astype(f32)
    row8 = lax.broadcasted_iota(i32, (8, 128), 0)
    lane8 = lax.broadcasted_iota(i32, (8, 128), 1)
    key = counts * 1024.0 - (row8 * 128 + lane8).astype(f32)
    flat = [key[z : z + 1] for z in range(8)]
    ranks = [jnp.zeros((128, 128), f32) for _ in range(8)]
    for z in range(8):
        own = column(flat[z])
        ranks = [r + jnp.where(own > line, 1.0, 0.0) for r, line in zip(ranks, flat)]
    rank = jnp.concatenate([jnp.sum(r, axis=0, keepdims=True) for r in ranks], axis=1).astype(i32)
    rank_ref[...] = jnp.broadcast_to(rank, (8, 1024))
    node = lax.broadcasted_iota(i32, (8, 1024), 1)
    wide = lax.broadcasted_iota(i32, (8, 1024), 0)
    line = jnp.concatenate([counts[z : z + 1] for z in range(8)], axis=1)
    tail = jnp.where(wide == 1, (node >> 7).astype(f32), (node & 127).astype(f32))
    tail = jnp.where(wide == 0, line, tail)
    rows = [jnp.concatenate([a[:, z, :] for z in range(8)], axis=1) for a in (chunk, lane)]
    rows = jnp.concatenate(rows + [tail], axis=0).astype(bf16)
    slot = lax.broadcasted_iota(i32, (NB, 128), 0)
    words, most = [], []
    for t in range(4):
        found = dot_t(rows, rank_rows(rank, t * 256, 256))
        tail = found[2 * NB : 2 * NB + 8]
        scnt_ref[:, t * 256 : t * 256 + 256] = jnp.broadcast_to(tail[0:1], (8, 256))
        cell = (tail[1:2] * 128.0 + tail[2:3]) * 16384.0
        word = (found[0:NB] * 128.0 + found[NB : 2 * NB] + cell).astype(i32)
        length = tail[0:1].astype(i32)
        for h in range(2):
            at = slice(h * 128, h * 128 + 128)
            words.append(jnp.where(slot < length[:, at], word[:, at], -1))
            most.append(jnp.max(length[:, at]))
    end = 0
    for t in range(8):
        code_ref[pl.ds(end, NB), :] = words[t]
        end = end + most[t]
        tile_ref[t] = end
    code_ref[pl.ds(end, 16), :] = jnp.full((16, 128), -1, i32)
    tile_ref[8] = (end + 15) >> 4


def pair_sums(place_ref, tile_ref, code_ref, look_up, ki_ref, km_ref, turn, acc_ref):
    px, py, pz = place_ref[0], place_ref[1], place_ref[2]
    x0 = px.astype(f32) * 8.0 + 0.5
    y0 = py.astype(f32) * 16.0 + 0.5
    z0 = pz.astype(f32) * 8.0 + 0.5
    turn[...] = jnp.zeros(turn.shape, f32)
    steps = tile_ref[8]
    ends = [tile_ref[t] for t in range(7)]

    def gather(b):
        lines = []
        for half in range(2):
            code = code_ref[pl.ds(pl.multiple_of(b * 16 + half * 8, 8), 8), :]
            cell = code >> 14
            centres = (
                (((cell >> 4) & 7).astype(f32) + x0) * (1.0 / GRID),
                ((cell & 15).astype(f32) + y0) * (1.0 / GRID),
                ((cell >> 7).astype(f32) + z0) * (1.0 / GRID),
            )
            values = look_up(code, b * 2 + half)
            for c in range(6):
                value = values[c]
                if c < 3:
                    value = value - centres[c]
                turn[half, c] = jnp.where(code >= 0, value, 0.0)
            lines += [turn[half, :, n, :] for n in range(8)]
        return jnp.concatenate(lines, axis=1)

    def add(b, pair):
        hidden = gelu_twice(dot(ki_ref[...], pair.astype(bf16))).astype(bf16)
        hidden = gelu_twice(dot(km_ref[...], hidden))
        for r in range(16):
            tile = sum((b * 16 + r >= end).astype(i32) for end in ends)
            acc_ref[tile] += hidden[:, r * 128 : r * 128 + 128]

    def step(b, pair):
        following = gather(b + 1)
        add(b, pair)
        return following

    add(steps - 1, lax.fori_loop(0, steps - 1, step, gather(0)))


def lane_gather(line, at):
    return jnp.take_along_axis(jnp.broadcast_to(line, (8, 128)), at, axis=1, mode="promise_in_bounds")


def packed(parts, words):
    most = jnp.zeros((24, 128), f32)
    for part in parts:
        most = jnp.maximum(most, jnp.max(jnp.abs(part[...]), axis=0))
    most = jnp.maximum(jnp.max(most, axis=1, keepdims=True), 1e-30)
    place = jnp.broadcast_to(jnp.max(most[0:12], axis=0, keepdims=True), (12, 128))
    normal = jnp.broadcast_to(jnp.max(most[12:24], axis=0, keepdims=True), (12, 128))
    upper, lower = 32767.0 / place, 32767.0 / normal
    for n in range(9 * len(parts)):
        part = parts[n // 9]
        p = (part[n % 9, 0:12] * upper + 32768.5).astype(i32)
        q = (part[n % 9, 12:24] * lower + 32768.5).astype(i32)
        words[n] = (p << 16) | q
    return place[0:8] * (1.0 / 32767.0), normal[0:8] * (1.0 / 32767.0)


def pick_word(words, c, code, count):
    levels = (count - 1).bit_length()
    at = code & 127
    bits = [(code & (128 << n)) != 0 for n in range(levels)]

    def pick(lo, level):
        if lo >= count:
            return None
        if level == 0:
            row = c * 4 + lo % 4
            return lane_gather(words[lo // 4, row : row + 1, :], at)
        first = pick(lo, level - 1)
        second = pick(lo + (1 << (level - 1)), level - 1)
        return first if second is None else jnp.where(bits[level - 1], second, first)

    return pick(0, levels)


def near_kernel(tile_ref, same_ref, code_ref, out_ref, unit_ref, words):
    unit_ref[0], unit_ref[1] = packed((same_ref,), words)

    def step(b, carry):
        for half in range(2):
            code = code_ref[pl.ds(pl.multiple_of(b * 16 + half * 8, 8), 8), :] - 72 * 128
            for c in range(3):
                out_ref[b * 2 + half, c] = pick_word(words, c, code, 36)
        return carry

    lax.fori_loop(0, tile_ref[8], step, 0)


def encoder_kernel(
    place_ref,
    tile_ref,
    below_ref,
    above_ref,
    code_ref,
    near_ref,
    unit_ref,
    rank_ref,
    scnt_ref,
    ki_ref,
    km_ref,
    ko_ref,
    out_ref,
    words,
    turn,
    acc_ref,
):
    far_place, far_normal = packed((below_ref, above_ref), words)
    near_place, near_normal = unit_ref[0], unit_ref[1]
    acc_ref[...] = jnp.zeros(acc_ref.shape, f32)

    def look_up(code, block):
        near = (code & 16383) >= 72 * 128
        upper = jnp.where(near, near_place, far_place)
        lower = jnp.where(near, near_normal, far_normal)
        values = [None] * 6
        for c in range(3):
            word = jnp.where(near, near_ref[block, c], pick_word(words, c, code, 72))
            values[c] = (lax.shift_right_logical(word, 16) - 32768).astype(f32) * upper
            values[c + 3] = ((word & 65535) - 32768).astype(f32) * lower
        return values

    pair_sums(place_ref, tile_ref, code_ref, look_up, ki_ref, km_ref, turn, acc_ref)
    mean = jnp.concatenate([acc_ref[t] for t in range(8)], axis=1) * (0.5 / scnt_ref[0:1])
    upper = mean.astype(bf16)
    lower = (mean - upper.astype(f32)).astype(bf16)
    latent = (dot(ko_ref[...], upper) + dot(ko_ref[...], lower)).astype(bf16)
    rank = rank_ref[0:1]
    spread = jnp.zeros((64, 1024), f32)
    for t in range(4):
        spread = spread + dot(latent[:, t * 256 : t * 256 + 256], rank_rows(rank, t * 256, 256))
    out_ref[...] = spread.astype(bf16).reshape(8, 8, 1024)


def forward_kernel(m_ref, ahi_ref, alo_ref, whi_ref, wlo_ref, out_ref, wide):
    rows = [
        m_ref[s].astype(f32)[:, z * 128 : (z + 1) * 128] for s in range(8) for z in range(8)
    ]
    cells = jnp.concatenate(rows, axis=0).astype(bf16)
    z = dot(ahi_ref[...], cells) + dot(alo_ref[...], cells)
    right = []
    for kh in range(4):
        right += [z[kh * 64 + 32 : kh * 64 + 64], -z[kh * 64 : kh * 64 + 32]]
    both = jnp.concatenate([z, jnp.concatenate(right, axis=0)], axis=1).astype(bf16)
    p = dot_t(whi_ref[...], both) + dot_t(wlo_ref[...], both)
    for kh in range(4):
        for h in range(2):
            line = jnp.concatenate(
                [p[q * 64 : (q + 1) * 64, kh * 64 : (kh + 1) * 64] for q in (2 * h, 2 * h + 1)], axis=1
            )
            for jh in range(8):
                wide[pl.ds(((jh * 4 + kh) * 8) * 2 + h, 8, stride=2), :] = line[jh * 8 : jh * 8 + 8]
    out_ref[...] = wide[...].astype(bf16)


def mix_kernel(r_ref, w_ref, own_ref, sel_ref, place_ref, half_ref, out_ref):
    s = jnp.sum(r_ref[...].astype(f32), axis=0)
    s = s.astype(bf16).astype(f32)
    own = own_ref[...]
    g = jnp.zeros((16, 128), f32)
    for ch in range(8):
        line = jnp.concatenate([s[2 * ch : 2 * ch + 1], s[2 * ch + 1 : 2 * ch + 2]], axis=1)
        g = g + dot((line * own).astype(bf16), w_ref[ch])
    spread = dot(g.astype(bf16), sel_ref[...]) * place_ref[...]
    d = dot(half_ref[...], spread.astype(bf16))
    d = jnp.concatenate([d[0:2, oh * 128 : (oh + 1) * 128] for oh in range(8)], axis=0).astype(bf16)
    for n in range(32):
        out_ref[n] = d


def inverse_kernel(q_ref, v_ref, bc_ref, bs_ref, partner_ref, out_ref):
    blocks = []
    for kh in range(4):
        rows = jnp.concatenate([q_ref[jh, kh] for jh in range(8)], axis=0).astype(f32)
        blocks.append(jnp.concatenate([rows[:, 0:64], rows[:, 64:128]], axis=0))
    x = jnp.concatenate(blocks, axis=1)
    row = lax.broadcasted_iota(i32, (256, 256), 0)
    lane = lax.broadcasted_iota(i32, (256, 256), 1)
    x = jnp.where((row == 0) & (lane < 8), 0.0, x)
    xb = x.astype(bf16)
    twin = dot(partner_ref[...], xb[:, 0:128])
    low = lane[0:1, 0:128]
    side = jnp.where(low < 8, 0.5, jnp.where(low < 16, -0.5, 0.0))
    weight = jnp.where(lane[0:1, :] < 16, 0.5, 2.0)
    power = jnp.sum(x * x, axis=0, keepdims=True) * weight
    cross = jnp.sum(x[:, 0:128] * twin, axis=0, keepdims=True) * side
    power = jnp.broadcast_to(power[:, 0:128] + power[:, 128:256] + cross, (8, 128))
    for shift in (8, 16, 32, 64):
        power = power + pltpu.roll(power, shift, 1)
    scale = lax.rsqrt(power * (1.0 / (CELLS * CELLS)) + NORM_FLOOR)[0:1]
    scale = jnp.concatenate([scale, scale], axis=1)
    g = (dot(v_ref[...], xb) * scale).astype(bf16)
    out = dot_t(bc_ref[...], g[0:128]) + dot_t(bs_ref[...], g[128:256])
    out_ref[...] = out.astype(bf16).reshape(8, 8, 8, 128)


def output_kernel(y_ref, lat_ref, w_ref, out_ref):
    for z in range(8):
        y = jnp.concatenate([y_ref[s, z].astype(f32) for s in range(8)], axis=0)
        lat = jnp.concatenate(
            [lat_ref[s].astype(f32)[:, z * 128 : (z + 1) * 128] for s in range(8)], axis=0
        )
        both = jnp.concatenate([lat, y], axis=0).T.astype(bf16)
        v = dot(both, w_ref[...])
        out_ref[:, z, :] = 0.5 * gelu_twice(v)


def call(kernel, shape, dtype, *args, scratch=(), smem=0):
    return pl.pallas_call(
        kernel,
        out_shape=jax.ShapeDtypeStruct(shape, dtype),
        in_specs=[SMEM] * smem + [VMEM] * (len(args) - smem),
        out_specs=VMEM,
        scratch_shapes=list(scratch),
        compiler_params=pltpu.CompilerParams(vmem_limit_bytes=48 * 1024 * 1024),
    )(*args)


def sorted_nodes(place, near, valid, kernel_in, kernel_mid):
    shapes = (
        ((ROWS, 128), i32),
        ((8, 1024), i32),
        ((8, 1024), f32),
        ((80, 8), bf16),
        ((80, 80), bf16),
        ((9,), i32),
    )
    return pl.pallas_call(
        sort_kernel,
        out_shape=[jax.ShapeDtypeStruct(*s) for s in shapes],
        in_specs=[SMEM] + [VMEM] * 4,
        out_specs=[VMEM] * 5 + [SMEM],
        compiler_params=pltpu.CompilerParams(vmem_limit_bytes=48 * 1024 * 1024),
        name="sort",
    )(place, near, valid, kernel_in, kernel_mid)


def near_words(tiles, same, code):
    shapes = (((ROWS // 8, 3, 8, 128), i32), ((2, 8, 128), f32))
    return pl.pallas_call(
        near_kernel,
        out_shape=[jax.ShapeDtypeStruct(*s) for s in shapes],
        in_specs=[SMEM, VMEM, VMEM],
        out_specs=[VMEM] * 2,
        scratch_shapes=[pltpu.VMEM((9, 12, 128), i32)],
        compiler_params=pltpu.CompilerParams(vmem_limit_bytes=48 * 1024 * 1024),
        name="near",
    )(tiles, same, code)


def beside(cells, axis):
    count = lax.axis_size(axis)
    ends = count - 1
    lower = lax.ppermute(cells, axis, [(i, i + 1) for i in range(ends)])
    upper = lax.ppermute(cells, axis, [(i + 1, i) for i in range(ends)])
    return lower, cells, upper


def turned(cos, sin, phase):
    c, s = jnp.cos(phase), jnp.sin(phase)
    return cos * c - sin * s, sin * c + cos * s


def layer(point_data, neighbours, counts, kernel_in, kernel_mid, kernel_out, spectral, skip_weight):
    gx = lax.axis_index("gx")
    gy = lax.axis_index("gy")
    gz = lax.axis_index(GZ)
    place = jnp.stack([gx, gy, gz]).astype(i32)

    own = point_data.reshape(1, 24, 128)
    near = neighbours[0].transpose(3, 2, 0, 1).reshape(NB, 8, 128)
    valid = counts[0].transpose(2, 0, 1).reshape(8, 128)

    line = jnp.concatenate(beside(own, "gx"), axis=0)
    plane = jnp.concatenate(beside(line, "gy"), axis=0)
    tables = sorted_nodes(place, near, valid, kernel_in, kernel_mid)
    plane, tables = lax.optimization_barrier((plane, tables))
    code, rank, sorted_counts, ki, km, tiles = tables
    below, same, above = beside(plane, GZ)
    words, units = near_words(tiles, same, code)
    latent = call(
        encoder_kernel,
        (8, 8, 1024),
        bf16,
        place,
        tiles,
        below,
        above,
        code,
        words,
        units,
        rank,
        sorted_counts,
        ki,
        km,
        kernel_out.T,
        scratch=(
            pltpu.VMEM((18, 12, 128), i32),
            pltpu.VMEM((2, 8, 8, 128), f32),
            pltpu.VMEM((8, 80, 128), f32),
        ),
        smem=2,
    )

    latent, spectral, gx, gy = lax.optimization_barrier((latent, spectral, gx, gy))
    (ffi, ffj), (ifi, ifj), xl, yl = plane_tables()
    local = angle(1, ffi[:, None] * xl[None, :] + ffj[:, None] * yl[None, :])
    phase = ((jnp.asarray(ffi, i32) * 8 * gx + jnp.asarray(ffj, i32) * 16 * gy) % GRID).astype(f32)
    cos, sin = turned(
        np.cos(local).astype(np.float32),
        np.sin(local).astype(np.float32),
        (phase * (2.0 * math.pi / GRID))[:, None],
    )
    whi, wlo = split_two(jnp.concatenate([cos, sin], axis=1))
    local = angle(1, ifi[None, :] * xl[:, None] + ifj[None, :] * yl[:, None])
    phase = ((jnp.asarray(ifi, i32) * 8 * gx + jnp.asarray(ifj, i32) * 16 * gy) % GRID).astype(f32)
    cos, sin = turned(
        np.cos(local).astype(np.float32),
        np.sin(local).astype(np.float32),
        (phase * (2.0 * math.pi / GRID))[None, :],
    )
    back = jnp.concatenate([cos, sin], axis=0).astype(bf16)

    w = spectral.reshape(2, 2, 2, 4, 8, 8, 64).transpose(0, 4, 2, 1, 3, 5, 6)
    wr, wi = w[0], w[1]
    mixing = jnp.stack(
        [jnp.concatenate([wr, wi], axis=-1), jnp.concatenate([-wi, wr], axis=-1)], axis=3
    ).reshape(8, 256, 128)
    joint = jnp.concatenate([skip_weight, jnp.eye(64, dtype=bf16)], axis=0)

    depth = lax.all_to_all(latent, GZ, split_axis=0, concat_axis=0)
    ahi, alo = third_forward()
    partial = call(forward_kernel, (512, 128), bf16, depth, ahi, alo, whi, wlo, scratch=(pltpu.VMEM((512, 128), f32),))
    partial = lax.all_to_all(partial.reshape(256, 2, 128), ALL, split_axis=0, concat_axis=0)
    own_mask, place_mask, half = mode_masks()
    mixed = call(
        mix_kernel,
        (32, 16, 128),
        bf16,
        partial.reshape(32, 16, 128),
        mixing,
        own_mask,
        placing(),
        place_mask,
        half,
    )
    mixed = lax.all_to_all(mixed.reshape(256, 2, 128), ALL, split_axis=0, concat_axis=0)
    third = third_inverse()
    branch = call(
        inverse_kernel,
        (8, 8, 8, 128),
        bf16,
        mixed.reshape(8, 4, 16, 128),
        back,
        third[:, :256],
        third[:, 256:],
        partner_table(),
    )
    branch = lax.all_to_all(branch, GZ, split_axis=0, concat_axis=0)
    out = call(output_kernel, (128, 8, 64), f32, branch, latent, joint)
    return out.reshape(1, 8, 16, 8, 64)


def solution(mesh):
    split = Mesh(
        mesh.devices.reshape(mesh.shape["gx"], mesh.shape["gy"], 4, 2), ("gx", "gy", "gz_0", "gz_1")
    )
    return jax.shard_map(
        layer,
        mesh=split,
        in_specs=(
            P(None, None, ALL),
            P(None, "gx", "gy", GZ, None),
            P(None, "gx", "gy", GZ),
            P(),
            P(),
            P(),
            P(None, GZ, "gx", "gy", None, None),
            P(),
        ),
        out_specs=P(None, "gx", "gy", GZ, None),
        check_vma=False,
    )
```

```python
import math

import jax
import jax.numpy as jnp
import numpy as np
from jax import lax
from jax.experimental import pallas as pl
from jax.experimental.pallas import tpu as pltpu
from jax.sharding import Mesh
from jax.sharding import PartitionSpec as P

f32 = jnp.float32
bf16 = jnp.bfloat16
i32 = jnp.int32

GRID = 64
NB = 32
ROWS = 8 * NB + 32
CELLS = float(GRID**3)
NORM_FLOOR = 1.0
GZ = ("gz_0", "gz_1")
ALL = ("gx", "gy", "gz_0", "gz_1")
C0 = math.sqrt(2.0 / math.pi)
C1 = C0 * 0.044715
VMEM = pl.BlockSpec(memory_space=pltpu.VMEM)
SMEM = pl.BlockSpec(memory_space=pltpu.SMEM)


def freq(n):
    return np.where(n < 8, n, n - 16)


def angle(f, m):
    return 2.0 * math.pi * ((f * m) % GRID) / GRID


def split_two(a):
    hi = a.astype(bf16)
    lo = (a - hi.astype(a.dtype)).astype(bf16)
    return hi, lo


def third_forward():
    kh, r, kl, c = np.meshgrid(*map(np.arange, (4, 2, 4, 8)), indexing="ij")
    k, r, c = (4 * kh + kl).reshape(-1, 1), r.reshape(-1, 1), c.reshape(-1, 1)
    z = np.repeat(np.arange(64), 8)[None, :]
    cc = np.tile(np.arange(8), 64)[None, :]
    a = angle(k, z)
    v = np.where(r == 0, np.cos(a), -np.sin(a)) * (c == cc)
    return split_two(v)


def third_inverse():
    z = np.repeat(np.arange(64), 8)[:, None]
    o = np.tile(np.arange(8), 64)[:, None]
    s, kh, kl, r, oo = (
        a.reshape(1, -1) for a in np.meshgrid(*map(np.arange, (2, 4, 4, 2, 8)), indexing="ij")
    )
    k = 4 * kh + kl
    a = angle(k, z)
    w = np.where(k == 0, 1.0, 2.0) / CELLS
    cos, sin = np.cos(a), np.sin(a)
    v = np.where(s == 0, np.where(r == 0, cos, -sin), np.where(r == 0, -sin, -cos))
    return (v * w * (o == oo)).astype(bf16)


def plane_tables():
    jl, il, jh, ih = (a.reshape(-1) for a in np.meshgrid(*map(np.arange, (2, 2, 8, 8)), indexing="ij"))
    fwd = freq(2 * ih + il), freq(2 * jh + jl)
    il, jh, ih, jl = (a.reshape(-1) for a in np.meshgrid(*map(np.arange, (2, 8, 8, 2)), indexing="ij"))
    inv = freq(2 * ih + il), freq(2 * jh + jl)
    return fwd, inv, np.repeat(np.arange(8), 16), np.tile(np.arange(16), 8)


def partner_table():
    _, (fi, fj), _, _ = plane_tables()
    hit = (fi[:, None] == -fi[None, :]) & (fj[:, None] == -fj[None, :])
    return hit.astype(np.float32).astype(bf16)


def mode_masks():
    jl, il, kl = (a.reshape(-1, 1) for a in np.meshgrid(*map(np.arange, (2, 2, 4)), indexing="ij"))
    jc, ic, _, kc, _ = (
        a.reshape(1, -1) for a in np.meshgrid(*map(np.arange, (2, 2, 2, 4, 8)), indexing="ij")
    )
    own = ((jl == jc) & (il == ic) & (kl == kc)).astype(np.float32)
    _, ib, kb, _, _ = (
        a.reshape(1, -1) for a in np.meshgrid(*map(np.arange, (8, 2, 4, 2, 8)), indexing="ij")
    )
    place = ((il == ib) & (kl == kb)).astype(np.float32)
    half = np.zeros((8, 16), np.float32)
    half[jl[:, 0], np.arange(16)] = 1.0
    return own, place, half.astype(bf16)


def placing():
    ro, oh, ol = (a.reshape(-1, 1) for a in np.meshgrid(*map(np.arange, (2, 8, 8)), indexing="ij"))
    oc, _, _, rc, lc = (
        a.reshape(1, -1) for a in np.meshgrid(*map(np.arange, (8, 2, 4, 2, 8)), indexing="ij")
    )
    return ((ro == rc) & (oh == oc) & (ol == lc)).astype(np.float32).astype(bf16)


def dot(a, b):
    return jnp.dot(a, b, preferred_element_type=f32)


def dot_t(a, b):
    return lax.dot_general(a, b, (((1,), (1,)), ((), ())), preferred_element_type=f32)


def gelu_twice(v):
    return v * jnp.tanh(v * (v * v * C1 + C0)) + v


def column(line):
    return jnp.broadcast_to(line, (128, 128)).T


def rank_rows(rank, first, count):
    r = lax.broadcasted_iota(i32, (count, 1024), 0) + first
    return jnp.where(r == rank, 1.0, 0.0).astype(bf16)


def sort_kernel(
    place_ref, nb_ref, cnt_ref, kernel_in_ref, kernel_mid_ref, code_ref, rank_ref, scnt_ref, ki_ref, km_ref, tile_ref
):
    ki = jnp.concatenate([kernel_in_ref[...].astype(f32), jnp.zeros((2, 80), f32)], axis=0)
    ki_ref[...] = jnp.concatenate([ki, jnp.zeros((8, 48), f32)], axis=1).T[0:80].astype(bf16)
    km = jnp.concatenate([kernel_mid_ref[...].astype(f32) * 0.5, jnp.zeros((80, 48), f32)], axis=1)
    km_ref[...] = km.T[0:80].astype(bf16)
    px, py, pz = place_ref[0], place_ref[1], place_ref[2]
    j = nb_ref[...]
    owner = j >> 9
    dz = (owner & 7) - pz + 1
    dy = ((owner >> 3) & 3) - py + 1
    dx = (owner >> 5) - px + 1
    group = jnp.where(dz == 1, 72, (dz >> 1) * 36)
    chunk = ((group + (dy * 3 + dx) * 4 + ((j >> 7) & 3)) & 127).astype(f32)
    lane = (j & 127).astype(f32)
    counts = cnt_ref[...].astype(f32)
    row8 = lax.broadcasted_iota(i32, (8, 128), 0)
    lane8 = lax.broadcasted_iota(i32, (8, 128), 1)
    key = counts * 1024.0 - (row8 * 128 + lane8).astype(f32)
    flat = [key[z : z + 1] for z in range(8)]
    ranks = [jnp.zeros((128, 128), f32) for _ in range(8)]
    for z in range(8):
        own = column(flat[z])
        ranks = [r + jnp.where(own > line, 1.0, 0.0) for r, line in zip(ranks, flat)]
    rank = jnp.concatenate([jnp.sum(r, axis=0, keepdims=True) for r in ranks], axis=1).astype(i32)
    rank_ref[...] = jnp.broadcast_to(rank, (8, 1024))
    node = lax.broadcasted_iota(i32, (8, 1024), 1)
    wide = lax.broadcasted_iota(i32, (8, 1024), 0)
    line = jnp.concatenate([counts[z : z + 1] for z in range(8)], axis=1)
    tail = jnp.where(wide == 1, (node >> 7).astype(f32), (node & 127).astype(f32))
    tail = jnp.where(wide == 0, line, tail)
    rows = [jnp.concatenate([a[:, z, :] for z in range(8)], axis=1) for a in (chunk, lane)]
    rows = jnp.concatenate(rows + [tail], axis=0).astype(bf16)
    slot = lax.broadcasted_iota(i32, (NB, 128), 0)
    words, most = [], []
    for t in range(4):
        found = dot_t(rows, rank_rows(rank, t * 256, 256))
        tail = found[2 * NB : 2 * NB + 8]
        scnt_ref[:, t * 256 : t * 256 + 256] = jnp.broadcast_to(tail[0:1], (8, 256))
        cell = (tail[1:2] * 128.0 + tail[2:3]) * 16384.0
        word = (found[0:NB] * 128.0 + found[NB : 2 * NB] + cell).astype(i32)
        length = tail[0:1].astype(i32)
        for h in range(2):
            at = slice(h * 128, h * 128 + 128)
            words.append(jnp.where(slot < length[:, at], word[:, at], -1))
            most.append(jnp.max(length[:, at]))
    end = 0
    for t in range(8):
        code_ref[pl.ds(end, NB), :] = words[t]
        end = end + most[t]
        tile_ref[t] = end
    code_ref[pl.ds(end, 16), :] = jnp.full((16, 128), -1, i32)
    tile_ref[8] = (end + 15) >> 4


def pair_sums(place_ref, tile_ref, code_ref, look_up, ki_ref, km_ref, turn, acc_refs):
    px, py, pz = place_ref[0], place_ref[1], place_ref[2]
    x0 = px.astype(f32) * 8.0 + 0.5
    y0 = py.astype(f32) * 16.0 + 0.5
    z0 = pz.astype(f32) * 8.0 + 0.5
    turn[...] = jnp.zeros(turn.shape, f32)
    steps = tile_ref[8]
    ends = [tile_ref[t] for t in range(7)]

    def gather(b):
        lines = []
        for half in range(2):
            code = code_ref[pl.ds(pl.multiple_of(b * 16 + half * 8, 8), 8), :]
            cell = code >> 14
            centres = (
                (((cell >> 4) & 7).astype(f32) + x0) * (1.0 / GRID),
                ((cell & 15).astype(f32) + y0) * (1.0 / GRID),
                ((cell >> 7).astype(f32) + z0) * (1.0 / GRID),
            )
            values = look_up(code, b * 2 + half)
            for c in range(6):
                value = values[c]
                if c < 3:
                    value = value - centres[c]
                turn[half, c] = jnp.where(code >= 0, value, 0.0)
            lines += [turn[half, :, n, :] for n in range(8)]
        return jnp.concatenate(lines, axis=1)

    def add(b, pair):
        hidden = gelu_twice(dot(ki_ref[...], pair.astype(bf16))).astype(bf16)
        hidden = gelu_twice(dot(km_ref[...], hidden))
        for r in range(16):
            tile = sum((b * 16 + r >= end).astype(i32) for end in ends)
            acc_refs[r % 2][tile] += hidden[:, r * 128 : r * 128 + 128]

    def step(b, pair):
        following = gather(b + 1)
        add(b, pair)
        return following

    add(steps - 1, lax.fori_loop(0, steps - 1, step, gather(0)))


def lane_gather(line, at):
    return jnp.take_along_axis(jnp.broadcast_to(line, (8, 128)), at, axis=1, mode="promise_in_bounds")


def packed(parts, words):
    most = jnp.zeros((24, 128), f32)
    for part in parts:
        most = jnp.maximum(most, jnp.max(jnp.abs(part[...]), axis=0))
    most = jnp.maximum(jnp.max(most, axis=1, keepdims=True), 1e-30)
    place = jnp.broadcast_to(jnp.max(most[0:12], axis=0, keepdims=True), (12, 128))
    normal = jnp.broadcast_to(jnp.max(most[12:24], axis=0, keepdims=True), (12, 128))
    upper, lower = 32767.0 / place, 32767.0 / normal
    for n in range(9 * len(parts)):
        part = parts[n // 9]
        p = (part[n % 9, 0:12] * upper + 32768.5).astype(i32)
        q = (part[n % 9, 12:24] * lower + 32768.5).astype(i32)
        words[n] = (p << 16) | q
    return place[0:8] * (1.0 / 32767.0), normal[0:8] * (1.0 / 32767.0)


def pick_word(words, c, code, count):
    levels = (count - 1).bit_length()
    at = code & 127
    bits = [(code & (128 << n)) != 0 for n in range(levels)]

    def pick(lo, level):
        if lo >= count:
            return None
        if level == 0:
            row = c * 4 + lo % 4
            return lane_gather(words[lo // 4, row : row + 1, :], at)
        first = pick(lo, level - 1)
        second = pick(lo + (1 << (level - 1)), level - 1)
        return first if second is None else jnp.where(bits[level - 1], second, first)

    return pick(0, levels)


def near_kernel(tile_ref, same_ref, code_ref, out_ref, unit_ref, words):
    unit_ref[0], unit_ref[1] = packed((same_ref,), words)

    def step(b, carry):
        for half in range(2):
            code = code_ref[pl.ds(pl.multiple_of(b * 16 + half * 8, 8), 8), :] - 72 * 128
            for c in range(3):
                out_ref[b * 2 + half, c] = pick_word(words, c, code, 36)
        return carry

    lax.fori_loop(0, tile_ref[8], step, 0)


def encoder_kernel(
    place_ref,
    tile_ref,
    below_ref,
    above_ref,
    code_ref,
    near_ref,
    unit_ref,
    rank_ref,
    scnt_ref,
    ki_ref,
    km_ref,
    ko_ref,
    out_ref,
    words,
    turn,
    even_ref,
    odd_ref,
):
    far_place, far_normal = packed((below_ref, above_ref), words)
    near_place, near_normal = unit_ref[0], unit_ref[1]
    for ref in (even_ref, odd_ref):
        ref[...] = jnp.zeros(ref.shape, f32)

    def look_up(code, block):
        near = (code & 16383) >= 72 * 128
        upper = jnp.where(near, near_place, far_place)
        lower = jnp.where(near, near_normal, far_normal)
        values = [None] * 6
        for c in range(3):
            word = jnp.where(near, near_ref[block, c], pick_word(words, c, code, 72))
            values[c] = (lax.shift_right_logical(word, 16) - 32768).astype(f32) * upper
            values[c + 3] = ((word & 65535) - 32768).astype(f32) * lower
        return values

    pair_sums(place_ref, tile_ref, code_ref, look_up, ki_ref, km_ref, turn, (even_ref, odd_ref))
    mean = jnp.concatenate([even_ref[t] + odd_ref[t] for t in range(8)], axis=1) * (0.5 / scnt_ref[0:1])
    upper = mean.astype(bf16)
    lower = (mean - upper.astype(f32)).astype(bf16)
    latent = (dot(ko_ref[...], upper) + dot(ko_ref[...], lower)).astype(bf16)
    rank = rank_ref[0:1]
    spread = jnp.zeros((64, 1024), f32)
    for t in range(4):
        spread = spread + dot(latent[:, t * 256 : t * 256 + 256], rank_rows(rank, t * 256, 256))
    out_ref[...] = spread.astype(bf16).reshape(8, 8, 1024)


def forward_kernel(m_ref, ahi_ref, alo_ref, whi_ref, wlo_ref, out_ref, wide):
    rows = [
        m_ref[s].astype(f32)[:, z * 128 : (z + 1) * 128] for s in range(8) for z in range(8)
    ]
    cells = jnp.concatenate(rows, axis=0).astype(bf16)
    z = dot(ahi_ref[...], cells) + dot(alo_ref[...], cells)
    right = []
    for kh in range(4):
        right += [z[kh * 64 + 32 : kh * 64 + 64], -z[kh * 64 : kh * 64 + 32]]
    both = jnp.concatenate([z, jnp.concatenate(right, axis=0)], axis=1).astype(bf16)
    p = dot_t(whi_ref[...], both) + dot_t(wlo_ref[...], both)
    for kh in range(4):
        for h in range(2):
            line = jnp.concatenate(
                [p[q * 64 : (q + 1) * 64, kh * 64 : (kh + 1) * 64] for q in (2 * h, 2 * h + 1)], axis=1
            )
            for jh in range(8):
                wide[pl.ds(((jh * 4 + kh) * 8) * 2 + h, 8, stride=2), :] = line[jh * 8 : jh * 8 + 8]
    out_ref[...] = wide[...].astype(bf16)


def mix_kernel(r_ref, w_ref, own_ref, sel_ref, place_ref, half_ref, out_ref):
    s = jnp.sum(r_ref[...].astype(f32), axis=0)
    s = s.astype(bf16).astype(f32)
    own = own_ref[...]
    g = jnp.zeros((16, 128), f32)
    for ch in range(8):
        line = jnp.concatenate([s[2 * ch : 2 * ch + 1], s[2 * ch + 1 : 2 * ch + 2]], axis=1)
        g = g + dot((line * own).astype(bf16), w_ref[ch])
    spread = dot(g.astype(bf16), sel_ref[...]) * place_ref[...]
    d = dot(half_ref[...], spread.astype(bf16))
    d = jnp.concatenate([d[0:2, oh * 128 : (oh + 1) * 128] for oh in range(8)], axis=0).astype(bf16)
    for n in range(32):
        out_ref[n] = d


def inverse_kernel(q_ref, v_ref, bc_ref, bs_ref, partner_ref, out_ref):
    blocks = []
    for kh in range(4):
        rows = jnp.concatenate([q_ref[jh, kh] for jh in range(8)], axis=0).astype(f32)
        blocks.append(jnp.concatenate([rows[:, 0:64], rows[:, 64:128]], axis=0))
    x = jnp.concatenate(blocks, axis=1)
    row = lax.broadcasted_iota(i32, (256, 256), 0)
    lane = lax.broadcasted_iota(i32, (256, 256), 1)
    x = jnp.where((row == 0) & (lane < 8), 0.0, x)
    xb = x.astype(bf16)
    twin = dot(partner_ref[...], xb[:, 0:128])
    low = lane[0:1, 0:128]
    side = jnp.where(low < 8, 0.5, jnp.where(low < 16, -0.5, 0.0))
    weight = jnp.where(lane[0:1, :] < 16, 0.5, 2.0)
    power = jnp.sum(x * x, axis=0, keepdims=True) * weight
    cross = jnp.sum(x[:, 0:128] * twin, axis=0, keepdims=True) * side
    power = jnp.broadcast_to(power[:, 0:128] + power[:, 128:256] + cross, (8, 128))
    for shift in (8, 16, 32, 64):
        power = power + pltpu.roll(power, shift, 1)
    scale = lax.rsqrt(power * (1.0 / (CELLS * CELLS)) + NORM_FLOOR)[0:1]
    scale = jnp.concatenate([scale, scale], axis=1)
    g = (dot(v_ref[...], xb) * scale).astype(bf16)
    out = dot_t(bc_ref[...], g[0:128]) + dot_t(bs_ref[...], g[128:256])
    out_ref[...] = out.astype(bf16).reshape(8, 8, 8, 128)


def output_kernel(y_ref, lat_ref, w_ref, out_ref):
    for z in range(8):
        y = jnp.concatenate([y_ref[s, z].astype(f32) for s in range(8)], axis=0)
        lat = jnp.concatenate(
            [lat_ref[s].astype(f32)[:, z * 128 : (z + 1) * 128] for s in range(8)], axis=0
        )
        both = jnp.concatenate([lat, y], axis=0).T.astype(bf16)
        v = dot(both, w_ref[...])
        out_ref[:, z, :] = 0.5 * gelu_twice(v)


def call(kernel, shape, dtype, *args, scratch=(), smem=0):
    return pl.pallas_call(
        kernel,
        out_shape=jax.ShapeDtypeStruct(shape, dtype),
        in_specs=[SMEM] * smem + [VMEM] * (len(args) - smem),
        out_specs=VMEM,
        scratch_shapes=list(scratch),
        compiler_params=pltpu.CompilerParams(vmem_limit_bytes=48 * 1024 * 1024),
    )(*args)


def sorted_nodes(place, near, valid, kernel_in, kernel_mid):
    shapes = (
        ((ROWS, 128), i32),
        ((8, 1024), i32),
        ((8, 1024), f32),
        ((80, 8), bf16),
        ((80, 80), bf16),
        ((9,), i32),
    )
    return pl.pallas_call(
        sort_kernel,
        out_shape=[jax.ShapeDtypeStruct(*s) for s in shapes],
        in_specs=[SMEM] + [VMEM] * 4,
        out_specs=[VMEM] * 5 + [SMEM],
        compiler_params=pltpu.CompilerParams(vmem_limit_bytes=48 * 1024 * 1024),
        name="sort",
    )(place, near, valid, kernel_in, kernel_mid)


def near_words(tiles, same, code):
    shapes = (((ROWS // 8, 3, 8, 128), i32), ((2, 8, 128), f32))
    return pl.pallas_call(
        near_kernel,
        out_shape=[jax.ShapeDtypeStruct(*s) for s in shapes],
        in_specs=[SMEM, VMEM, VMEM],
        out_specs=[VMEM] * 2,
        scratch_shapes=[pltpu.VMEM((9, 12, 128), i32)],
        compiler_params=pltpu.CompilerParams(vmem_limit_bytes=48 * 1024 * 1024),
        name="near",
    )(tiles, same, code)


def beside(cells, axis):
    count = lax.axis_size(axis)
    ends = count - 1
    lower = lax.ppermute(cells, axis, [(i, i + 1) for i in range(ends)])
    upper = lax.ppermute(cells, axis, [(i + 1, i) for i in range(ends)])
    return lower, cells, upper


def turned(cos, sin, phase):
    c, s = jnp.cos(phase), jnp.sin(phase)
    return cos * c - sin * s, sin * c + cos * s


def layer(point_data, neighbours, counts, kernel_in, kernel_mid, kernel_out, spectral, skip_weight):
    gx = lax.axis_index("gx")
    gy = lax.axis_index("gy")
    gz = lax.axis_index(GZ)
    place = jnp.stack([gx, gy, gz]).astype(i32)

    own = point_data.reshape(1, 24, 128)
    near = neighbours[0].transpose(3, 2, 0, 1).reshape(NB, 8, 128)
    valid = counts[0].transpose(2, 0, 1).reshape(8, 128)

    line = jnp.concatenate(beside(own, "gx"), axis=0)
    plane = jnp.concatenate(beside(line, "gy"), axis=0)
    tables = sorted_nodes(place, near, valid, kernel_in, kernel_mid)
    plane, tables = lax.optimization_barrier((plane, tables))
    code, rank, sorted_counts, ki, km, tiles = tables
    below, same, above = beside(plane, GZ)
    words, units = near_words(tiles, same, code)
    latent = call(
        encoder_kernel,
        (8, 8, 1024),
        bf16,
        place,
        tiles,
        below,
        above,
        code,
        words,
        units,
        rank,
        sorted_counts,
        ki,
        km,
        kernel_out.T,
        scratch=(
            pltpu.VMEM((18, 12, 128), i32),
            pltpu.VMEM((2, 8, 8, 128), f32),
            pltpu.VMEM((8, 80, 128), f32),
            pltpu.VMEM((8, 80, 128), f32),
        ),
        smem=2,
    )

    latent, spectral, gx, gy = lax.optimization_barrier((latent, spectral, gx, gy))
    (ffi, ffj), (ifi, ifj), xl, yl = plane_tables()
    local = angle(1, ffi[:, None] * xl[None, :] + ffj[:, None] * yl[None, :])
    phase = ((jnp.asarray(ffi, i32) * 8 * gx + jnp.asarray(ffj, i32) * 16 * gy) % GRID).astype(f32)
    cos, sin = turned(
        np.cos(local).astype(np.float32),
        np.sin(local).astype(np.float32),
        (phase * (2.0 * math.pi / GRID))[:, None],
    )
    whi, wlo = split_two(jnp.concatenate([cos, sin], axis=1))
    local = angle(1, ifi[None, :] * xl[:, None] + ifj[None, :] * yl[:, None])
    phase = ((jnp.asarray(ifi, i32) * 8 * gx + jnp.asarray(ifj, i32) * 16 * gy) % GRID).astype(f32)
    cos, sin = turned(
        np.cos(local).astype(np.float32),
        np.sin(local).astype(np.float32),
        (phase * (2.0 * math.pi / GRID))[None, :],
    )
    back = jnp.concatenate([cos, sin], axis=0).astype(bf16)

    w = spectral.reshape(2, 2, 2, 4, 8, 8, 64).transpose(0, 4, 2, 1, 3, 5, 6)
    wr, wi = w[0], w[1]
    mixing = jnp.stack(
        [jnp.concatenate([wr, wi], axis=-1), jnp.concatenate([-wi, wr], axis=-1)], axis=3
    ).reshape(8, 256, 128)
    joint = jnp.concatenate([skip_weight, jnp.eye(64, dtype=bf16)], axis=0)

    depth = lax.all_to_all(latent, GZ, split_axis=0, concat_axis=0)
    ahi, alo = third_forward()
    partial = call(forward_kernel, (512, 128), bf16, depth, ahi, alo, whi, wlo, scratch=(pltpu.VMEM((512, 128), f32),))
    partial = lax.all_to_all(partial.reshape(256, 2, 128), ALL, split_axis=0, concat_axis=0)
    own_mask, place_mask, half = mode_masks()
    mixed = call(
        mix_kernel,
        (32, 16, 128),
        bf16,
        partial.reshape(32, 16, 128),
        mixing,
        own_mask,
        placing(),
        place_mask,
        half,
    )
    mixed = lax.all_to_all(mixed.reshape(256, 2, 128), ALL, split_axis=0, concat_axis=0)
    third = third_inverse()
    branch = call(
        inverse_kernel,
        (8, 8, 8, 128),
        bf16,
        mixed.reshape(8, 4, 16, 128),
        back,
        third[:, :256],
        third[:, 256:],
        partner_table(),
    )
    branch = lax.all_to_all(branch, GZ, split_axis=0, concat_axis=0)
    out = call(output_kernel, (128, 8, 64), f32, branch, latent, joint)
    return out.reshape(1, 8, 16, 8, 64)


def solution(mesh):
    split = Mesh(
        mesh.devices.reshape(mesh.shape["gx"], mesh.shape["gy"], 4, 2), ("gx", "gy", "gz_0", "gz_1")
    )
    return jax.shard_map(
        layer,
        mesh=split,
        in_specs=(
            P(None, None, ALL),
            P(None, "gx", "gy", GZ, None),
            P(None, "gx", "gy", GZ),
            P(),
            P(),
            P(),
            P(None, GZ, "gx", "gy", None, None),
            P(),
        ),
        out_specs=P(None, "gx", "gy", GZ, None),
        check_vma=False,
    )
```
